32 devices in a mesh: rep: 1 (over z), dp: 32 (over x, y, core).
Axes of the slice: x: 4, y: 4, z: 1, core: 2. Of those that a mesh axis runs over, the one named last changes fastest.
The devices are a block of a 4x4x8 slice.
Arguments:
- x: bfloat16 [32, 2048, 1152], P(('rep', 'dp'))
- dy: bfloat16 [32, 2048, 1152], P(('rep', 'dp'))
- w_gate: bfloat16 [2, 1152, 4608], replicated
- w_up: bfloat16 [2, 1152, 4608], replicated
- w_down: bfloat16 [2, 4608, 1152], replicated
- m_w_gate: float32 [2, 1152, 4608], P(None, 'dp')
- m_w_up: float32 [2, 1152, 4608], P(None, 'dp')
- m_w_down: float32 [2, 4608, 1152], P(None, 'dp')
- v_w_gate: float32 [2, 1152, 4608], P(None, 'dp')
- v_w_up: float32 [2, 1152, 4608], P(None, 'dp')
- v_w_down: float32 [2, 4608, 1152], P(None, 'dp')
Outputs:
- output 1: bfloat16 [2, 1152, 4608], P('rep')
- output 2: bfloat16 [2, 1152, 4608], P('rep')
- output 3: bfloat16 [2, 4608, 1152], P('rep')
- output 4: float32 [2, 1152, 4608], P('rep', 'dp')
- output 5: float32 [2, 1152, 4608], P('rep', 'dp')
- output 6: float32 [2, 4608, 1152], P('rep', 'dp')
- output 7: float32 [2, 1152, 4608], P('rep', 'dp')
- output 8: float32 [2, 1152, 4608], P('rep', 'dp')
- output 9: float32 [2, 4608, 1152], P('rep', 'dp')
All inputs are finite; a program needn't handle non-finite values.
Results may differ from the reference program's by a relative error of at most 0.022.
Values are sent between devices in bfloat16 or wider.
A program may use at most 768 MiB of HBM per device.

```python
import jax
import jax.numpy as jnp
from jax import lax

SEQUENCES = 32
TOKENS = 2048
D = 1152
FF = 4608
LAYERS = 2
NAMES = ("w_gate", "w_up", "w_down")
SHAPES = {"w_gate": (LAYERS, D, FF), "w_up": (LAYERS, D, FF), "w_down": (LAYERS, FF, D)}


def bump(key, n, height):
    away = (jnp.arange(n, dtype=jnp.int32) - jax.random.randint(key, (), 0, n, jnp.int32)) % n
    return jnp.where(away < n // 8, height, 1.0)


def together(key, own, strength):
    shared = jax.random.normal(key, own.shape[1:], jnp.float32)
    return (own + strength * shared) * lax.rsqrt(1 + strength * strength)


def setup_inputs(seed: int = 0, part: int = 0) -> dict:
    kx, kdy, ka, kb, kz, kf, kh, kl, *keys = jax.random.split(jax.random.key(seed), 8 + 3 * len(NAMES))
    kx, kdy, ka, kb = (jax.random.fold_in(k, part) for k in (kx, kdy, ka, kb))
    kw, km, kv = (keys[i::3] for i in range(3))
    shape = (SEQUENCES, TOKENS, D)
    much_x, much_dy = jax.random.uniform(kz, (2,), jnp.float32, 0.0, 1.0)
    loud = 2.0 ** jax.random.uniform(jax.random.fold_in(kz, 1), (), jnp.float32, -1.0, 2.0)
    layers = 2.0 ** jax.random.uniform(kl, (LAYERS, 1, 1), jnp.float32, -1.0, 1.0)
    x = together(ka, jax.random.normal(kx, shape, jnp.float32), much_x) * bump(kf, D, 4.0)
    dy = together(kb, jax.random.normal(kdy, shape, jnp.float32), much_dy)
    drawn = {"x": x.astype(jnp.bfloat16), "dy": (loud * dy * (SEQUENCES * TOKENS) ** -0.5).astype(jnp.bfloat16)}
    for key, name in zip(kw, NAMES, strict=True):
        w = jax.random.normal(key, SHAPES[name], jnp.float32) * SHAPES[name][1] ** -0.5
        drawn[name] = (w * {"w_gate": 1.0, "w_up": bump(kh, FF, 4.0), "w_down": layers}[name]).astype(jnp.bfloat16)
    for key, name in zip(km, NAMES, strict=True):
        drawn[f"m_{name}"] = 0.1 * jax.random.normal(key, SHAPES[name], jnp.float32)
    for key, name in zip(kv, NAMES, strict=True):
        drawn[f"v_{name}"] = jax.random.uniform(key, SHAPES[name], jnp.float32, 0.005, 0.015)
    return drawn


def matmul(a, w):
    return jnp.dot(a, w, preferred_element_type=jnp.float32).astype(jnp.bfloat16)


def normed(h):
    wide = h.astype(jnp.float32)
    scale = lax.rsqrt(jnp.mean(wide**2, -1, keepdims=True) + 1e-6)
    return (wide * scale).astype(jnp.bfloat16)


def layer(h, w):
    a = normed(h)
    gate = jnp.dot(a, w["w_gate"], preferred_element_type=jnp.float32)
    up = jnp.dot(a, w["w_up"], preferred_element_type=jnp.float32)
    return h + matmul((jax.nn.silu(gate) * up).astype(jnp.bfloat16), w["w_down"])


def adamw(w, m, v, g):
    m = 0.9 * m + 0.1 * g
    v = 0.95 * v + 0.05 * g * g
    step = m * lax.rsqrt(v + 1e-8) + 0.1 * w
    return (w - 0.02 * step).astype(jnp.bfloat16), m, v


def clipped(gradients, sum_of_squares, count):
    factor = jnp.minimum(1.0, 0.5 * lax.rsqrt(sum_of_squares / count + 1e-30))
    return [g * factor for g in gradients]


def stack(weights, h):
    return lax.scan(lambda h, w: (layer(h, w), None), h, weights)[0]


def reference(x, dy, w_gate, w_up, w_down, m_w_gate, m_w_up, m_w_down, v_w_gate, v_w_up, v_w_down):
    weights = dict(zip(NAMES, (w_gate, w_up, w_down), strict=True))

    def take(so_far, sequence):
        h, by_y = sequence
        _, back = jax.vjp(lambda w: stack(w, h), weights)
        return jax.tree.map(lambda total, term: total + term.astype(jnp.float32), so_far, back(by_y)[0]), None

    none_yet = {name: jnp.zeros(w.shape, jnp.float32) for name, w in weights.items()}
    by_weights, _ = lax.scan(take, none_yet, (x, dy))
    gradients = [by_weights[name].astype(jnp.bfloat16).astype(jnp.float32) for name in NAMES]
    gradients = clipped(gradients, sum(jnp.sum(g * g) for g in gradients), sum(g.size for g in gradients))
    new = [
        adamw(w.astype(jnp.float32), m, v, g)
        for w, m, v, g in zip((w_gate, w_up, w_down), (m_w_gate, m_w_up, m_w_down), (v_w_gate, v_w_up, v_w_down), gradients, strict=True)
    ]
    return tuple(one[which] for which in range(3) for one in new)
```

```python
import functools
import math

import jax
import jax.numpy as jnp
from jax import lax
from jax.experimental import pallas as pl
from jax.experimental.pallas import tpu as pltpu
from jax.sharding import PartitionSpec as P

F32, BF16 = jnp.float32, jnp.bfloat16
VMEM_LIMIT = 67_043_328
NN = (((1,), (0,)), ((), ()))
NT = (((1,), (1,)), ((), ()))
TN = (((0,), (0,)), ((), ()))


def dot(a, b, dims=NN):
    return lax.dot_general(a, b, dims, preferred_element_type=F32)


def sigmoid(x):
    return 1.0 / (1.0 + jnp.exp(-x))


def whole(shape):
    return pl.BlockSpec(shape, lambda *_: (0,) * len(shape), pipeline_mode=pl.Buffered(1))


def call(body, flops, moved, params=None, **kw):
    return pl.pallas_call(
        body,
        cost_estimate=pl.CostEstimate(flops=int(flops), bytes_accessed=int(moved), transcendentals=0),
        compiler_params=pltpu.CompilerParams(vmem_limit_bytes=VMEM_LIMIT, **(params or {})),
        **kw,
    )


def row_scale(wide):
    return lax.rsqrt(jnp.mean(wide * wide, -1, keepdims=True) + 1e-6)


def normed(x):
    tokens, d = x.shape
    bm = 512

    def body(x, a, a_t):
        wide = x[...].astype(F32)
        unit = wide * row_scale(wide)
        a[...] = unit.astype(BF16)
        a_t[...] = unit.T.astype(BF16)

    return call(
        body,
        10 * tokens * d,
        6 * tokens * d,
        name="normed",
        grid=(tokens // bm,),
        in_specs=[pl.BlockSpec((bm, d), lambda i: (i, 0))],
        out_specs=[pl.BlockSpec((bm, d), lambda i: (i, 0)), pl.BlockSpec((d, bm), lambda i: (0, i))],
        out_shape=(jax.ShapeDtypeStruct((tokens, d), BF16), jax.ShapeDtypeStruct((d, tokens), BF16)),
    )(x)


def hidden_forward(layer, a, w_gate, w_up):
    tokens, d = a.shape
    ff = w_gate.shape[-1]
    bf, bm = 256, 512

    def body(a, wg, wu, gate, up, hid):
        for i in range(tokens // bm):
            r = slice(i * bm, (i + 1) * bm)
            g, u = dot(a[r, :], wg[...]), dot(a[r, :], wu[...])
            gate[r, :] = g
            up[r, :] = u
            hid[r, :] = (g * sigmoid(g) * u).astype(BF16)

    w_spec = pl.BlockSpec((None, d, bf), lambda j: (layer, 0, j))
    o_spec = pl.BlockSpec((tokens, bf), lambda j: (0, j))
    wide = jax.ShapeDtypeStruct((tokens, ff), F32)
    return call(
        body,
        4 * tokens * d * ff,
        10 * tokens * ff + 4 * d * ff,
        name="hidden_forward",
        grid=(ff // bf,),
        in_specs=[whole((tokens, d)), w_spec, w_spec],
        out_specs=[o_spec] * 3,
        out_shape=(wide, wide, jax.ShapeDtypeStruct((tokens, ff), BF16)),
    )(a, w_gate, w_up)


def down_forward(layer, x, hid, w_down):
    tokens, ff = hid.shape
    d = x.shape[-1]
    bm = 256

    def body(x, hid, wd, h1, a1, a1_t):
        h = (x[...].astype(F32) + dot(hid[...], wd[...]).astype(BF16).astype(F32)).astype(BF16)
        h1[...] = h
        wide = h.astype(F32)
        unit = wide * row_scale(wide)
        a1[...] = unit.astype(BF16)
        a1_t[...] = unit.T.astype(BF16)

    rows = pl.BlockSpec((bm, d), lambda i: (i, 0))
    out = jax.ShapeDtypeStruct((tokens, d), BF16)
    return call(
        body,
        2 * tokens * d * ff,
        2 * tokens * ff + 2 * d * ff,
        name="down_forward",
        grid=(tokens // bm,),
        in_specs=[
            rows,
            pl.BlockSpec((bm, ff), lambda i: (i, 0)),
            pl.BlockSpec((None, ff, d), lambda i: (layer, 0, 0), pipeline_mode=pl.Buffered(1)),
        ],
        out_specs=[rows, rows, pl.BlockSpec((d, bm), lambda i: (0, i))],
        out_shape=(out, out, jax.ShapeDtypeStruct((d, tokens), BF16)),
    )(x, hid, w_down)


def gate_up_cotangents(g, u, dh):
    dh = dh.astype(BF16).astype(F32)
    s = sigmoid(g)
    silu = g * s
    return (dh * u * (s + silu * (1.0 - s))).astype(BF16), (dh * silu).astype(BF16), (silu * u).astype(BF16)


def last_layer(layer, a, dy, w_gate, w_up, w_down):
    tokens, d = a.shape
    ff = w_gate.shape[-1]
    bf, bm = 256, 512

    def body(a, dy, wg, wu, wd, hid, dg, du):
        for i in range(tokens // bm):
            r = slice(i * bm, (i + 1) * bm)
            g, u = dot(a[r, :], wg[...]), dot(a[r, :], wu[...])
            dg[r, :], du[r, :], hid[r, :] = gate_up_cotangents(g, u, dot(dy[r, :], wd[...], NT))

    w_spec = pl.BlockSpec((None, d, bf), lambda j: (layer, 0, j))
    o_spec = pl.BlockSpec((tokens, bf), lambda j: (0, j))
    out = jax.ShapeDtypeStruct((tokens, ff), BF16)
    return call(
        body,
        6 * tokens * d * ff,
        6 * tokens * ff + 6 * d * ff,
        name="last_layer",
        grid=(ff // bf,),
        in_specs=[whole((tokens, d)), whole((tokens, d)), w_spec, w_spec, pl.BlockSpec((None, bf, d), lambda j: (layer, j, 0))],
        out_specs=[o_spec] * 3,
        out_shape=(out, out, out),
    )(a, dy, w_gate, w_up, w_down)


def states_cotangent(layer, h, dy, dg, du, w_gate, w_up):
    tokens, ff = dg.shape
    d = h.shape[-1]
    bf, bm, be = 512, 1024, 256
    n = ff // bf

    def body(h, dy, dg, du, wg, wu, out, total):
        j = pl.program_id(0)

        @pl.when(j == 0)
        def _():
            total[...] = jnp.zeros_like(total)

        for i in range(tokens // bm):
            r = slice(i * bm, (i + 1) * bm)
            total[r, :] += dot(dg[r, :], wg[...], NT) + dot(du[r, :], wu[...], NT)

        @pl.when(j == n - 1)
        def _():
            def rows(i, _):
                r = pl.ds(pl.multiple_of(i * be, be), be)
                wide = h[r, :].astype(F32)
                da = total[r, :].astype(BF16).astype(F32)
                s = row_scale(wide)
                back = da * s - wide * (s * s * s * jnp.mean(da * wide, -1, keepdims=True))
                out[r, :] = (dy[r, :].astype(F32) + back).astype(BF16)
                return 0

            lax.fori_loop(0, tokens // be, rows, 0)

    w_spec = pl.BlockSpec((None, d, bf), lambda j: (layer, 0, j))
    t_spec = pl.BlockSpec((tokens, bf), lambda j: (0, j))
    return call(
        body,
        4 * tokens * d * ff,
        4 * tokens * ff + 4 * d * ff,
        name="states_cotangent",
        grid=(n,),
        in_specs=[whole((tokens, d)), whole((tokens, d)), t_spec, t_spec, w_spec, w_spec],
        out_specs=whole((tokens, d)),
        out_shape=jax.ShapeDtypeStruct((tokens, d), BF16),
        scratch_shapes=[pltpu.VMEM((tokens, d), F32)],
    )(h, dy, dg, du, w_gate, w_up)


SLOTS, ARRIVALS = 3, 4


def pair_scratch(rows, columns):
    return [
        pltpu.VMEM((SLOTS, 2, rows, columns), BF16),
        pltpu.VMEM((ARRIVALS, rows, columns), BF16),
        pltpu.SemaphoreType.DMA((SLOTS,)),
        pltpu.SemaphoreType.DMA((ARRIVALS,)),
    ]


def pair_step(n, make, out, made, came, sent, arrived):
    j = pl.program_id(0)
    me = lax.axis_index("dp")
    core = lax.rem(me, 2)
    other = me + 1 - 2 * core

    def transfer(step):
        slot, place = lax.rem(step, SLOTS), lax.rem(step, ARRIVALS)
        return pltpu.make_async_remote_copy(
            src_ref=made.at[slot, 1 - core],
            dst_ref=came.at[place],
            send_sem=sent.at[slot],
            recv_sem=arrived.at[place],
            device_id={"dp": other},
            device_id_type=pl.DeviceIdType.MESH,
        )

    @pl.when(j == 0)
    def _():
        barrier = pltpu.get_barrier_semaphore()
        pl.semaphore_signal(barrier, inc=1, device_id={"dp": other}, device_id_type=pl.DeviceIdType.MESH)
        pl.semaphore_wait(barrier, 1)

    @pl.when(j >= 2)
    def _():
        transfer(j - 2).wait()
        own = made[lax.rem(j - 2, SLOTS), core]
        out[...] = (own.astype(F32) + came[lax.rem(j - 2, ARRIVALS)].astype(F32)).astype(BF16)

    @pl.when(j < n)
    def _():
        make(made.at[lax.rem(j, SLOTS)])
        transfer(j).start()


def pair_params(number):
    return {"collective_id": number, "has_side_effects": True}


def down_gradient(number, hid, dy, layers, layer, into=None):
    tokens, ff = hid.shape
    d = dy.shape[-1]
    chips = lax.axis_size("dp") // 2
    own = ff // (2 * chips)
    bf = 1152
    n, per = ff // bf, bf // (2 * own)

    def body(hid, dy, *rest):
        out, *scratch = rest[0 if into is None else 1 :]

        def make(slot):
            block = dot(hid[...], dy[...], TN)
            for i in range(per):
                for half in range(2):
                    at = (2 * i + half) * own
                    slot[half, i * own : (i + 1) * own, :] = block[at : at + own].astype(BF16)

        pair_step(n, make, out, *scratch)

    more = [] if into is None else [into]
    return call(
        body,
        2 * tokens * d * ff,
        2 * tokens * ff + d * ff,
        pair_params(number),
        name=f"down_gradient_{number}",
        grid=(n + 2,),
        in_specs=[
            pl.BlockSpec((tokens, bf), lambda j: (0, jnp.minimum(j, n - 1))),
            whole((tokens, d)),
            *[pl.BlockSpec(memory_space=pl.ANY) for _ in more],
        ],
        out_specs=pl.BlockSpec((bf // 2, d), lambda j: (jnp.maximum(j - 2, 0), layer)),
        out_shape=jax.ShapeDtypeStruct((ff // 2, d * layers), BF16),
        scratch_shapes=pair_scratch(bf // 2, d),
        input_output_aliases={2: 0} if more else {},
    )(hid, dy, *more)


PART = 256


def halves_specs(shape, first, n, half, layer=None, transposed=False):
    def spec(h):
        def at(j):
            k = h * half + first + jnp.minimum(j, n - 1)
            index = (k, 0) if transposed else (0, k)
            return index if layer is None else (layer, *index)

        return pl.BlockSpec(shape, at)

    return [spec(0), spec(1)]


def gate_up_gradient(number, first, n, a_t, dg, du):
    d, tokens = a_t.shape
    half = dg.shape[-1] // (2 * PART)

    def body(a_t, dg0, dg1, du0, du1, out, *scratch):
        def make(slot):
            for h, (dg, du) in enumerate(((dg0, du0), (dg1, du1))):
                slot[h, :, :PART] = dot(a_t[...], dg[...]).astype(BF16)
                slot[h, :, PART:] = dot(a_t[...], du[...]).astype(BF16)

        pair_step(n, make, out, *scratch)

    t_specs = halves_specs((tokens, PART), first, n, half)
    return call(
        body,
        8 * tokens * d * PART * n,
        8 * tokens * PART * n,
        pair_params(number),
        name=f"gate_up_gradient_{number}",
        grid=(n + 2,),
        in_specs=[whole((d, tokens)), *t_specs, *t_specs],
        out_specs=pl.BlockSpec((d, 2 * PART), lambda j: (0, jnp.maximum(j - 2, 0))),
        out_shape=jax.ShapeDtypeStruct((d, 2 * PART * n), BF16),
        scratch_shapes=pair_scratch(d, 2 * PART),
    )(a_t, dg, dg, du, du)


SIDE = 4
PLACES = 4


def first_layer_gradient(number, layer, a_t, dy, gate, up, w_down):
    d, tokens = a_t.shape
    half = gate.shape[-1] // (2 * PART)
    n = half
    bm = 512
    rows = d // SIDE**2
    mid = PART // 2

    def body(a_t, dy, g0, g1, u0, u1, w0, w1, out, dg, du, made, came, sums, across1, pass1, got1, total1, across2, pass2, got2, ps, pr, sent, arrived):
        j = pl.program_id(0)
        me = lax.axis_index("dp")
        core = lax.rem(me, 2)
        other = me + 1 - 2 * core
        x, y = lax.div(me, 2 * SIDE), lax.rem(lax.div(me, 2), SIDE)

        def at(x, y):
            return {"dp": (x * SIDE + y) * 2 + core}

        def beside(axis, way):
            to = lax.rem((x if axis == 0 else y) + (1 if way == 0 else SIDE - 1), SIDE)
            return at(to, y) if axis == 0 else at(x, to)

        here = (x, y)

        def transfer(stage, color, way, block):
            place, slot = lax.rem(block, PLACES), lax.rem(block, SLOTS)
            first, second = color, 1 - color
            columns = slice(color * PART, (color + 1) * PART)
            if stage == 1:
                far = lax.rem(here[first] + 2, SIDE)
                part = slice(2 * way, 2 * way + 2)
                src = sums.at[slot, far, part, :, columns] if color == 0 else sums.at[slot, part, far, :, columns]
                dst = across1.at[color, place, way]
            elif stage == 2:
                src, dst = pass1.at[color, place, way], got1.at[color, place, way]
            elif stage == 3:
                far = lax.rem(here[second] + 2, SIDE)
                src = total1.at[color, place, far, :, slice(way * mid, (way + 1) * mid)]
                dst = across2.at[color, place, way]
            else:
                src, dst = pass2.at[color, place, way], got2.at[color, place, way]
            index = ((stage - 1) * 2 + color) * 2 + way
            return pltpu.make_async_remote_copy(
                src_ref=src,
                dst_ref=dst,
                send_sem=sent.at[index, place],
                recv_sem=arrived.at[index, place],
                device_id=beside(first if stage <= 2 else second, way),
                device_id_type=pl.DeviceIdType.MESH,
            )

        def swap(block):
            slot, place = lax.rem(block, SLOTS), lax.rem(block, PLACES)
            return pltpu.make_async_remote_copy(
                src_ref=made.at[slot, 1 - core],
                dst_ref=came.at[place],
                send_sem=ps.at[slot],
                recv_sem=pr.at[place],
                device_id={"dp": other},
                device_id_type=pl.DeviceIdType.MESH,
            )

        def of(color, slot, i):
            columns = slice(color * PART, (color + 1) * PART)
            t = sums[slot, i, :, :, columns] if color == 0 else sums[slot, :, i, :, columns]
            return t.astype(F32)

        def stage(lag, act):
            @pl.when((j >= lag) & (j < n + lag))
            def _():
                act(j - lag)

        @pl.when(j == 0)
        def _():
            barrier = pltpu.get_barrier_semaphore()
            for peer in ({"dp": other}, beside(0, 0), beside(0, 1), beside(1, 0), beside(1, 1)):
                pl.semaphore_signal(barrier, inc=1, device_id=peer, device_id_type=pl.DeviceIdType.MESH)
            pl.semaphore_wait(barrier, 5)

        def last(block):
            place = lax.rem(block, PLACES)
            for color in range(2):
                for way in range(2):
                    transfer(4, color, way, block).wait()
                b = here[1 - color]
                t = total1[color, place, b].astype(F32) + got2[color, place, 0].astype(F32) + got2[color, place, 1].astype(F32)
                out[color] = t.astype(BF16)

        def fourth(block):
            place = lax.rem(block, PLACES)
            for color in range(2):
                for way in range(2):
                    transfer(3, color, way, block).wait()
                for way in range(2):
                    b = lax.rem(here[1 - color] + (1 if way == 0 else SIDE - 1), SIDE)
                    pass2[color, place, way] = total1[color, place, b]
                    c = slice(way * mid, (way + 1) * mid)
                    more = total1[color, place, b, :, c].astype(F32) + across2[color, place, way].astype(F32)
                    pass2[color, place, way, :, c] = more.astype(BF16)
                    transfer(4, color, way, block).start()

        def third(block):
            place, slot = lax.rem(block, PLACES), lax.rem(block, SLOTS)
            for color in range(2):
                for way in range(2):
                    transfer(2, color, way, block).wait()
                t = of(color, slot, here[color]) + got1[color, place, 0].astype(F32) + got1[color, place, 1].astype(F32)
                total1[color, place] = t.astype(BF16)
                for way in range(2):
                    transfer(3, color, way, block).start()

        def second(block):
            place, slot = lax.rem(block, PLACES), lax.rem(block, SLOTS)
            for color in range(2):
                for way in range(2):
                    transfer(1, color, way, block).wait()
                for way in range(2):
                    t = of(color, slot, lax.rem(here[color] + (1 if way == 0 else SIDE - 1), SIDE))
                    p = slice(2 * way, 2 * way + 2)
                    q = slice(2 - 2 * way, 4 - 2 * way)
                    pass1[color, place, way, p] = (t[p] + across1[color, place, way].astype(F32)).astype(BF16)
                    pass1[color, place, way, q] = t[q].astype(BF16)
                    transfer(2, color, way, block).start()

        def first(block):
            place, slot = lax.rem(block, PLACES), lax.rem(block, SLOTS)
            swap(block).wait()
            for k in range(SIDE**2):
                r = slice(k * rows, (k + 1) * rows)
                t = made[slot, core, r, :].astype(F32) + came[place, r, :].astype(F32)
                sums[slot, k // SIDE, k % SIDE] = t.astype(BF16)
            for color in range(2):
                for way in range(2):
                    transfer(1, color, way, block).start()

        def make(block):
            slot = lax.rem(block, SLOTS)
            for h, (g, u, w) in enumerate(((g0, u0, w0), (g1, u1, w1))):
                for i in range(tokens // bm):
                    r = slice(i * bm, (i + 1) * bm)
                    dg[h, r, :], du[h, r, :], _ = gate_up_cotangents(g[r, :], u[r, :], dot(dy[r, :], w[...], NT))
                made[slot, h, :, :PART] = dot(a_t[...], dg[h]).astype(BF16)
                made[slot, h, :, PART:] = dot(a_t[...], du[h]).astype(BF16)
            swap(block).start()

        stage(6, last)
        stage(5, fourth)
        stage(4, third)
        stage(3, second)
        stage(2, first)
        stage(0, make)

    t_specs = halves_specs((tokens, PART), 0, n, half)
    block = (SIDE, rows, PART)
    return call(
        body,
        12 * tokens * d * PART * n,
        16 * tokens * PART * n,
        pair_params(number),
        name="first_layer_gradient",
        grid=(n + 6,),
        in_specs=[whole((d, tokens)), whole((tokens, d)), *t_specs, *t_specs, *halves_specs((None, PART, d), 0, n, half, layer, True)],
        out_specs=pl.BlockSpec((2, rows, PART), lambda j: (0, 0, jnp.maximum(j - 6, 0))),
        out_shape=jax.ShapeDtypeStruct((2, rows, PART * n), BF16),
        scratch_shapes=[
            pltpu.VMEM((2, tokens, PART), BF16),
            pltpu.VMEM((2, tokens, PART), BF16),
            pltpu.VMEM((SLOTS, 2, d, 2 * PART), BF16),
            pltpu.VMEM((PLACES, d, 2 * PART), BF16),
            pltpu.VMEM((SLOTS, SIDE, SIDE, rows, 2 * PART), BF16),
            pltpu.VMEM((2, PLACES, 2, SIDE // 2, rows, PART), BF16),
            pltpu.VMEM((2, PLACES, 2, *block), BF16),
            pltpu.VMEM((2, PLACES, 2, *block), BF16),
            pltpu.VMEM((2, PLACES, *block), BF16),
            pltpu.VMEM((2, PLACES, 2, rows, mid), BF16),
            pltpu.VMEM((2, PLACES, 2, rows, PART), BF16),
            pltpu.VMEM((2, PLACES, 2, rows, PART), BF16),
            pltpu.SemaphoreType.DMA((SLOTS,)),
            pltpu.SemaphoreType.DMA((PLACES,)),
            pltpu.SemaphoreType.DMA((16, PLACES)),
            pltpu.SemaphoreType.DMA((16, PLACES)),
        ],
    )(a_t, dy, gate, gate, up, up, w_down, w_down)


def summed_over_group(number, part):
    n = lax.axis_size("dp")

    def body(part, out, came, sent, arrived):
        me = lax.axis_index("dp")
        barrier = pltpu.get_barrier_semaphore()

        def greet(i, _):
            pl.semaphore_signal(barrier, inc=1, device_id={"dp": lax.rem(me + i, n)}, device_id_type=pl.DeviceIdType.MESH)
            return 0

        lax.fori_loop(1, n, greet, 0)
        pl.semaphore_wait(barrier, n - 1)

        def transfer(i):
            return pltpu.make_async_remote_copy(
                src_ref=part,
                dst_ref=came.at[i],
                send_sem=sent.at[i],
                recv_sem=arrived.at[i],
                device_id={"dp": lax.rem(me + i, n)},
                device_id_type=pl.DeviceIdType.MESH,
            )

        lax.fori_loop(1, n, lambda i, _: (transfer(i).start(), 0)[1], 0)
        came[0] = part[...]
        lax.fori_loop(1, n, lambda i, _: (transfer(i).wait(), 0)[1], 0)
        out[...] = lax.fori_loop(0, n, lambda i, total: total + came[lax.rem(me - i + n, n)], jnp.zeros_like(part[...]))

    tile = pl.BlockSpec(memory_space=pltpu.VMEM)
    return call(
        body,
        1e6,
        1e6,
        pair_params(number),
        name="summed_over_group",
        in_specs=[tile],
        out_specs=tile,
        out_shape=jax.ShapeDtypeStruct(part.shape, F32),
        scratch_shapes=[pltpu.VMEM((n, *part.shape), F32), pltpu.SemaphoreType.DMA((n,)), pltpu.SemaphoreType.DMA((n,))],
    )(part)


def placed_columns(gathered):
    n, two, layers, rows, half = gathered.shape
    group = 8
    per = group // 2

    def body(t, gate, up):
        for i, out in enumerate((gate, up)):
            for k in range(group):
                out[k // 2 * rows : (k // 2 + 1) * rows, k % 2 * half : (k % 2 + 1) * half] = t[k, i]

    out = pl.BlockSpec((None, per * rows, 2 * half), lambda l, i: (l, i, 0))
    shape = jax.ShapeDtypeStruct((layers, n // 2 * rows, 2 * half), BF16)
    return call(
        body,
        1,
        4 * gathered.size,
        name="placed_columns",
        grid=(layers, n // group),
        in_specs=[pl.BlockSpec((group, two, None, rows, half), lambda l, i: (i, 0, l, 0, 0))],
        out_specs=[out, out],
        out_shape=(shape, shape),
    )(gathered)


def placed_rows(gathered):
    n, layers, rows, d = gathered.shape
    group = 8

    def body(t, out):
        for k in range(group):
            out[k * rows : (k + 1) * rows] = t[k]

    return call(
        body,
        1,
        4 * gathered.size,
        name="placed_rows",
        grid=(layers, n // group),
        in_specs=[pl.BlockSpec((group, None, rows, d), lambda l, i: (i, l, 0, 0))],
        out_specs=pl.BlockSpec((None, group * rows, d), lambda l, i: (l, i, 0)),
        out_shape=jax.ShapeDtypeStruct((layers, n * rows, d), BF16),
    )(gathered)


def adamw(w, m, v, g):
    m = 0.9 * m + 0.1 * g
    v = 0.95 * v + 0.05 * g * g
    step = m * lax.rsqrt(v + 1e-8) + 0.1 * w
    return (w - 0.02 * step).astype(BF16), m, v


def solution(mesh):
    size = mesh.shape["dp"]
    chips = size // 2
    same_core = [[2 * chip + core for chip in range(chips)] for core in range(2)]
    swap = [(i, i + 1 - 2 * (i % 2)) for i in range(size)]

    def summed(part):
        return lax.psum_scatter(part, "dp", scatter_dimension=0, axis_index_groups=same_core, tiled=True)

    def step(x, dy, w_gate, w_up, w_down, m_gate, m_up, m_down, v_gate, v_up, v_down):
        me = lax.axis_index("dp")
        core, chip = me % 2, me // 2
        x, dy = x[0], dy[0]
        layers, d, ff = w_gate.shape
        own_half = ff // 2

        def to_halves(t):
            mine = lax.dynamic_slice_in_dim(t, core * own_half, own_half, 2)
            theirs = lax.ppermute(lax.dynamic_slice_in_dim(t, (1 - core) * own_half, own_half, 2), "dp", swap)
            return jnp.where(core == 0, jnp.concatenate([mine, theirs], 1), jnp.concatenate([theirs, mine], 1))

        def from_halves(t):
            rows = t.shape[1] // 2
            mine = lax.dynamic_slice_in_dim(t, core * rows, rows, 1)
            theirs = lax.ppermute(lax.dynamic_slice_in_dim(t, (1 - core) * rows, rows, 1), "dp", swap)
            return jnp.where(core == 0, jnp.concatenate([mine, theirs], 2), jnp.concatenate([theirs, mine], 2))

        m_gate, m_up, v_gate, v_up = (to_halves(t) for t in (m_gate, m_up, v_gate, v_up))

        a0, a0_t = normed(x)
        gate, up, hid0 = hidden_forward(0, a0, w_gate, w_up)
        h1, a1, a1_t = down_forward(0, x, hid0, w_down)
        hid1, dg1, du1 = last_layer(1, a1, dy, w_gate, w_up, w_down)
        steps = ff // (2 * PART)
        gate_up1 = gate_up_gradient(1, 0, steps, a1_t, dg1, du1)
        hid1, gate_up1 = lax.optimization_barrier((hid1, gate_up1))
        down = down_gradient(2, hid1, dy, layers, 1)
        dg1, du1, down = lax.optimization_barrier((dg1, du1, down))
        gate_up1 = summed(gate_up1)
        dh = states_cotangent(1, h1, dy, dg1, du1, w_gate, w_up)
        down_made = down_gradient(3, hid0, dh, layers, 0, down)
        down = summed(down_made)
        down0, down1 = (down[:, i * d : (i + 1) * d] for i in range(layers))
        dh, down_made = lax.optimization_barrier((dh, down_made))
        gate0, up0 = first_layer_gradient(4, 0, a0_t, dh, gate, up, w_down)

        gate_up1 = gate_up1.reshape(gate_up1.shape[0], steps, 2, PART)
        gate1, up1 = (gate_up1[:, :, i].reshape(gate_up1.shape[0], own_half) for i in range(2))
        gradients = [jnp.stack(pair).astype(F32) for pair in ((gate0, gate1), (up0, up1), (down0, down1))]
        part = sum(jnp.sum(g * g) for g in gradients)
        total = summed_over_group(5, jnp.full((8, 128), part, F32))[0, 0]
        count = 3 * layers * d * ff
        factor = jnp.minimum(1.0, 0.5 * lax.rsqrt(total / count + 1e-30))

        rows = d // chips
        blocks = [
            lax.dynamic_slice(w, (0, chip * rows, core * own_half), (layers, rows, own_half)) for w in (w_gate, w_up)
        ] + [lax.dynamic_slice_in_dim(w_down, me * (ff // size), ff // size, 1)]
        new = [
            adamw(w.astype(F32), m, v, g * factor)
            for w, m, v, g in zip(blocks, (m_gate, m_up, m_down), (v_gate, v_up, v_down), gradients, strict=True)
        ]
        gate_up = lax.all_gather(jnp.stack([new[0][0], new[1][0]]), "dp")
        gate_up, new_down = lax.optimization_barrier((gate_up, new[2][0]))
        weights = [*placed_columns(gate_up), placed_rows(lax.all_gather(new_down, "dp"))]
        moments = [[from_halves(one[k]) for one in new[:2]] + [new[2][k]] for k in (1, 2)]
        return (*weights, *moments[0], *moments[1])

    sequences = P(("rep", "dp"))
    return jax.shard_map(
        step,
        mesh=mesh,
        in_specs=(sequences, sequences, P(), P(), P(), *[P(None, "dp")] * 6),
        out_specs=(P("rep"), P("rep"), P("rep"), *[P("rep", "dp")] * 6),
        check_vma=False,
    )
```

```python
import functools
import math

import jax
import jax.numpy as jnp
from jax import lax
from jax.experimental import pallas as pl
from jax.experimental.pallas import tpu as pltpu
from jax.sharding import PartitionSpec as P

F32, BF16 = jnp.float32, jnp.bfloat16
VMEM_LIMIT = 67_043_328
NN = (((1,), (0,)), ((), ()))
NT = (((1,), (1,)), ((), ()))
TN = (((0,), (0,)), ((), ()))


def dot(a, b, dims=NN):
    return lax.dot_general(a, b, dims, preferred_element_type=F32)


def sigmoid(x):
    return 1.0 / (1.0 + jnp.exp(-x))


def whole(shape):
    return pl.BlockSpec(shape, lambda *_: (0,) * len(shape), pipeline_mode=pl.Buffered(1))


def call(body, flops, moved, params=None, **kw):
    return pl.pallas_call(
        body,
        cost_estimate=pl.CostEstimate(flops=int(flops), bytes_accessed=int(moved), transcendentals=0),
        compiler_params=pltpu.CompilerParams(**{"vmem_limit_bytes": VMEM_LIMIT, **(params or {})}),
        **kw,
    )


def row_scale(wide):
    return lax.rsqrt(jnp.mean(wide * wide, -1, keepdims=True) + 1e-6)


def normed(x):
    tokens, d = x.shape
    bm = 512

    def body(x, a, a_t):
        wide = x[...].astype(F32)
        unit = wide * row_scale(wide)
        a[...] = unit.astype(BF16)
        a_t[...] = unit.T.astype(BF16)

    return call(
        body,
        10 * tokens * d,
        6 * tokens * d,
        name="normed",
        grid=(tokens // bm,),
        in_specs=[pl.BlockSpec((bm, d), lambda i: (i, 0))],
        out_specs=[pl.BlockSpec((bm, d), lambda i: (i, 0)), pl.BlockSpec((d, bm), lambda i: (0, i))],
        out_shape=(jax.ShapeDtypeStruct((tokens, d), BF16), jax.ShapeDtypeStruct((d, tokens), BF16)),
    )(x)


def hidden_forward(layer, a, w_gate, w_up):
    tokens, d = a.shape
    ff = w_gate.shape[-1]
    bf, bm = 256, 512

    def body(a, wg, wu, gate, up, hid):
        for i in range(tokens // bm):
            r = slice(i * bm, (i + 1) * bm)
            g, u = dot(a[r, :], wg[...]), dot(a[r, :], wu[...])
            gate[r, :] = g
            up[r, :] = u
            hid[r, :] = (g * sigmoid(g) * u).astype(BF16)

    w_spec = pl.BlockSpec((None, d, bf), lambda j: (layer, 0, j))
    o_spec = pl.BlockSpec((tokens, bf), lambda j: (0, j))
    wide = jax.ShapeDtypeStruct((tokens, ff), F32)
    return call(
        body,
        4 * tokens * d * ff,
        10 * tokens * ff + 4 * d * ff,
        name="hidden_forward",
        grid=(ff // bf,),
        in_specs=[whole((tokens, d)), w_spec, w_spec],
        out_specs=[o_spec] * 3,
        out_shape=(wide, wide, jax.ShapeDtypeStruct((tokens, ff), BF16)),
    )(a, w_gate, w_up)


def down_forward(layer, x, hid, w_down):
    tokens, ff = hid.shape
    d = x.shape[-1]
    bm = 256

    def body(x, hid, wd, h1, a1, a1_t):
        h = (x[...].astype(F32) + dot(hid[...], wd[...]).astype(BF16).astype(F32)).astype(BF16)
        h1[...] = h
        wide = h.astype(F32)
        unit = wide * row_scale(wide)
        a1[...] = unit.astype(BF16)
        a1_t[...] = unit.T.astype(BF16)

    rows = pl.BlockSpec((bm, d), lambda i: (i, 0))
    out = jax.ShapeDtypeStruct((tokens, d), BF16)
    return call(
        body,
        2 * tokens * d * ff,
        2 * tokens * ff + 2 * d * ff,
        name="down_forward",
        grid=(tokens // bm,),
        in_specs=[
            rows,
            pl.BlockSpec((bm, ff), lambda i: (i, 0)),
            pl.BlockSpec((None, ff, d), lambda i: (layer, 0, 0), pipeline_mode=pl.Buffered(1)),
        ],
        out_specs=[rows, rows, pl.BlockSpec((d, bm), lambda i: (0, i))],
        out_shape=(out, out, jax.ShapeDtypeStruct((d, tokens), BF16)),
    )(x, hid, w_down)


def gate_up_cotangents(g, u, dh):
    dh = dh.astype(BF16).astype(F32)
    s = sigmoid(g)
    silu = g * s
    return (dh * u * (s + silu * (1.0 - s))).astype(BF16), (dh * silu).astype(BF16), (silu * u).astype(BF16)


def last_layer(layer, a, dy, w_gate, w_up, w_down):
    tokens, d = a.shape
    ff = w_gate.shape[-1]
    bf, bm = 256, 512

    def body(a, dy, wg, wu, wd, hid, dg, du):
        for i in range(tokens // bm):
            r = slice(i * bm, (i + 1) * bm)
            g, u = dot(a[r, :], wg[...]), dot(a[r, :], wu[...])
            dg[r, :], du[r, :], hid[r, :] = gate_up_cotangents(g, u, dot(dy[r, :], wd[...], NT))

    w_spec = pl.BlockSpec((None, d, bf), lambda j: (layer, 0, j))
    o_spec = pl.BlockSpec((tokens, bf), lambda j: (0, j))
    out = jax.ShapeDtypeStruct((tokens, ff), BF16)
    return call(
        body,
        6 * tokens * d * ff,
        6 * tokens * ff + 6 * d * ff,
        name="last_layer",
        grid=(ff // bf,),
        in_specs=[whole((tokens, d)), whole((tokens, d)), w_spec, w_spec, pl.BlockSpec((None, bf, d), lambda j: (layer, j, 0))],
        out_specs=[o_spec] * 3,
        out_shape=(out, out, out),
    )(a, dy, w_gate, w_up, w_down)


def states_cotangent(layer, h, dy, dg, du, w_gate, w_up):
    tokens, ff = dg.shape
    d = h.shape[-1]
    bf, bm, be = 512, 1024, 256
    n = ff // bf

    def body(h, dy, dg, du, wg, wu, out, total):
        j = pl.program_id(0)

        @pl.when(j == 0)
        def _():
            total[...] = jnp.zeros_like(total)

        for i in range(tokens // bm):
            r = slice(i * bm, (i + 1) * bm)
            total[r, :] += dot(dg[r, :], wg[...], NT) + dot(du[r, :], wu[...], NT)

        @pl.when(j == n - 1)
        def _():
            def rows(i, _):
                r = pl.ds(pl.multiple_of(i * be, be), be)
                wide = h[r, :].astype(F32)
                da = total[r, :].astype(BF16).astype(F32)
                s = row_scale(wide)
                back = da * s - wide * (s * s * s * jnp.mean(da * wide, -1, keepdims=True))
                out[r, :] = (dy[r, :].astype(F32) + back).astype(BF16)
                return 0

            lax.fori_loop(0, tokens // be, rows, 0)

    w_spec = pl.BlockSpec((None, d, bf), lambda j: (layer, 0, j))
    t_spec = pl.BlockSpec((tokens, bf), lambda j: (0, j))
    return call(
        body,
        4 * tokens * d * ff,
        4 * tokens * ff + 4 * d * ff,
        name="states_cotangent",
        grid=(n,),
        in_specs=[whole((tokens, d)), whole((tokens, d)), t_spec, t_spec, w_spec, w_spec],
        out_specs=whole((tokens, d)),
        out_shape=jax.ShapeDtypeStruct((tokens, d), BF16),
        scratch_shapes=[pltpu.VMEM((tokens, d), F32)],
    )(h, dy, dg, du, w_gate, w_up)


SLOTS, ARRIVALS = 3, 4


def pair_scratch(rows, columns):
    return [
        pltpu.VMEM((SLOTS, 2, rows, columns), BF16),
        pltpu.VMEM((ARRIVALS, rows, columns), BF16),
        pltpu.SemaphoreType.DMA((SLOTS,)),
        pltpu.SemaphoreType.DMA((ARRIVALS,)),
    ]


def pair_step(n, make, out, made, came, sent, arrived):
    j = pl.program_id(0)
    me = lax.axis_index("dp")
    core = lax.rem(me, 2)
    other = me + 1 - 2 * core

    def transfer(step):
        slot, place = lax.rem(step, SLOTS), lax.rem(step, ARRIVALS)
        return pltpu.make_async_remote_copy(
            src_ref=made.at[slot, 1 - core],
            dst_ref=came.at[place],
            send_sem=sent.at[slot],
            recv_sem=arrived.at[place],
            device_id={"dp": other},
            device_id_type=pl.DeviceIdType.MESH,
        )

    @pl.when(j == 0)
    def _():
        barrier = pltpu.get_barrier_semaphore()
        pl.semaphore_signal(barrier, inc=1, device_id={"dp": other}, device_id_type=pl.DeviceIdType.MESH)
        pl.semaphore_wait(barrier, 1)

    @pl.when(j >= 2)
    def _():
        transfer(j - 2).wait()
        own = made[lax.rem(j - 2, SLOTS), core]
        out[...] = (own.astype(F32) + came[lax.rem(j - 2, ARRIVALS)].astype(F32)).astype(BF16)

    @pl.when(j < n)
    def _():
        make(made.at[lax.rem(j, SLOTS)])
        transfer(j).start()


def pair_params(number):
    return {"collective_id": number, "has_side_effects": True}


def down_gradient(number, hid, dy):
    tokens, ff = hid.shape
    d = dy.shape[-1]
    chips = lax.axis_size("dp") // 2
    own = ff // (2 * chips)
    bf = 1152
    n, per = ff // bf, bf // (2 * own)

    def body(hid, dy, out, *scratch):
        def make(slot):
            block = dot(hid[...], dy[...], TN)
            for i in range(per):
                for half in range(2):
                    at = (2 * i + half) * own
                    slot[half, i * own : (i + 1) * own, :] = block[at : at + own].astype(BF16)

        pair_step(n, make, out, *scratch)

    return call(
        body,
        2 * tokens * d * ff,
        2 * tokens * ff + d * ff,
        pair_params(number),
        name=f"down_gradient_{number}",
        grid=(n + 2,),
        in_specs=[pl.BlockSpec((tokens, bf), lambda j: (0, jnp.minimum(j, n - 1))), whole((tokens, d))],
        out_specs=pl.BlockSpec((bf // 2, d), lambda j: (jnp.maximum(j - 2, 0), 0)),
        out_shape=jax.ShapeDtypeStruct((ff // 2, d), BF16),
        scratch_shapes=pair_scratch(bf // 2, d),
    )(hid, dy)


PART = 256


def halves_specs(shape, first, n, half, layer=None, transposed=False):
    def spec(h):
        def at(j):
            k = h * half + first + jnp.minimum(j, n - 1)
            index = (k, 0) if transposed else (0, k)
            return index if layer is None else (layer, *index)

        return pl.BlockSpec(shape, at)

    return [spec(0), spec(1)]


def gate_up_gradient(number, first, n, a_t, dg, du):
    d, tokens = a_t.shape
    half = dg.shape[-1] // (2 * PART)

    def body(a_t, dg0, dg1, du0, du1, out, *scratch):
        def make(slot):
            for h, (dg, du) in enumerate(((dg0, du0), (dg1, du1))):
                slot[h, :, :PART] = dot(a_t[...], dg[...]).astype(BF16)
                slot[h, :, PART:] = dot(a_t[...], du[...]).astype(BF16)

        pair_step(n, make, out, *scratch)

    t_specs = halves_specs((tokens, PART), first, n, half)
    return call(
        body,
        8 * tokens * d * PART * n,
        8 * tokens * PART * n,
        pair_params(number),
        name=f"gate_up_gradient_{number}",
        grid=(n + 2,),
        in_specs=[whole((d, tokens)), *t_specs, *t_specs],
        out_specs=pl.BlockSpec((d, 2 * PART), lambda j: (0, jnp.maximum(j - 2, 0))),
        out_shape=jax.ShapeDtypeStruct((d, 2 * PART * n), BF16),
        scratch_shapes=pair_scratch(d, 2 * PART),
    )(a_t, dg, dg, du, du)


SIDE = 4
PLACES = 4


def first_layer_gradient(number, layer, a_t, dy, gate, up, w_down):
    d, tokens = a_t.shape
    half = gate.shape[-1] // (2 * PART)
    n = half
    bm = 512
    rows = d // SIDE**2
    mid = PART // 2

    def body(a_t, dy, g0, g1, u0, u1, w0, w1, out, dg, du, made, came, sums, across1, pass1, got1, total1, across2, pass2, got2, ps, pr, sent, arrived):
        j = pl.program_id(0)
        me = lax.axis_index("dp")
        core = lax.rem(me, 2)
        other = me + 1 - 2 * core
        x, y = lax.div(me, 2 * SIDE), lax.rem(lax.div(me, 2), SIDE)

        def at(x, y):
            return {"dp": (x * SIDE + y) * 2 + core}

        def beside(axis, way):
            to = lax.rem((x if axis == 0 else y) + (1 if way == 0 else SIDE - 1), SIDE)
            return at(to, y) if axis == 0 else at(x, to)

        here = (x, y)

        def transfer(stage, color, way, block):
            place, slot = lax.rem(block, PLACES), lax.rem(block, SLOTS)
            first, second = color, 1 - color
            columns = slice(color * PART, (color + 1) * PART)
            if stage == 1:
                far = lax.rem(here[first] + 2, SIDE)
                part = slice(2 * way, 2 * way + 2)
                src = sums.at[slot, far, part, :, columns] if color == 0 else sums.at[slot, part, far, :, columns]
                dst = across1.at[color, place, way]
            elif stage == 2:
                src, dst = pass1.at[color, place, way], got1.at[color, place, way]
            elif stage == 3:
                far = lax.rem(here[second] + 2, SIDE)
                src = total1.at[color, place, far, :, slice(way * mid, (way + 1) * mid)]
                dst = across2.at[color, place, way]
            else:
                src, dst = pass2.at[color, place, way], got2.at[color, place, way]
            index = ((stage - 1) * 2 + color) * 2 + way
            return pltpu.make_async_remote_copy(
                src_ref=src,
                dst_ref=dst,
                send_sem=sent.at[index, place],
                recv_sem=arrived.at[index, place],
                device_id=beside(first if stage <= 2 else second, way),
                device_id_type=pl.DeviceIdType.MESH,
            )

        def swap(block):
            slot, place = lax.rem(block, SLOTS), lax.rem(block, PLACES)
            return pltpu.make_async_remote_copy(
                src_ref=made.at[slot, 1 - core],
                dst_ref=came.at[place],
                send_sem=ps.at[slot],
                recv_sem=pr.at[place],
                device_id={"dp": other},
                device_id_type=pl.DeviceIdType.MESH,
            )

        def of(color, slot, i):
            columns = slice(color * PART, (color + 1) * PART)
            t = sums[slot, i, :, :, columns] if color == 0 else sums[slot, :, i, :, columns]
            return t.astype(F32)

        def stage(lag, act):
            @pl.when((j >= lag) & (j < n + lag))
            def _():
                act(j - lag)

        @pl.when(j == 0)
        def _():
            barrier = pltpu.get_barrier_semaphore()
            for peer in ({"dp": other}, beside(0, 0), beside(0, 1), beside(1, 0), beside(1, 1)):
                pl.semaphore_signal(barrier, inc=1, device_id=peer, device_id_type=pl.DeviceIdType.MESH)
            pl.semaphore_wait(barrier, 5)

        def last(block):
            place = lax.rem(block, PLACES)
            for color in range(2):
                for way in range(2):
                    transfer(4, color, way, block).wait()
                b = here[1 - color]
                t = total1[color, place, b].astype(F32) + got2[color, place, 0].astype(F32) + got2[color, place, 1].astype(F32)
                out[color] = t.astype(BF16)

        def fourth(block):
            place = lax.rem(block, PLACES)
            for color in range(2):
                for way in range(2):
                    transfer(3, color, way, block).wait()
                for way in range(2):
                    b = lax.rem(here[1 - color] + (1 if way == 0 else SIDE - 1), SIDE)
                    pass2[color, place, way] = total1[color, place, b]
                    c = slice(way * mid, (way + 1) * mid)
                    more = total1[color, place, b, :, c].astype(F32) + across2[color, place, way].astype(F32)
                    pass2[color, place, way, :, c] = more.astype(BF16)
                    transfer(4, color, way, block).start()

        def third(block):
            place, slot = lax.rem(block, PLACES), lax.rem(block, SLOTS)
            for color in range(2):
                for way in range(2):
                    transfer(2, color, way, block).wait()
                t = of(color, slot, here[color]) + got1[color, place, 0].astype(F32) + got1[color, place, 1].astype(F32)
                total1[color, place] = t.astype(BF16)
                for way in range(2):
                    transfer(3, color, way, block).start()

        def second(block):
            place, slot = lax.rem(block, PLACES), lax.rem(block, SLOTS)
            for color in range(2):
                for way in range(2):
                    transfer(1, color, way, block).wait()
                for way in range(2):
                    t = of(color, slot, lax.rem(here[color] + (1 if way == 0 else SIDE - 1), SIDE))
                    p = slice(2 * way, 2 * way + 2)
                    q = slice(2 - 2 * way, 4 - 2 * way)
                    pass1[color, place, way, p] = (t[p] + across1[color, place, way].astype(F32)).astype(BF16)
                    pass1[color, place, way, q] = t[q].astype(BF16)
                    transfer(2, color, way, block).start()

        def first(block):
            place, slot = lax.rem(block, PLACES), lax.rem(block, SLOTS)
            swap(block).wait()
            for k in range(SIDE**2):
                r = slice(k * rows, (k + 1) * rows)
                t = made[slot, core, r, :].astype(F32) + came[place, r, :].astype(F32)
                sums[slot, k // SIDE, k % SIDE] = t.astype(BF16)
            for color in range(2):
                for way in range(2):
                    transfer(1, color, way, block).start()

        def make(block):
            slot = lax.rem(block, SLOTS)
            for h, (g, u, w) in enumerate(((g0, u0, w0), (g1, u1, w1))):
                for i in range(tokens // bm):
                    r = slice(i * bm, (i + 1) * bm)
                    dg[h, r, :], du[h, r, :], _ = gate_up_cotangents(g[r, :], u[r, :], dot(dy[r, :], w[...], NT))
                made[slot, h, :, :PART] = dot(a_t[...], dg[h]).astype(BF16)
                made[slot, h, :, PART:] = dot(a_t[...], du[h]).astype(BF16)
            swap(block).start()

        stage(6, last)
        stage(5, fourth)
        stage(4, third)
        stage(3, second)
        stage(2, first)
        stage(0, make)

    t_specs = halves_specs((tokens, PART), 0, n, half)
    block = (SIDE, rows, PART)
    return call(
        body,
        12 * tokens * d * PART * n,
        16 * tokens * PART * n,
        pair_params(number),
        name="first_layer_gradient",
        grid=(n + 6,),
        in_specs=[whole((d, tokens)), whole((tokens, d)), *t_specs, *t_specs, *halves_specs((None, PART, d), 0, n, half, layer, True)],
        out_specs=pl.BlockSpec((2, rows, PART), lambda j: (0, 0, jnp.maximum(j - 6, 0))),
        out_shape=jax.ShapeDtypeStruct((2, rows, PART * n), BF16),
        scratch_shapes=[
            pltpu.VMEM((2, tokens, PART), BF16),
            pltpu.VMEM((2, tokens, PART), BF16),
            pltpu.VMEM((SLOTS, 2, d, 2 * PART), BF16),
            pltpu.VMEM((PLACES, d, 2 * PART), BF16),
            pltpu.VMEM((SLOTS, SIDE, SIDE, rows, 2 * PART), BF16),
            pltpu.VMEM((2, PLACES, 2, SIDE // 2, rows, PART), BF16),
            pltpu.VMEM((2, PLACES, 2, *block), BF16),
            pltpu.VMEM((2, PLACES, 2, *block), BF16),
            pltpu.VMEM((2, PLACES, *block), BF16),
            pltpu.VMEM((2, PLACES, 2, rows, mid), BF16),
            pltpu.VMEM((2, PLACES, 2, rows, PART), BF16),
            pltpu.VMEM((2, PLACES, 2, rows, PART), BF16),
            pltpu.SemaphoreType.DMA((SLOTS,)),
            pltpu.SemaphoreType.DMA((PLACES,)),
            pltpu.SemaphoreType.DMA((16, PLACES)),
            pltpu.SemaphoreType.DMA((16, PLACES)),
        ],
    )(a_t, dy, gate, gate, up, up, w_down, w_down)


def updated_and_gathered(number, gate_up0, gate_up1, down0, down1, w_gate, w_up, w_down, m_gate, m_up, m_down, v_gate, v_up, v_down):
    n = lax.axis_size("dp")
    layers, d, ff = w_gate.shape
    rows, half = gate_up0.shape[1:]
    own_rows, moment_rows = ff // n, d // n
    steps = half // PART
    width = 2 * half + d
    cut = -(-width // 256) * 128
    count = 3 * layers * d * ff
    parts = (slice(0, cut), slice(cut, width))
    plan = []

    def body(gu0, gu1, d0, d1, wg, wu, wd, mg, mu, md, vg, vu, vd, ag, wd1, nmg, nmu, nmd, nvg, nvu, nvd,
             w_gu, w_d, mom, mom_d, packs, spare, tile, tiles, load, swap_s, swap_r, norm_s, norm_r, sent, arrived):
        me = lax.axis_index("dp")
        core = lax.rem(me, 2)
        other = me + 1 - 2 * core
        chip = lax.div(me, 2)
        x, y = lax.div(chip, SIDE), lax.rem(chip, SIDE)
        here = (x, y)
        mine, theirs = (pl.ds(pl.multiple_of(c * half, 128), half) for c in (core, 1 - core))

        moments = (mg, mu, vg, vu)
        new_moments = (nmg, nmu, nvg, nvu)
        loads = [
            *[(t.at[:, :, mine], mom.at[k, core]) for k, t in enumerate(moments)],
            (md, mom_d.at[0]),
            (vd, mom_d.at[1]),
            (wg.at[:, pl.ds(pl.multiple_of(chip * rows, 8), rows), mine], w_gu.at[0]),
            (wu.at[:, pl.ds(pl.multiple_of(chip * rows, 8), rows), mine], w_gu.at[1]),
            (wd.at[:, pl.ds(pl.multiple_of(me * own_rows, 16), own_rows), :], w_d),
        ]
        loads = [pltpu.make_async_copy(a, b, load.at[k]) for k, (a, b) in enumerate(loads)]
        for copy in loads:
            copy.start()

        barrier = pltpu.get_barrier_semaphore()

        def greet(i, _):
            pl.semaphore_signal(barrier, inc=1, device_id={"dp": lax.rem(me + i, n)}, device_id_type=pl.DeviceIdType.MESH)
            return 0

        lax.fori_loop(1, n, greet, 0)

        def square(t):
            t = t.astype(F32)
            t = t * t
            return sum(t[k * 8 : (k + 1) * 8] for k in range(t.shape[0] // 8))

        def squares(k, total):
            at = pl.ds(pl.multiple_of(k * PART, PART), PART)
            both = pl.ds(pl.multiple_of(k * 2 * PART, PART), 2 * PART)
            two = square(gu1[:, both])
            return total + square(gu0[0, :, at]) + square(gu0[1, :, at]) + two[:, :PART] + two[:, PART:]

        total = lax.fori_loop(0, steps, squares, jnp.zeros((8, PART), F32))
        downs = square(d0[...]) + square(d1[...])
        total = total[:, :128] + total[:, 128:] + sum(downs[:, k * 128 : (k + 1) * 128] for k in range(d // 128))
        tile[...] = total
        tiles[0] = total

        pl.semaphore_wait(barrier, n - 1)

        def swap(src, dst, k):
            return pltpu.make_async_remote_copy(
                src_ref=src, dst_ref=dst, send_sem=swap_s.at[k], recv_sem=swap_r.at[k], device_id={"dp": other}, device_id_type=pl.DeviceIdType.MESH
            )

        def size(i):
            return pltpu.make_async_remote_copy(
                src_ref=tile,
                dst_ref=tiles.at[i],
                send_sem=norm_s.at[i],
                recv_sem=norm_r.at[i],
                device_id={"dp": lax.rem(me + i, n)},
                device_id_type=pl.DeviceIdType.MESH,
            )

        lax.fori_loop(1, n, lambda i, _: (size(i).start(), 0)[1], 0)
        swaps = [swap(t.at[:, :, theirs], mom.at[k, core], k) for k, t in enumerate(moments)]
        for copy in swaps:
            copy.start()
        for copy in loads:
            copy.wait()
        for copy in swaps:
            copy.wait()
        lax.fori_loop(1, n, lambda i, _: (size(i).wait(), 0)[1], 0)
        total = lax.fori_loop(0, n, lambda i, total: total + tiles[lax.rem(me - i + n, n)], jnp.zeros((8, 128), F32))
        total = jnp.sum(jnp.sum(total, 0, keepdims=True), 1, keepdims=True)
        factor = jnp.minimum(1.0, 0.5 * lax.rsqrt(total / count + 1e-30))

        def adamw(w, m, v, g):
            g = g * factor
            m = 0.9 * m + 0.1 * g
            v = 0.95 * v + 0.05 * g * g
            return w - 0.02 * (m * lax.rsqrt(v + 1e-8) + 0.1 * w), m, v

        def step_gate_up(layer):
            for gu in range(2):

                def columns(k, _, gu=gu):
                    at = pl.ds(pl.multiple_of(k * PART, PART), PART)
                    if layer == 0:
                        g = gu0[gu, :, at]
                    else:
                        g = gu1[:, pl.ds(pl.multiple_of((2 * k + gu) * PART, PART), PART)]
                    g = g.astype(F32)
                    w = w_gu[gu, layer, :, at].astype(F32)
                    new = []
                    for r in range(2):
                        p = slice(r * moment_rows, (r + 1) * moment_rows)
                        one, m, v = adamw(w[p], mom[gu, r, layer, :, at], mom[2 + gu, r, layer, :, at], g[p])
                        mom[gu, r, layer, :, at] = m
                        mom[2 + gu, r, layer, :, at] = v
                        new.append(one)
                    packs[layer, :, pl.ds(pl.multiple_of(gu * half + k * PART, PART), PART)] = jnp.concatenate(new, 0).astype(BF16)
                    return 0

                lax.fori_loop(0, steps, columns, 0)

        def step_down(layer, p, g):
            new, m, v = adamw(w_d[layer, p, :].astype(F32), mom_d[0, layer, p, :], mom_d[1, layer, p, :], g[p, :].astype(F32))
            mom_d[0, layer, p, :] = m
            mom_d[1, layer, p, :] = v
            return new.astype(BF16)

        def place(color, i, k, whose, part):
            i, k = (lax.rem(t + SIDE, SIDE) for t in (i, k))
            a, b = (i, k) if color == 0 else (k, i)
            return ag.at[a, b, whose, color, :, parts[part]]

        def beside(axis, way):
            to = lax.rem(here[axis] + (1 if way == 0 else SIDE - 1), SIDE)
            a, b = (to, y) if axis == 0 else (x, to)
            return {"dp": (a * SIDE + b) * 2 + core}

        started = {}

        def send(name, color, o, q, part, to):
            index = len(plan) if name not in plan else plan.index(name)
            if name not in plan:
                plan.append(name)
            dst = place(color, here[color] + o, here[1 - color] + q, core, part)
            src = packs.at[color, :, parts[part]] if (o, q) == (0, 0) else dst
            copy = pltpu.make_async_remote_copy(
                src_ref=src, dst_ref=dst, send_sem=sent.at[index], recv_sem=arrived.at[index], device_id=to, device_id_type=pl.DeviceIdType.MESH
            )
            copy.start()
            started[name] = copy

        def along_first(color, way, part):
            send(("a", color, way, part), color, 0, 0, part, beside(color, way))

        def on_first(color, way):
            send(("b", color, way), color, -1 if way == 0 else 1, 0, way, beside(color, way))

        def along_second(color, o, part):
            for way in range(2):
                send(("c", color, way, o, part), color, o, 0, part, beside(1 - color, way))

        def on_second(color, way, o):
            send(("d", color, way, o), color, o, -1 if way == 0 else 1, way, beside(1 - color, way))

        def share(color, o, q, part):
            send(("e", color, o, q, part), color, o, q, part, {"dp": other})

        def own(color):
            for part in range(2):
                for way in range(2):
                    along_first(color, way, part)
            for part in range(2):
                along_second(color, 0, part)
                share(color, 0, 0, part)
            copy = pltpu.make_async_copy(packs.at[color], ag.at[x, y, core, color], load.at[color])
            copy.start()
            return copy

        step_gate_up(0)
        packs[0, :, 2 * half :] = step_down(0, slice(0, rows), d0)
        kept = [own(0)]
        step_gate_up(1)
        packs[1, :, 2 * half :] = step_down(0, slice(rows, 2 * rows), d0)
        kept.append(own(1))
        spare[...] = step_down(1, slice(0, own_rows), d1)

        stores = [
            *[(mom.at[k, core], t.at[:, :, mine]) for k, t in enumerate(new_moments)],
            (mom_d.at[0], nmd),
            (mom_d.at[1], nvd),
            (spare, wd1),
        ]
        stores = [pltpu.make_async_copy(a, b, load.at[2 + k]) for k, (a, b) in enumerate(stores)]
        backs = [swap(mom.at[k, 1 - core], t.at[:, :, mine], 4 + k) for k, t in enumerate(new_moments)]
        for copy in (*stores, *backs):
            copy.start()

        both = [(color, way) for color in range(2) for way in range(2)]
        for part in range(2):
            for color, way in both:
                started["a", color, way, part].wait_recv()
                if way == part:
                    on_first(color, way)
                o = -1 if way == 0 else 1
                along_second(color, o, part)
                share(color, o, 0, part)

        def arrivals(o):
            for part in range(2):
                for color, way in both:
                    started["c", color, way, o, part].wait_recv()
                    if way == part:
                        on_second(color, way, o)
                    share(color, o, -1 if way == 0 else 1, part)

        arrivals(0)
        for color, way in both:
            started["b", color, way].wait_recv()
            along_second(color, 2, way)
            share(color, 2, 0, way)
        for o in (-1, 1, 2):
            arrivals(o)
        for o in (0, -1, 1, 2):
            for color, way in both:
                started["d", color, way, o].wait_recv()
                share(color, o, 2, way)
        for name, copy in started.items():
            copy.wait_send()
            if name[0] == "e":
                copy.wait_recv()
        for copy in (*kept, *stores, *backs):
            copy.wait()

    anywhere = pl.BlockSpec(memory_space=pl.ANY)
    vmem = pl.BlockSpec(memory_space=pltpu.VMEM)
    return call(
        body,
        1e9,
        1e8,
        pair_params(number),
        name="updated_and_gathered",
        in_specs=[vmem] * 4 + [anywhere] * 9,
        out_specs=[anywhere] * 8,
        out_shape=[
            jax.ShapeDtypeStruct((SIDE, SIDE, 2, 2, rows, width), BF16),
            jax.ShapeDtypeStruct((own_rows, d), BF16),
            *[jax.ShapeDtypeStruct(t.shape, F32) for t in (m_gate, m_up, m_down, v_gate, v_up, v_down)],
        ],
        scratch_shapes=[
            pltpu.VMEM((2, layers, rows, half), BF16),
            pltpu.VMEM((layers, own_rows, d), BF16),
            pltpu.VMEM((4, 2, layers, moment_rows, half), F32),
            pltpu.VMEM((2, layers, own_rows, d), F32),
            pltpu.VMEM((2, rows, width), BF16),
            pltpu.VMEM((own_rows, d), BF16),
            pltpu.VMEM((8, 128), F32),
            pltpu.VMEM((n, 8, 128), F32),
            pltpu.SemaphoreType.DMA((9,)),
            pltpu.SemaphoreType.DMA((8,)),
            pltpu.SemaphoreType.DMA((8,)),
            pltpu.SemaphoreType.DMA((n,)),
            pltpu.SemaphoreType.DMA((n,)),
            pltpu.SemaphoreType.DMA((124,)),
            pltpu.SemaphoreType.DMA((124,)),
        ],
    )(gate_up0, gate_up1, down0, down1, w_gate, w_up, w_down, m_gate, m_up, m_down, v_gate, v_up, v_down)


def placed(packs, layers, d, ff):
    rows, width = packs.shape[-2:]
    half = ff // 2
    per = 2

    def body(t, gate, up, down):
        for b in range(per):
            for core in range(2):
                for color in range(2):
                    r = slice(b * rows, (b + 1) * rows)
                    c = slice(core * half, (core + 1) * half)
                    gate[color, r, c] = t[b, core, color, :, :half]
                    up[color, r, c] = t[b, core, color, :, half : 2 * half]
                    at = ((b * 2 + core) * 2 + color) * rows
                    down[at : at + rows, :] = t[b, core, color, :, 2 * half :]

    n = SIDE // per
    out = pl.BlockSpec((layers, per * rows, ff), lambda i, j: (0, i * n + j, 0))
    return call(
        body,
        1,
        4 * packs.size,
        name="placed",
        grid=(SIDE, n),
        in_specs=[pl.BlockSpec((None, per, 2, 2, rows, width), lambda i, j: (i, j, 0, 0, 0, 0))],
        out_specs=[out, out, pl.BlockSpec((None, per * 4 * rows, d), lambda i, j: (0, i * n + j, 0))],
        out_shape=[jax.ShapeDtypeStruct((layers, d, ff), BF16)] * 2 + [jax.ShapeDtypeStruct((layers, ff, d), BF16)],
    )(packs)


def copied(*arrays):
    def body(*refs):
        for a, b in zip(refs[: len(arrays)], refs[len(arrays) :], strict=True):
            b[...] = a[...]

    specs = [pl.BlockSpec((1, *t.shape[1:]), lambda i: (i, 0, 0)) for t in arrays]
    return call(
        body,
        1,
        sum(8 * t.size for t in arrays),
        name="copied",
        grid=(arrays[0].shape[0],),
        in_specs=specs,
        out_specs=specs,
        out_shape=[jax.ShapeDtypeStruct(t.shape, t.dtype) for t in arrays],
    )(*arrays)


def placed_last(down, gathered):
    layers, ff, d = down.shape
    bm = 1152

    def body(down, t, out):
        out[...] = t[...]

    return call(
        body,
        1,
        4 * gathered.size,
        name="placed_last",
        grid=(ff // bm,),
        in_specs=[pl.BlockSpec(memory_space=pl.ANY), pl.BlockSpec((bm, d), lambda i: (i, 0))],
        out_specs=pl.BlockSpec((None, bm, d), lambda i: (layers - 1, i, 0)),
        out_shape=jax.ShapeDtypeStruct(down.shape, BF16),
        input_output_aliases={0: 0},
    )(down, gathered)


def solution(mesh):
    chips = mesh.shape["dp"] // 2
    same_core = [[2 * chip + core for chip in range(chips)] for core in range(2)]

    def summed(part):
        return lax.psum_scatter(part, "dp", scatter_dimension=0, axis_index_groups=same_core, tiled=True)

    def step(x, dy, w_gate, w_up, w_down, *moments):
        x, dy = x[0], dy[0]
        layers, d, ff = w_gate.shape

        a0, a0_t = normed(x)
        gate, up, hid0 = hidden_forward(0, a0, w_gate, w_up)
        h1, a1, a1_t = down_forward(0, x, hid0, w_down)
        hid1, dg1, du1 = last_layer(1, a1, dy, w_gate, w_up, w_down)
        down1 = down_gradient(1, hid1, dy)
        dg1, du1, down1 = lax.optimization_barrier((dg1, du1, down1))
        down1 = summed(down1)
        gate_up1 = gate_up_gradient(2, 0, ff // (2 * PART), a1_t, dg1, du1)
        dg1, du1, gate_up1 = lax.optimization_barrier((dg1, du1, gate_up1))
        gate_up1 = summed(gate_up1)
        dh = states_cotangent(1, h1, dy, dg1, du1, w_gate, w_up)
        down1, dh = lax.optimization_barrier((down1, dh))
        down0 = down_gradient(3, hid0, dh)
        gate_up1, dh, down0 = lax.optimization_barrier((gate_up1, dh, down0))
        down0 = summed(down0)
        gate_up0 = first_layer_gradient(4, 0, a0_t, dh, gate, up, w_down)
        packs, last, *moments = updated_and_gathered(5, gate_up0, gate_up1, down0, down1, w_gate, w_up, w_down, *moments)
        last = lax.all_gather(last, "dp", tiled=True)
        new_gate, new_up, new_down = placed(packs, layers, d, ff)
        moments[2], moments[5] = copied(moments[2], moments[5])
        new_down = placed_last(new_down, last)
        return new_gate, new_up, new_down, *moments

    sequences = P(("rep", "dp"))
    return jax.shard_map(
        step,
        mesh=mesh,
        in_specs=(sequences, sequences, P(), P(), P(), *[P(None, "dp")] * 6),
        out_specs=(P("rep"), P("rep"), P("rep"), *[P("rep", "dp")] * 6),
        check_vma=False,
    )
```

```python
import functools
import math

import jax
import jax.numpy as jnp
from jax import lax
from jax.experimental import pallas as pl
from jax.experimental.pallas import tpu as pltpu
from jax.sharding import PartitionSpec as P

F32, BF16 = jnp.float32, jnp.bfloat16
VMEM_LIMIT = 67_043_328
NN = (((1,), (0,)), ((), ()))
NT = (((1,), (1,)), ((), ()))
TN = (((0,), (0,)), ((), ()))


def dot(a, b, dims=NN):
    return lax.dot_general(a, b, dims, preferred_element_type=F32)


def sigmoid(x):
    return 1.0 / (1.0 + jnp.exp(-x))


def whole(shape):
    return pl.BlockSpec(shape, lambda *_: (0,) * len(shape), pipeline_mode=pl.Buffered(1))


def call(body, flops, moved, params=None, **kw):
    return pl.pallas_call(
        body,
        cost_estimate=pl.CostEstimate(flops=int(flops), bytes_accessed=int(moved), transcendentals=0),
        compiler_params=pltpu.CompilerParams(**{"vmem_limit_bytes": VMEM_LIMIT, **(params or {})}),
        **kw,
    )


def row_scale(wide):
    return lax.rsqrt(jnp.mean(wide * wide, -1, keepdims=True) + 1e-6)


def hidden_forward(layer, x, w_gate, w_up):
    tokens, d = x.shape
    ff = w_gate.shape[-1]
    bf, bm = 256, 512
    n = tokens // bm

    def body(x, wg, wu, gate, up, hid, a_t, x_in, a, came):
        j = pl.program_id(0)

        def rows(i):
            return pl.ds(pl.multiple_of(i * bm, bm), bm)

        def come(i):
            return pltpu.make_async_copy(x.at[rows(i)], x_in.at[rows(i)], came.at[i])

        def chunk(r):
            g, u = dot(a[r, :], wg[...]), dot(a[r, :], wu[...])
            gate[r, :] = g
            up[r, :] = u
            hid[r, :] = (g * sigmoid(g) * u).astype(BF16)

        @pl.when(j == 0)
        def _():
            for i in range(n):
                come(i).start()

            def first(i, _):
                come(i).wait()
                wide = x_in[rows(i), :].astype(F32)
                a[rows(i), :] = (wide * row_scale(wide)).astype(BF16)
                chunk(rows(i))
                return 0

            lax.fori_loop(0, n, first, 0)

        @pl.when(j > 0)
        def _():
            for i in range(n):
                chunk(slice(i * bm, (i + 1) * bm))

        @pl.when(j == 1)
        def _():
            a_t[...] = a[...].T

    w_spec = pl.BlockSpec((None, d, bf), lambda j: (layer, 0, j))
    o_spec = pl.BlockSpec((tokens, bf), lambda j: (0, j))
    wide = jax.ShapeDtypeStruct((tokens, ff), F32)
    return call(
        body,
        4 * tokens * d * ff,
        10 * tokens * ff + 4 * d * ff,
        name="hidden_forward",
        grid=(ff // bf,),
        in_specs=[pl.BlockSpec(memory_space=pl.ANY), w_spec, w_spec],
        out_specs=[*[o_spec] * 3, whole((d, tokens))],
        out_shape=(wide, wide, jax.ShapeDtypeStruct((tokens, ff), BF16), jax.ShapeDtypeStruct((d, tokens), BF16)),
        scratch_shapes=[pltpu.VMEM((tokens, d), BF16), pltpu.VMEM((tokens, d), BF16), pltpu.SemaphoreType.DMA((n,))],
    )(x, w_gate, w_up)


def down_forward(layer, x, hid, w_down):
    tokens, ff = hid.shape
    d = x.shape[-1]
    bm = 256

    def body(x, hid, wd, h1, a1, a1_t):
        h = (x[...].astype(F32) + dot(hid[...], wd[...]).astype(BF16).astype(F32)).astype(BF16)
        h1[...] = h
        wide = h.astype(F32)
        unit = wide * row_scale(wide)
        a1[...] = unit.astype(BF16)
        a1_t[...] = unit.T.astype(BF16)

    rows = pl.BlockSpec((bm, d), lambda i: (i, 0))
    out = jax.ShapeDtypeStruct((tokens, d), BF16)
    return call(
        body,
        2 * tokens * d * ff,
        2 * tokens * ff + 2 * d * ff,
        name="down_forward",
        grid=(tokens // bm,),
        in_specs=[
            rows,
            pl.BlockSpec((bm, ff), lambda i: (i, 0)),
            pl.BlockSpec((None, ff, d), lambda i: (layer, 0, 0), pipeline_mode=pl.Buffered(1)),
        ],
        out_specs=[rows, rows, pl.BlockSpec((d, bm), lambda i: (0, i))],
        out_shape=(out, out, jax.ShapeDtypeStruct((d, tokens), BF16)),
    )(x, hid, w_down)


def gate_up_cotangents(g, u, dh):
    dh = dh.astype(BF16).astype(F32)
    s = sigmoid(g)
    silu = g * s
    return (dh * u * (s + silu * (1.0 - s))).astype(BF16), (dh * silu).astype(BF16), (silu * u).astype(BF16)


def last_layer(layer, a, dy, w_gate, w_up, w_down):
    tokens, d = a.shape
    ff = w_gate.shape[-1]
    bf, bm = 256, 512

    def body(a, dy, wg, wu, wd, hid, dg, du):
        for i in range(tokens // bm):
            r = slice(i * bm, (i + 1) * bm)
            g, u = dot(a[r, :], wg[...]), dot(a[r, :], wu[...])
            dg[r, :], du[r, :], hid[r, :] = gate_up_cotangents(g, u, dot(dy[r, :], wd[...], NT))

    w_spec = pl.BlockSpec((None, d, bf), lambda j: (layer, 0, j))
    o_spec = pl.BlockSpec((tokens, bf), lambda j: (0, j))
    out = jax.ShapeDtypeStruct((tokens, ff), BF16)
    return call(
        body,
        6 * tokens * d * ff,
        6 * tokens * ff + 6 * d * ff,
        name="last_layer",
        grid=(ff // bf,),
        in_specs=[whole((tokens, d)), whole((tokens, d)), w_spec, w_spec, pl.BlockSpec((None, bf, d), lambda j: (layer, j, 0))],
        out_specs=[o_spec] * 3,
        out_shape=(out, out, out),
    )(a, dy, w_gate, w_up, w_down)


def states_cotangent(layer, h, dy, dg, du, w_gate, w_up):
    tokens, ff = dg.shape
    d = h.shape[-1]
    bm, bk = 256, 512
    n = ff // bk

    def body(h, dy, dg, du, wg, wu, out, w, total, came):
        def k(c):
            return pl.ds(pl.multiple_of(c * bk, bk), bk)

        def come(c):
            return [pltpu.make_async_copy(t.at[layer, :, k(c)], w.at[i, :, k(c)], came.at[i, c]) for i, t in enumerate((wg, wu))]

        def rest(da):
            wide = h[...].astype(F32)
            da = da.astype(BF16).astype(F32)
            s = row_scale(wide)
            back = da * s - wide * (s * s * s * jnp.mean(da * wide, -1, keepdims=True))
            out[...] = (dy[...].astype(F32) + back).astype(BF16)

        @pl.when(pl.program_id(0) == 0)
        def _():
            for c in range(n):
                for copy in come(c):
                    copy.start()
            total[...] = jnp.zeros_like(total)

            def add(c, _):
                for copy in come(c):
                    copy.wait()
                total[...] += dot(dg[:, k(c)], w[0, :, k(c)], NT) + dot(du[:, k(c)], w[1, :, k(c)], NT)
                return 0

            lax.fori_loop(0, n, add, 0)
            rest(total[...])

        @pl.when(pl.program_id(0) > 0)
        def _():
            rest(dot(dg[...], w[0], NT) + dot(du[...], w[1], NT))

    rows = pl.BlockSpec((bm, d), lambda i: (i, 0))
    wide_rows = pl.BlockSpec((bm, ff), lambda i: (i, 0))
    anywhere = pl.BlockSpec(memory_space=pl.ANY)
    return call(
        body,
        4 * tokens * d * ff,
        4 * tokens * ff + 4 * d * ff,
        name="states_cotangent",
        grid=(tokens // bm,),
        in_specs=[rows, rows, wide_rows, wide_rows, anywhere, anywhere],
        out_specs=rows,
        out_shape=jax.ShapeDtypeStruct((tokens, d), BF16),
        scratch_shapes=[pltpu.VMEM((2, d, ff), BF16), pltpu.VMEM((bm, d), F32), pltpu.SemaphoreType.DMA((2, n))],
    )(h, dy, dg, du, w_gate, w_up)


SLOTS, ARRIVALS = 3, 4


def pair_scratch(rows, columns):
    return [
        pltpu.VMEM((SLOTS, 2, rows, columns), BF16),
        pltpu.VMEM((ARRIVALS, rows, columns), BF16),
        pltpu.SemaphoreType.DMA((SLOTS,)),
        pltpu.SemaphoreType.DMA((ARRIVALS,)),
    ]


def pair_step(n, make, out, made, came, sent, arrived):
    j = pl.program_id(0)
    me = lax.axis_index("dp")
    core = lax.rem(me, 2)
    other = me + 1 - 2 * core

    def transfer(step):
        slot, place = lax.rem(step, SLOTS), lax.rem(step, ARRIVALS)
        return pltpu.make_async_remote_copy(
            src_ref=made.at[slot, 1 - core],
            dst_ref=came.at[place],
            send_sem=sent.at[slot],
            recv_sem=arrived.at[place],
            device_id={"dp": other},
            device_id_type=pl.DeviceIdType.MESH,
        )

    @pl.when(j == 0)
    def _():
        barrier = pltpu.get_barrier_semaphore()
        pl.semaphore_signal(barrier, inc=1, device_id={"dp": other}, device_id_type=pl.DeviceIdType.MESH)
        pl.semaphore_wait(barrier, 1)

    @pl.when(j >= 2)
    def _():
        transfer(j - 2).wait()
        own = made[lax.rem(j - 2, SLOTS), core]
        out[...] = (own.astype(F32) + came[lax.rem(j - 2, ARRIVALS)].astype(F32)).astype(BF16)

    @pl.when(j < n)
    def _():
        make(made.at[lax.rem(j, SLOTS)])
        transfer(j).start()


def pair_params(number):
    return {"collective_id": number, "has_side_effects": True}


def down_gradient(number, hid, dy):
    tokens, ff = hid.shape
    d = dy.shape[-1]
    chips = lax.axis_size("dp") // 2
    own = ff // (2 * chips)
    bf = 1152
    n, per = ff // bf, bf // (2 * own)

    def body(hid, dy, out, *scratch):
        def make(slot):
            block = dot(hid[...], dy[...], TN)
            for i in range(per):
                for half in range(2):
                    at = (2 * i + half) * own
                    slot[half, i * own : (i + 1) * own, :] = block[at : at + own].astype(BF16)

        pair_step(n, make, out, *scratch)

    return call(
        body,
        2 * tokens * d * ff,
        2 * tokens * ff + d * ff,
        pair_params(number),
        name=f"down_gradient_{number}",
        grid=(n + 2,),
        in_specs=[pl.BlockSpec((tokens, bf), lambda j: (0, jnp.minimum(j, n - 1))), whole((tokens, d))],
        out_specs=pl.BlockSpec((bf // 2, d), lambda j: (jnp.maximum(j - 2, 0), 0)),
        out_shape=jax.ShapeDtypeStruct((ff // 2, d), BF16),
        scratch_shapes=pair_scratch(bf // 2, d),
    )(hid, dy)


PART = 256


def halves_specs(shape, first, n, half, layer=None, transposed=False):
    def spec(h):
        def at(j):
            k = h * half + first + jnp.minimum(j, n - 1)
            index = (k, 0) if transposed else (0, k)
            return index if layer is None else (layer, *index)

        return pl.BlockSpec(shape, at)

    return [spec(0), spec(1)]


def gate_up_gradient(number, first, n, a_t, dg, du):
    d, tokens = a_t.shape
    half = dg.shape[-1] // (2 * PART)

    def body(a_t, dg0, dg1, du0, du1, out, *scratch):
        def make(slot):
            for h, (dg, du) in enumerate(((dg0, du0), (dg1, du1))):
                slot[h, :, :PART] = dot(a_t[...], dg[...]).astype(BF16)
                slot[h, :, PART:] = dot(a_t[...], du[...]).astype(BF16)

        pair_step(n, make, out, *scratch)

    t_specs = halves_specs((tokens, PART), first, n, half)
    return call(
        body,
        8 * tokens * d * PART * n,
        8 * tokens * PART * n,
        pair_params(number),
        name=f"gate_up_gradient_{number}",
        grid=(n + 2,),
        in_specs=[whole((d, tokens)), *t_specs, *t_specs],
        out_specs=pl.BlockSpec((d, 2 * PART), lambda j: (0, jnp.maximum(j - 2, 0))),
        out_shape=jax.ShapeDtypeStruct((d, 2 * PART * n), BF16),
        scratch_shapes=pair_scratch(d, 2 * PART),
    )(a_t, dg, dg, du, du)


SIDE = 4
PLACES = 4


def first_layer_gradient(number, layer, a_t, dy, gate, up, w_down):
    d, tokens = a_t.shape
    half = gate.shape[-1] // (2 * PART)
    n = half
    bm = 512
    rows = d // SIDE**2
    mid = PART // 2

    def body(a_t, dy, g0, g1, u0, u1, w0, w1, out, dg, du, made, came, sums, across1, pass1, got1, total1, across2, pass2, got2, ps, pr, sent, arrived):
        j = pl.program_id(0)
        me = lax.axis_index("dp")
        core = lax.rem(me, 2)
        other = me + 1 - 2 * core
        x, y = lax.div(me, 2 * SIDE), lax.rem(lax.div(me, 2), SIDE)

        def at(x, y):
            return {"dp": (x * SIDE + y) * 2 + core}

        def beside(axis, way):
            to = lax.rem((x if axis == 0 else y) + (1 if way == 0 else SIDE - 1), SIDE)
            return at(to, y) if axis == 0 else at(x, to)

        here = (x, y)

        def transfer(stage, color, way, block):
            place, slot = lax.rem(block, PLACES), lax.rem(block, SLOTS)
            first, second = color, 1 - color
            columns = slice(color * PART, (color + 1) * PART)
            if stage == 1:
                far = lax.rem(here[first] + 2, SIDE)
                part = slice(2 * way, 2 * way + 2)
                src = sums.at[slot, far, part, :, columns] if color == 0 else sums.at[slot, part, far, :, columns]
                dst = across1.at[color, place, way]
            elif stage == 2:
                src, dst = pass1.at[color, place, way], got1.at[color, place, way]
            elif stage == 3:
                far = lax.rem(here[second] + 2, SIDE)
                src = total1.at[color, place, far, :, slice(way * mid, (way + 1) * mid)]
                dst = across2.at[color, place, way]
            else:
                src, dst = pass2.at[color, place, way], got2.at[color, place, way]
            index = ((stage - 1) * 2 + color) * 2 + way
            return pltpu.make_async_remote_copy(
                src_ref=src,
                dst_ref=dst,
                send_sem=sent.at[index, place],
                recv_sem=arrived.at[index, place],
                device_id=beside(first if stage <= 2 else second, way),
                device_id_type=pl.DeviceIdType.MESH,
            )

        def swap(block):
            slot, place = lax.rem(block, SLOTS), lax.rem(block, PLACES)
            return pltpu.make_async_remote_copy(
                src_ref=made.at[slot, 1 - core],
                dst_ref=came.at[place],
                send_sem=ps.at[slot],
                recv_sem=pr.at[place],
                device_id={"dp": other},
                device_id_type=pl.DeviceIdType.MESH,
            )

        def of(color, slot, i):
            columns = slice(color * PART, (color + 1) * PART)
            t = sums[slot, i, :, :, columns] if color == 0 else sums[slot, :, i, :, columns]
            return t.astype(F32)

        def stage(lag, act):
            @pl.when((j >= lag) & (j < n + lag))
            def _():
                act(j - lag)

        @pl.when(j == 0)
        def _():
            barrier = pltpu.get_barrier_semaphore()
            for peer in ({"dp": other}, beside(0, 0), beside(0, 1), beside(1, 0), beside(1, 1)):
                pl.semaphore_signal(barrier, inc=1, device_id=peer, device_id_type=pl.DeviceIdType.MESH)
            pl.semaphore_wait(barrier, 5)

        def last(block):
            place = lax.rem(block, PLACES)
            for color in range(2):
                for way in range(2):
                    transfer(4, color, way, block).wait()
                b = here[1 - color]
                t = total1[color, place, b].astype(F32) + got2[color, place, 0].astype(F32) + got2[color, place, 1].astype(F32)
                out[color] = t.astype(BF16)

        def fourth(block):
            place = lax.rem(block, PLACES)
            for color in range(2):
                for way in range(2):
                    transfer(3, color, way, block).wait()
                for way in range(2):
                    b = lax.rem(here[1 - color] + (1 if way == 0 else SIDE - 1), SIDE)
                    pass2[color, place, way] = total1[color, place, b]
                    c = slice(way * mid, (way + 1) * mid)
                    more = total1[color, place, b, :, c].astype(F32) + across2[color, place, way].astype(F32)
                    pass2[color, place, way, :, c] = more.astype(BF16)
                    transfer(4, color, way, block).start()

        def third(block):
            place, slot = lax.rem(block, PLACES), lax.rem(block, SLOTS)
            for color in range(2):
                for way in range(2):
                    transfer(2, color, way, block).wait()
                t = of(color, slot, here[color]) + got1[color, place, 0].astype(F32) + got1[color, place, 1].astype(F32)
                total1[color, place] = t.astype(BF16)
                for way in range(2):
                    transfer(3, color, way, block).start()

        def second(block):
            place, slot = lax.rem(block, PLACES), lax.rem(block, SLOTS)
            for color in range(2):
                for way in range(2):
                    transfer(1, color, way, block).wait()
                for way in range(2):
                    t = of(color, slot, lax.rem(here[color] + (1 if way == 0 else SIDE - 1), SIDE))
                    p = slice(2 * way, 2 * way + 2)
                    q = slice(2 - 2 * way, 4 - 2 * way)
                    pass1[color, place, way, p] = (t[p] + across1[color, place, way].astype(F32)).astype(BF16)
                    pass1[color, place, way, q] = t[q].astype(BF16)
                    transfer(2, color, way, block).start()

        def first(block):
            place, slot = lax.rem(block, PLACES), lax.rem(block, SLOTS)
            swap(block).wait()
            for k in range(SIDE**2):
                r = slice(k * rows, (k + 1) * rows)
                t = made[slot, core, r, :].astype(F32) + came[place, r, :].astype(F32)
                sums[slot, k // SIDE, k % SIDE] = t.astype(BF16)
            for color in range(2):
                for way in range(2):
                    transfer(1, color, way, block).start()

        def make(block):
            slot = lax.rem(block, SLOTS)
            for h, (g, u, w) in enumerate(((g0, u0, w0), (g1, u1, w1))):
                for i in range(tokens // bm):
                    r = slice(i * bm, (i + 1) * bm)
                    dg[h, r, :], du[h, r, :], _ = gate_up_cotangents(g[r, :], u[r, :], dot(dy[r, :], w[...], NT))
                made[slot, h, :, :PART] = dot(a_t[...], dg[h]).astype(BF16)
                made[slot, h, :, PART:] = dot(a_t[...], du[h]).astype(BF16)
            swap(block).start()

        stage(6, last)
        stage(5, fourth)
        stage(4, third)
        stage(3, second)
        stage(2, first)
        stage(0, make)

    t_specs = halves_specs((tokens, PART), 0, n, half)
    block = (SIDE, rows, PART)
    return call(
        body,
        12 * tokens * d * PART * n,
        16 * tokens * PART * n,
        pair_params(number),
        name="first_layer_gradient",
        grid=(n + 6,),
        in_specs=[whole((d, tokens)), whole((tokens, d)), *t_specs, *t_specs, *halves_specs((None, PART, d), 0, n, half, layer, True)],
        out_specs=pl.BlockSpec((2, rows, PART), lambda j: (0, 0, jnp.maximum(j - 6, 0))),
        out_shape=jax.ShapeDtypeStruct((2, rows, PART * n), BF16),
        scratch_shapes=[
            pltpu.VMEM((2, tokens, PART), BF16),
            pltpu.VMEM((2, tokens, PART), BF16),
            pltpu.VMEM((SLOTS, 2, d, 2 * PART), BF16),
            pltpu.VMEM((PLACES, d, 2 * PART), BF16),
            pltpu.VMEM((SLOTS, SIDE, SIDE, rows, 2 * PART), BF16),
            pltpu.VMEM((2, PLACES, 2, SIDE // 2, rows, PART), BF16),
            pltpu.VMEM((2, PLACES, 2, *block), BF16),
            pltpu.VMEM((2, PLACES, 2, *block), BF16),
            pltpu.VMEM((2, PLACES, *block), BF16),
            pltpu.VMEM((2, PLACES, 2, rows, mid), BF16),
            pltpu.VMEM((2, PLACES, 2, rows, PART), BF16),
            pltpu.VMEM((2, PLACES, 2, rows, PART), BF16),
            pltpu.SemaphoreType.DMA((SLOTS,)),
            pltpu.SemaphoreType.DMA((PLACES,)),
            pltpu.SemaphoreType.DMA((16, PLACES)),
            pltpu.SemaphoreType.DMA((16, PLACES)),
        ],
    )(a_t, dy, gate, gate, up, up, w_down, w_down)


def updated_and_gathered(number, gate_up0, gate_up1, down0, down1, w_gate, w_up, w_down, m_gate, m_up, m_down, v_gate, v_up, v_down):
    n = lax.axis_size("dp")
    layers, d, ff = w_gate.shape
    rows, half = gate_up0.shape[1:]
    own_rows, moment_rows = ff // n, d // n
    steps = half // PART
    width = 2 * half + d
    cut = -(-width // 256) * 128
    count = 3 * layers * d * ff
    parts = (slice(0, cut), slice(cut, width))
    plan = []

    def body(gu0, gu1, d0, d1, wg, wu, wd, mg, mu, md, vg, vu, vd, ag, wd1, nmg, nmu, nmd, nvg, nvu, nvd,
             w_gu, w_d, mom, mom_d, packs, spare, tile, tiles, load, swap_s, swap_r, norm_s, norm_r, sent, arrived):
        me = lax.axis_index("dp")
        core = lax.rem(me, 2)
        other = me + 1 - 2 * core
        chip = lax.div(me, 2)
        x, y = lax.div(chip, SIDE), lax.rem(chip, SIDE)
        here = (x, y)
        mine, theirs = (pl.ds(pl.multiple_of(c * half, 128), half) for c in (core, 1 - core))

        moments = (mg, mu, vg, vu)
        new_moments = (nmg, nmu, nvg, nvu)
        loads = [
            *[(t.at[:, :, mine], mom.at[k, core]) for k, t in enumerate(moments)],
            (md, mom_d.at[0]),
            (vd, mom_d.at[1]),
            (wg.at[:, pl.ds(pl.multiple_of(chip * rows, 8), rows), mine], w_gu.at[0]),
            (wu.at[:, pl.ds(pl.multiple_of(chip * rows, 8), rows), mine], w_gu.at[1]),
            (wd.at[:, pl.ds(pl.multiple_of(me * own_rows, 16), own_rows), :], w_d),
        ]
        loads = [pltpu.make_async_copy(a, b, load.at[k]) for k, (a, b) in enumerate(loads)]
        for copy in loads:
            copy.start()

        barrier = pltpu.get_barrier_semaphore()

        def greet(i, _):
            pl.semaphore_signal(barrier, inc=1, device_id={"dp": lax.rem(me + i, n)}, device_id_type=pl.DeviceIdType.MESH)
            return 0

        lax.fori_loop(1, n, greet, 0)

        def square(t):
            t = t.astype(F32)
            t = t * t
            return sum(t[k * 8 : (k + 1) * 8] for k in range(t.shape[0] // 8))

        def squares(k, total):
            at = pl.ds(pl.multiple_of(k * PART, PART), PART)
            both = pl.ds(pl.multiple_of(k * 2 * PART, PART), 2 * PART)
            two = square(gu1[:, both])
            return total + square(gu0[0, :, at]) + square(gu0[1, :, at]) + two[:, :PART] + two[:, PART:]

        total = lax.fori_loop(0, steps, squares, jnp.zeros((8, PART), F32))
        downs = square(d0[...]) + square(d1[...])
        total = total[:, :128] + total[:, 128:] + sum(downs[:, k * 128 : (k + 1) * 128] for k in range(d // 128))
        tile[...] = total
        tiles[0] = total

        pl.semaphore_wait(barrier, n - 1)

        def swap(src, dst, k):
            return pltpu.make_async_remote_copy(
                src_ref=src, dst_ref=dst, send_sem=swap_s.at[k], recv_sem=swap_r.at[k], device_id={"dp": other}, device_id_type=pl.DeviceIdType.MESH
            )

        def size(i):
            return pltpu.make_async_remote_copy(
                src_ref=tile,
                dst_ref=tiles.at[i],
                send_sem=norm_s.at[i],
                recv_sem=norm_r.at[i],
                device_id={"dp": lax.rem(me + i, n)},
                device_id_type=pl.DeviceIdType.MESH,
            )

        lax.fori_loop(1, n, lambda i, _: (size(i).start(), 0)[1], 0)
        swaps = [swap(t.at[:, :, theirs], mom.at[k, core], k) for k, t in enumerate(moments)]
        for copy in swaps:
            copy.start()
        for copy in loads:
            copy.wait()
        for copy in swaps:
            copy.wait()
        lax.fori_loop(1, n, lambda i, _: (size(i).wait(), 0)[1], 0)
        total = lax.fori_loop(0, n, lambda i, total: total + tiles[lax.rem(me - i + n, n)], jnp.zeros((8, 128), F32))
        total = jnp.sum(jnp.sum(total, 0, keepdims=True), 1, keepdims=True)
        factor = jnp.minimum(1.0, 0.5 * lax.rsqrt(total / count + 1e-30))

        def adamw(w, m, v, g):
            g = g * factor
            m = 0.9 * m + 0.1 * g
            v = 0.95 * v + 0.05 * g * g
            return w - 0.02 * (m * lax.rsqrt(v + 1e-8) + 0.1 * w), m, v

        def step_gate_up(layer):
            for gu in range(2):

                def columns(k, _, gu=gu):
                    at = pl.ds(pl.multiple_of(k * PART, PART), PART)
                    if layer == 0:
                        g = gu0[gu, :, at]
                    else:
                        g = gu1[:, pl.ds(pl.multiple_of((2 * k + gu) * PART, PART), PART)]
                    g = g.astype(F32)
                    w = w_gu[gu, layer, :, at].astype(F32)
                    new = []
                    for r in range(2):
                        p = slice(r * moment_rows, (r + 1) * moment_rows)
                        one, m, v = adamw(w[p], mom[gu, r, layer, :, at], mom[2 + gu, r, layer, :, at], g[p])
                        mom[gu, r, layer, :, at] = m
                        mom[2 + gu, r, layer, :, at] = v
                        new.append(one)
                    packs[layer, :, pl.ds(pl.multiple_of(gu * half + k * PART, PART), PART)] = jnp.concatenate(new, 0).astype(BF16)
                    return 0

                lax.fori_loop(0, steps, columns, 0)

        def step_down(layer, p, g):
            new, m, v = adamw(w_d[layer, p, :].astype(F32), mom_d[0, layer, p, :], mom_d[1, layer, p, :], g[p, :].astype(F32))
            mom_d[0, layer, p, :] = m
            mom_d[1, layer, p, :] = v
            return new.astype(BF16)

        def place(color, i, k, whose, part):
            i, k = (lax.rem(t + SIDE, SIDE) for t in (i, k))
            a, b = (i, k) if color == 0 else (k, i)
            return ag.at[a, b, whose, color, :, parts[part]]

        def beside(axis, way):
            to = lax.rem(here[axis] + (1 if way == 0 else SIDE - 1), SIDE)
            a, b = (to, y) if axis == 0 else (x, to)
            return {"dp": (a * SIDE + b) * 2 + core}

        started = {}

        def send(name, color, o, q, part, to):
            index = len(plan) if name not in plan else plan.index(name)
            if name not in plan:
                plan.append(name)
            dst = place(color, here[color] + o, here[1 - color] + q, core, part)
            src = packs.at[color, :, parts[part]] if (o, q) == (0, 0) else dst
            copy = pltpu.make_async_remote_copy(
                src_ref=src, dst_ref=dst, send_sem=sent.at[index], recv_sem=arrived.at[index], device_id=to, device_id_type=pl.DeviceIdType.MESH
            )
            copy.start()
            started[name] = copy

        def along_first(color, way, part):
            send(("a", color, way, part), color, 0, 0, part, beside(color, way))

        def on_first(color, way):
            send(("b", color, way), color, -1 if way == 0 else 1, 0, way, beside(color, way))

        def along_second(color, o, part):
            for way in range(2):
                send(("c", color, way, o, part), color, o, 0, part, beside(1 - color, way))

        def on_second(color, way, o):
            send(("d", color, way, o), color, o, -1 if way == 0 else 1, way, beside(1 - color, way))

        def share(color, o, q, part):
            send(("e", color, o, q, part), color, o, q, part, {"dp": other})

        def own(color):
            for part in range(2):
                for way in range(2):
                    along_first(color, way, part)
            for part in range(2):
                along_second(color, 0, part)
                share(color, 0, 0, part)
            copy = pltpu.make_async_copy(packs.at[color], ag.at[x, y, core, color], load.at[color])
            copy.start()
            return copy

        step_gate_up(0)
        packs[0, :, 2 * half :] = step_down(0, slice(0, rows), d0)
        kept = [own(0)]
        step_gate_up(1)
        packs[1, :, 2 * half :] = step_down(0, slice(rows, 2 * rows), d0)
        kept.append(own(1))
        spare[...] = step_down(1, slice(0, own_rows), d1)

        stores = [
            *[(mom.at[k, core], t.at[:, :, mine]) for k, t in enumerate(new_moments)],
            (mom_d.at[0], nmd),
            (mom_d.at[1], nvd),
            (spare, wd1),
        ]
        stores = [pltpu.make_async_copy(a, b, load.at[2 + k]) for k, (a, b) in enumerate(stores)]
        backs = [swap(mom.at[k, 1 - core], t.at[:, :, mine], 4 + k) for k, t in enumerate(new_moments)]
        for copy in (*stores, *backs):
            copy.start()

        both = [(color, way) for color in range(2) for way in range(2)]
        for part in range(2):
            for color, way in both:
                started["a", color, way, part].wait_recv()
                if way == part:
                    on_first(color, way)
                o = -1 if way == 0 else 1
                along_second(color, o, part)
                share(color, o, 0, part)

        def arrivals(o):
            for part in range(2):
                for color, way in both:
                    started["c", color, way, o, part].wait_recv()
                    if way == part:
                        on_second(color, way, o)
                    share(color, o, -1 if way == 0 else 1, part)

        arrivals(0)
        for color, way in both:
            started["b", color, way].wait_recv()
            along_second(color, 2, way)
            share(color, 2, 0, way)
        for o in (-1, 1, 2):
            arrivals(o)
        for o in (0, -1, 1, 2):
            for color, way in both:
                started["d", color, way, o].wait_recv()
                share(color, o, 2, way)
        for name, copy in started.items():
            copy.wait_send()
            if name[0] == "e":
                copy.wait_recv()
        for copy in (*kept, *stores, *backs):
            copy.wait()

    anywhere = pl.BlockSpec(memory_space=pl.ANY)
    vmem = pl.BlockSpec(memory_space=pltpu.VMEM)
    return call(
        body,
        1e9,
        1e8,
        pair_params(number),
        name="updated_and_gathered",
        in_specs=[vmem] * 4 + [anywhere] * 9,
        out_specs=[anywhere] * 8,
        out_shape=[
            jax.ShapeDtypeStruct((SIDE, SIDE, 2, 2, rows, width), BF16),
            jax.ShapeDtypeStruct((own_rows, d), BF16),
            *[jax.ShapeDtypeStruct(t.shape, F32) for t in (m_gate, m_up, m_down, v_gate, v_up, v_down)],
        ],
        scratch_shapes=[
            pltpu.VMEM((2, layers, rows, half), BF16),
            pltpu.VMEM((layers, own_rows, d), BF16),
            pltpu.VMEM((4, 2, layers, moment_rows, half), F32),
            pltpu.VMEM((2, layers, own_rows, d), F32),
            pltpu.VMEM((2, rows, width), BF16),
            pltpu.VMEM((own_rows, d), BF16),
            pltpu.VMEM((8, 128), F32),
            pltpu.VMEM((n, 8, 128), F32),
            pltpu.SemaphoreType.DMA((9,)),
            pltpu.SemaphoreType.DMA((8,)),
            pltpu.SemaphoreType.DMA((8,)),
            pltpu.SemaphoreType.DMA((n,)),
            pltpu.SemaphoreType.DMA((n,)),
            pltpu.SemaphoreType.DMA((124,)),
            pltpu.SemaphoreType.DMA((124,)),
        ],
    )(gate_up0, gate_up1, down0, down1, w_gate, w_up, w_down, m_gate, m_up, m_down, v_gate, v_up, v_down)


def placed(packs, layers, d, ff):
    rows, width = packs.shape[-2:]
    half = ff // 2
    per = 2

    def body(t, gate, up, down):
        for b in range(per):
            for core in range(2):
                for color in range(2):
                    r = slice(b * rows, (b + 1) * rows)
                    c = slice(core * half, (core + 1) * half)
                    gate[color, r, c] = t[b, core, color, :, :half]
                    up[color, r, c] = t[b, core, color, :, half : 2 * half]
                    at = ((b * 2 + core) * 2 + color) * rows
                    down[at : at + rows, :] = t[b, core, color, :, 2 * half :]

    n = SIDE // per
    out = pl.BlockSpec((layers, per * rows, ff), lambda i, j: (0, i * n + j, 0))
    return call(
        body,
        1,
        4 * packs.size,
        name="placed",
        grid=(SIDE, n),
        in_specs=[pl.BlockSpec((None, per, 2, 2, rows, width), lambda i, j: (i, j, 0, 0, 0, 0))],
        out_specs=[out, out, pl.BlockSpec((None, per * 4 * rows, d), lambda i, j: (0, i * n + j, 0))],
        out_shape=[jax.ShapeDtypeStruct((layers, d, ff), BF16)] * 2 + [jax.ShapeDtypeStruct((layers, ff, d), BF16)],
    )(packs)


def copied(*arrays):
    def body(*refs):
        for a, b in zip(refs[: len(arrays)], refs[len(arrays) :], strict=True):
            b[...] = a[...]

    specs = [pl.BlockSpec((1, *t.shape[1:]), lambda i: (i, 0, 0)) for t in arrays]
    return call(
        body,
        1,
        sum(8 * t.size for t in arrays),
        name="copied",
        grid=(arrays[0].shape[0],),
        in_specs=specs,
        out_specs=specs,
        out_shape=[jax.ShapeDtypeStruct(t.shape, t.dtype) for t in arrays],
    )(*arrays)


def placed_last(down, gathered):
    layers, ff, d = down.shape
    bm = 1152

    def body(down, t, out):
        out[...] = t[...]

    return call(
        body,
        1,
        4 * gathered.size,
        name="placed_last",
        grid=(ff // bm,),
        in_specs=[pl.BlockSpec(memory_space=pl.ANY), pl.BlockSpec((bm, d), lambda i: (i, 0))],
        out_specs=pl.BlockSpec((None, bm, d), lambda i: (layers - 1, i, 0)),
        out_shape=jax.ShapeDtypeStruct(down.shape, BF16),
        input_output_aliases={0: 0},
    )(down, gathered)


def solution(mesh):
    chips = mesh.shape["dp"] // 2
    same_core = [[2 * chip + core for chip in range(chips)] for core in range(2)]

    def summed(part):
        return lax.psum_scatter(part, "dp", scatter_dimension=0, axis_index_groups=same_core, tiled=True)

    def step(x, dy, w_gate, w_up, w_down, *moments):
        x, dy = x[0], dy[0]
        layers, d, ff = w_gate.shape

        gate, up, hid0, a0_t = hidden_forward(0, x, w_gate, w_up)
        h1, a1, a1_t = down_forward(0, x, hid0, w_down)
        hid1, dg1, du1 = last_layer(1, a1, dy, w_gate, w_up, w_down)
        gate_up1 = gate_up_gradient(1, 0, ff // (2 * PART), a1_t, dg1, du1)
        hid1, gate_up1 = lax.optimization_barrier((hid1, gate_up1))
        gate_up1 = summed(gate_up1)
        down1 = down_gradient(2, hid1, dy)
        dg1, du1, down1 = lax.optimization_barrier((dg1, du1, down1))
        down1 = summed(down1)
        dh = states_cotangent(1, h1, dy, dg1, du1, w_gate, w_up)
        down0 = down_gradient(3, hid0, dh)
        dh, down0 = lax.optimization_barrier((dh, down0))
        down0 = summed(down0)
        gate_up0 = first_layer_gradient(4, 0, a0_t, dh, gate, up, w_down)
        gate_up0, gate_up1 = lax.optimization_barrier((gate_up0, gate_up1))
        gate_up1, down1 = lax.optimization_barrier((gate_up1, down1))
        down1, down0 = lax.optimization_barrier((down1, down0))
        packs, last, *moments = updated_and_gathered(5, gate_up0, gate_up1, down0, down1, w_gate, w_up, w_down, *moments)
        last = lax.all_gather(last, "dp", tiled=True)
        new_gate, new_up, new_down = placed(packs, layers, d, ff)
        moments[2], moments[5] = copied(moments[2], moments[5])
        new_down = placed_last(new_down, last)
        return new_gate, new_up, new_down, *moments

    sequences = P(("rep", "dp"))
    return jax.shard_map(
        step,
        mesh=mesh,
        in_specs=(sequences, sequences, P(), P(), P(), *[P(None, "dp")] * 6),
        out_specs=(P("rep"), P("rep"), P("rep"), *[P("rep", "dp")] * 6),
        check_vma=False,
    )
```

```python
import functools
import math

import jax
import jax.numpy as jnp
from jax import lax
from jax.experimental import pallas as pl
from jax.experimental.pallas import tpu as pltpu
from jax.sharding import PartitionSpec as P

F32, BF16 = jnp.float32, jnp.bfloat16
VMEM_LIMIT = 67_043_328
NN = (((1,), (0,)), ((), ()))
NT = (((1,), (1,)), ((), ()))
TN = (((0,), (0,)), ((), ()))


def dot(a, b, dims=NN):
    return lax.dot_general(a, b, dims, preferred_element_type=F32)


def sigmoid(x):
    return 1.0 / (1.0 + jnp.exp(-x))


def whole(shape):
    return pl.BlockSpec(shape, lambda *_: (0,) * len(shape), pipeline_mode=pl.Buffered(1))


def call(body, flops, moved, params=None, **kw):
    return pl.pallas_call(
        body,
        cost_estimate=pl.CostEstimate(flops=int(flops), bytes_accessed=int(moved), transcendentals=0),
        compiler_params=pltpu.CompilerParams(**{"vmem_limit_bytes": VMEM_LIMIT, **(params or {})}),
        **kw,
    )


def row_scale(wide):
    return lax.rsqrt(jnp.mean(wide * wide, -1, keepdims=True) + 1e-6)


def hidden_forward(layer, x, w_gate, w_up):
    tokens, d = x.shape
    ff = w_gate.shape[-1]
    bf, bm = 256, 512
    n = tokens // bm

    def body(x, wg, wu, gate, up, hid, a_t, x_in, a, came):
        j = pl.program_id(0)

        def rows(i):
            return pl.ds(pl.multiple_of(i * bm, bm), bm)

        def come(i):
            return pltpu.make_async_copy(x.at[rows(i)], x_in.at[rows(i)], came.at[i])

        def chunk(r):
            g, u = dot(a[r, :], wg[...]), dot(a[r, :], wu[...])
            gate[r, :] = g
            up[r, :] = u
            hid[r, :] = (g * sigmoid(g) * u).astype(BF16)

        @pl.when(j == 0)
        def _():
            for i in range(n):
                come(i).start()

            def first(i, _):
                come(i).wait()
                wide = x_in[rows(i), :].astype(F32)
                unit = wide * row_scale(wide)
                a[rows(i), :] = unit.astype(BF16)
                a_t[:, rows(i)] = unit.T.astype(BF16)
                chunk(rows(i))
                return 0

            lax.fori_loop(0, n, first, 0)

        @pl.when(j > 0)
        def _():
            for i in range(n):
                chunk(slice(i * bm, (i + 1) * bm))

    w_spec = pl.BlockSpec((None, d, bf), lambda j: (layer, 0, j))
    o_spec = pl.BlockSpec((tokens, bf), lambda j: (0, j))
    wide = jax.ShapeDtypeStruct((tokens, ff), F32)
    return call(
        body,
        4 * tokens * d * ff,
        10 * tokens * ff + 4 * d * ff,
        name="hidden_forward",
        grid=(ff // bf,),
        in_specs=[pl.BlockSpec(memory_space=pl.ANY), w_spec, w_spec],
        out_specs=[*[o_spec] * 3, whole((d, tokens))],
        out_shape=(wide, wide, jax.ShapeDtypeStruct((tokens, ff), BF16), jax.ShapeDtypeStruct((d, tokens), BF16)),
        scratch_shapes=[pltpu.VMEM((tokens, d), BF16), pltpu.VMEM((tokens, d), BF16), pltpu.SemaphoreType.DMA((n,))],
    )(x, w_gate, w_up)


def down_forward(layer, x, hid, w_down):
    tokens, ff = hid.shape
    d = x.shape[-1]
    bm = 256

    def body(x, hid, wd, h1, a1, a1_t):
        h = (x[...].astype(F32) + dot(hid[...], wd[...]).astype(BF16).astype(F32)).astype(BF16)
        h1[...] = h
        wide = h.astype(F32)
        unit = wide * row_scale(wide)
        a1[...] = unit.astype(BF16)
        a1_t[...] = unit.T.astype(BF16)

    rows = pl.BlockSpec((bm, d), lambda i: (i, 0))
    out = jax.ShapeDtypeStruct((tokens, d), BF16)
    return call(
        body,
        2 * tokens * d * ff,
        2 * tokens * ff + 2 * d * ff,
        name="down_forward",
        grid=(tokens // bm,),
        in_specs=[
            rows,
            pl.BlockSpec((bm, ff), lambda i: (i, 0)),
            pl.BlockSpec((None, ff, d), lambda i: (layer, 0, 0), pipeline_mode=pl.Buffered(1)),
        ],
        out_specs=[rows, rows, pl.BlockSpec((d, bm), lambda i: (0, i))],
        out_shape=(out, out, jax.ShapeDtypeStruct((d, tokens), BF16)),
    )(x, hid, w_down)


def gate_up_cotangents(g, u, dh):
    dh = dh.astype(BF16).astype(F32)
    s = sigmoid(g)
    silu = g * s
    return (dh * u * (s + silu * (1.0 - s))).astype(BF16), (dh * silu).astype(BF16), (silu * u).astype(BF16)


def last_layer(layer, a, dy, w_gate, w_up, w_down):
    tokens, d = a.shape
    ff = w_gate.shape[-1]
    bf, bm = 256, 512

    def body(a, dy, wg, wu, wd, hid, dg, du):
        for i in range(tokens // bm):
            r = slice(i * bm, (i + 1) * bm)
            g, u = dot(a[r, :], wg[...]), dot(a[r, :], wu[...])
            dg[r, :], du[r, :], hid[r, :] = gate_up_cotangents(g, u, dot(dy[r, :], wd[...], NT))

    w_spec = pl.BlockSpec((None, d, bf), lambda j: (layer, 0, j))
    o_spec = pl.BlockSpec((tokens, bf), lambda j: (0, j))
    out = jax.ShapeDtypeStruct((tokens, ff), BF16)
    return call(
        body,
        6 * tokens * d * ff,
        6 * tokens * ff + 6 * d * ff,
        name="last_layer",
        grid=(ff // bf,),
        in_specs=[whole((tokens, d)), whole((tokens, d)), w_spec, w_spec, pl.BlockSpec((None, bf, d), lambda j: (layer, j, 0))],
        out_specs=[o_spec] * 3,
        out_shape=(out, out, out),
    )(a, dy, w_gate, w_up, w_down)


def states_cotangent(layer, h, dy, dg, du, w_gate, w_up):
    tokens, ff = dg.shape
    d = h.shape[-1]
    bm, bk = 256, 512
    n = ff // bk

    def body(h, dy, dg, du, wg, wu, out, w, total, came):
        def k(c):
            return pl.ds(pl.multiple_of(c * bk, bk), bk)

        def come(c):
            return [pltpu.make_async_copy(t.at[layer, :, k(c)], w.at[i, :, k(c)], came.at[i, c]) for i, t in enumerate((wg, wu))]

        def rest(da):
            wide = h[...].astype(F32)
            da = da.astype(BF16).astype(F32)
            s = row_scale(wide)
            back = da * s - wide * (s * s * s * jnp.mean(da * wide, -1, keepdims=True))
            out[...] = (dy[...].astype(F32) + back).astype(BF16)

        @pl.when(pl.program_id(0) == 0)
        def _():
            for c in range(n):
                for copy in come(c):
                    copy.start()
            total[...] = jnp.zeros_like(total)

            def add(c, _):
                for copy in come(c):
                    copy.wait()
                total[...] += dot(dg[:, k(c)], w[0, :, k(c)], NT) + dot(du[:, k(c)], w[1, :, k(c)], NT)
                return 0

            lax.fori_loop(0, n, add, 0)
            rest(total[...])

        @pl.when(pl.program_id(0) > 0)
        def _():
            rest(dot(dg[...], w[0], NT) + dot(du[...], w[1], NT))

    rows = pl.BlockSpec((bm, d), lambda i: (i, 0))
    wide_rows = pl.BlockSpec((bm, ff), lambda i: (i, 0))
    anywhere = pl.BlockSpec(memory_space=pl.ANY)
    return call(
        body,
        4 * tokens * d * ff,
        4 * tokens * ff + 4 * d * ff,
        name="states_cotangent",
        grid=(tokens // bm,),
        in_specs=[rows, rows, wide_rows, wide_rows, anywhere, anywhere],
        out_specs=rows,
        out_shape=jax.ShapeDtypeStruct((tokens, d), BF16),
        scratch_shapes=[pltpu.VMEM((2, d, ff), BF16), pltpu.VMEM((bm, d), F32), pltpu.SemaphoreType.DMA((2, n))],
    )(h, dy, dg, du, w_gate, w_up)


SLOTS, ARRIVALS = 3, 4


def pair_scratch(rows, columns):
    return [
        pltpu.VMEM((SLOTS, 2, rows, columns), BF16),
        pltpu.VMEM((ARRIVALS, rows, columns), BF16),
        pltpu.SemaphoreType.DMA((SLOTS,)),
        pltpu.SemaphoreType.DMA((ARRIVALS,)),
    ]


def pair_step(n, make, out, made, came, sent, arrived):
    j = pl.program_id(0)
    me = lax.axis_index("dp")
    core = lax.rem(me, 2)
    other = me + 1 - 2 * core

    def transfer(step):
        slot, place = lax.rem(step, SLOTS), lax.rem(step, ARRIVALS)
        return pltpu.make_async_remote_copy(
            src_ref=made.at[slot, 1 - core],
            dst_ref=came.at[place],
            send_sem=sent.at[slot],
            recv_sem=arrived.at[place],
            device_id={"dp": other},
            device_id_type=pl.DeviceIdType.MESH,
        )

    @pl.when(j == 0)
    def _():
        barrier = pltpu.get_barrier_semaphore()
        pl.semaphore_signal(barrier, inc=1, device_id={"dp": other}, device_id_type=pl.DeviceIdType.MESH)
        pl.semaphore_wait(barrier, 1)

    @pl.when(j >= 2)
    def _():
        transfer(j - 2).wait()
        own = made[lax.rem(j - 2, SLOTS), core]
        out[...] = (own.astype(F32) + came[lax.rem(j - 2, ARRIVALS)].astype(F32)).astype(BF16)

    @pl.when(j < n)
    def _():
        make(made.at[lax.rem(j, SLOTS)])
        transfer(j).start()


def pair_params(number):
    return {"collective_id": number, "has_side_effects": True}


def down_gradient(number, hid, dy):
    tokens, ff = hid.shape
    d = dy.shape[-1]
    chips = lax.axis_size("dp") // 2
    own = ff // (2 * chips)
    bf = 1152
    n, per = ff // bf, bf // (2 * own)

    def body(hid, dy, out, *scratch):
        def make(slot):
            block = dot(hid[...], dy[...], TN)
            for i in range(per):
                for half in range(2):
                    at = (2 * i + half) * own
                    slot[half, i * own : (i + 1) * own, :] = block[at : at + own].astype(BF16)

        pair_step(n, make, out, *scratch)

    return call(
        body,
        2 * tokens * d * ff,
        2 * tokens * ff + d * ff,
        pair_params(number),
        name=f"down_gradient_{number}",
        grid=(n + 2,),
        in_specs=[pl.BlockSpec((tokens, bf), lambda j: (0, jnp.minimum(j, n - 1))), whole((tokens, d))],
        out_specs=pl.BlockSpec((bf // 2, d), lambda j: (jnp.maximum(j - 2, 0), 0)),
        out_shape=jax.ShapeDtypeStruct((ff // 2, d), BF16),
        scratch_shapes=pair_scratch(bf // 2, d),
    )(hid, dy)


PART = 256


def halves_specs(shape, first, n, half, layer=None, transposed=False):
    def spec(h):
        def at(j):
            k = h * half + first + jnp.minimum(j, n - 1)
            index = (k, 0) if transposed else (0, k)
            return index if layer is None else (layer, *index)

        return pl.BlockSpec(shape, at)

    return [spec(0), spec(1)]


def gate_up_gradient(number, first, n, a_t, dg, du):
    d, tokens = a_t.shape
    half = dg.shape[-1] // (2 * PART)

    def body(a_t, dg0, dg1, du0, du1, out, *scratch):
        def make(slot):
            for h, (dg, du) in enumerate(((dg0, du0), (dg1, du1))):
                slot[h, :, :PART] = dot(a_t[...], dg[...]).astype(BF16)
                slot[h, :, PART:] = dot(a_t[...], du[...]).astype(BF16)

        pair_step(n, make, out, *scratch)

    t_specs = halves_specs((tokens, PART), first, n, half)
    return call(
        body,
        8 * tokens * d * PART * n,
        8 * tokens * PART * n,
        pair_params(number),
        name=f"gate_up_gradient_{number}",
        grid=(n + 2,),
        in_specs=[whole((d, tokens)), *t_specs, *t_specs],
        out_specs=pl.BlockSpec((d, 2 * PART), lambda j: (0, jnp.maximum(j - 2, 0))),
        out_shape=jax.ShapeDtypeStruct((d, 2 * PART * n), BF16),
        scratch_shapes=pair_scratch(d, 2 * PART),
    )(a_t, dg, dg, du, du)


SIDE = 4
PLACES = 4


def first_layer_gradient(number, layer, a_t, dy, gate, up, w_down):
    d, tokens = a_t.shape
    half = gate.shape[-1] // (2 * PART)
    n = half
    bm = 512
    rows = d // SIDE**2
    mid = PART // 2

    def body(a_t, dy, g0, g1, u0, u1, w0, w1, out, dg, du, made, came, sums, across1, pass1, got1, total1, across2, pass2, got2, ps, pr, sent, arrived):
        j = pl.program_id(0)
        me = lax.axis_index("dp")
        core = lax.rem(me, 2)
        other = me + 1 - 2 * core
        x, y = lax.div(me, 2 * SIDE), lax.rem(lax.div(me, 2), SIDE)

        def at(x, y):
            return {"dp": (x * SIDE + y) * 2 + core}

        def beside(axis, way):
            to = lax.rem((x if axis == 0 else y) + (1 if way == 0 else SIDE - 1), SIDE)
            return at(to, y) if axis == 0 else at(x, to)

        here = (x, y)

        def transfer(stage, color, way, block):
            place = lax.rem(block, PLACES)
            first, second = color, 1 - color
            columns = slice(color * PART, (color + 1) * PART)
            if stage == 1:
                far = lax.rem(here[first] + 2, SIDE)
                part = slice(2 * way, 2 * way + 2)
                src = sums.at[place, far, part, :, columns] if color == 0 else sums.at[place, part, far, :, columns]
                dst = across1.at[color, place, way]
            elif stage == 2:
                src, dst = pass1.at[color, lax.rem(block, 2), way], got1.at[color, place, way]
            elif stage == 3:
                far = lax.rem(here[second] + 2, SIDE)
                src = total1.at[color, place, far, :, slice(way * mid, (way + 1) * mid)]
                dst = across2.at[color, place, way]
            else:
                src, dst = pass2.at[color, place, way], got2.at[color, place, way]
            index = ((stage - 1) * 2 + color) * 2 + way
            return pltpu.make_async_remote_copy(
                src_ref=src,
                dst_ref=dst,
                send_sem=sent.at[index, place],
                recv_sem=arrived.at[index, place],
                device_id=beside(first if stage <= 2 else second, way),
                device_id_type=pl.DeviceIdType.MESH,
            )

        def swap(block):
            slot, place = lax.rem(block, SLOTS), lax.rem(block, PLACES)
            return pltpu.make_async_remote_copy(
                src_ref=made.at[slot, 1 - core],
                dst_ref=came.at[place],
                send_sem=ps.at[slot],
                recv_sem=pr.at[place],
                device_id={"dp": other},
                device_id_type=pl.DeviceIdType.MESH,
            )

        def of(color, place, i):
            columns = slice(color * PART, (color + 1) * PART)
            t = sums[place, i, :, :, columns] if color == 0 else sums[place, :, i, :, columns]
            return t.astype(F32)

        def stage(lag, act):
            @pl.when((j >= lag) & (j < n + lag))
            def _():
                act(j - lag)

        @pl.when(j == 0)
        def _():
            barrier = pltpu.get_barrier_semaphore()
            for peer in ({"dp": other}, beside(0, 0), beside(0, 1), beside(1, 0), beside(1, 1)):
                pl.semaphore_signal(barrier, inc=1, device_id=peer, device_id_type=pl.DeviceIdType.MESH)
            pl.semaphore_wait(barrier, 5)

        def last(block):
            place = lax.rem(block, PLACES)
            for color in range(2):
                for way in range(2):
                    transfer(4, color, way, block).wait()
                b = here[1 - color]
                t = total1[color, place, b].astype(F32) + got2[color, place, 0].astype(F32) + got2[color, place, 1].astype(F32)
                out[color] = t.astype(BF16)

        def fourth(block):
            place = lax.rem(block, PLACES)
            for color in range(2):
                for way in range(2):
                    transfer(3, color, way, block).wait()
                for way in range(2):
                    b = lax.rem(here[1 - color] + (1 if way == 0 else SIDE - 1), SIDE)
                    pass2[color, place, way] = total1[color, place, b]
                    c = slice(way * mid, (way + 1) * mid)
                    more = total1[color, place, b, :, c].astype(F32) + across2[color, place, way].astype(F32)
                    pass2[color, place, way, :, c] = more.astype(BF16)
                    transfer(4, color, way, block).start()

        def third(block):
            place = lax.rem(block, PLACES)
            for color in range(2):
                for way in range(2):
                    transfer(2, color, way, block).wait()
                t = of(color, place, here[color]) + got1[color, place, 0].astype(F32) + got1[color, place, 1].astype(F32)
                total1[color, place] = t.astype(BF16)
                for way in range(2):
                    transfer(3, color, way, block).start()

        def second(block):
            place = lax.rem(block, PLACES)
            for color in range(2):
                for way in range(2):
                    transfer(1, color, way, block).wait()
                for way in range(2):
                    t = of(color, place, lax.rem(here[color] + (1 if way == 0 else SIDE - 1), SIDE))
                    p = slice(2 * way, 2 * way + 2)
                    q = slice(2 - 2 * way, 4 - 2 * way)
                    pass1[color, lax.rem(block, 2), way, p] = (t[p] + across1[color, place, way].astype(F32)).astype(BF16)
                    pass1[color, lax.rem(block, 2), way, q] = t[q].astype(BF16)
                    transfer(2, color, way, block).start()

        def first(block):
            place, slot = lax.rem(block, PLACES), lax.rem(block, SLOTS)
            swap(block).wait()
            for k in range(SIDE**2):
                r = slice(k * rows, (k + 1) * rows)
                t = made[slot, core, r, :].astype(F32) + came[place, r, :].astype(F32)
                sums[place, k // SIDE, k % SIDE] = t.astype(BF16)
            for color in range(2):
                for way in range(2):
                    transfer(1, color, way, block).start()

        def make(block):
            slot = lax.rem(block, SLOTS)
            for h, (g, u, w) in enumerate(((g0, u0, w0), (g1, u1, w1))):
                for i in range(tokens // bm):
                    r = slice(i * bm, (i + 1) * bm)
                    dg[h, r, :], du[h, r, :], _ = gate_up_cotangents(g[r, :], u[r, :], dot(dy[r, :], w[...], NT))
                made[slot, h, :, :PART] = dot(a_t[...], dg[h]).astype(BF16)
                made[slot, h, :, PART:] = dot(a_t[...], du[h]).astype(BF16)
            swap(block).start()

        stage(8, last)
        stage(7, fourth)
        stage(6, third)
        stage(4, second)
        stage(2, first)
        stage(0, make)

    t_specs = halves_specs((tokens, PART), 0, n, half)
    block = (SIDE, rows, PART)
    return call(
        body,
        12 * tokens * d * PART * n,
        16 * tokens * PART * n,
        pair_params(number),
        name="first_layer_gradient",
        grid=(n + 8,),
        in_specs=[whole((d, tokens)), whole((tokens, d)), *t_specs, *t_specs, *halves_specs((None, PART, d), 0, n, half, layer, True)],
        out_specs=pl.BlockSpec((2, rows, PART), lambda j: (0, 0, jnp.maximum(j - 8, 0))),
        out_shape=jax.ShapeDtypeStruct((2, rows, PART * n), BF16),
        scratch_shapes=[
            pltpu.VMEM((2, tokens, PART), BF16),
            pltpu.VMEM((2, tokens, PART), BF16),
            pltpu.VMEM((SLOTS, 2, d, 2 * PART), BF16),
            pltpu.VMEM((PLACES, d, 2 * PART), BF16),
            pltpu.VMEM((PLACES, SIDE, SIDE, rows, 2 * PART), BF16),
            pltpu.VMEM((2, PLACES, 2, SIDE // 2, rows, PART), BF16),
            pltpu.VMEM((2, 2, 2, *block), BF16),
            pltpu.VMEM((2, PLACES, 2, *block), BF16),
            pltpu.VMEM((2, PLACES, *block), BF16),
            pltpu.VMEM((2, PLACES, 2, rows, mid), BF16),
            pltpu.VMEM((2, PLACES, 2, rows, PART), BF16),
            pltpu.VMEM((2, PLACES, 2, rows, PART), BF16),
            pltpu.SemaphoreType.DMA((SLOTS,)),
            pltpu.SemaphoreType.DMA((PLACES,)),
            pltpu.SemaphoreType.DMA((16, PLACES)),
            pltpu.SemaphoreType.DMA((16, PLACES)),
        ],
    )(a_t, dy, gate, gate, up, up, w_down, w_down)


def updated_and_gathered(number, gate_up0, gate_up1, down0, down1, w_gate, w_up, w_down, m_gate, m_up, m_down, v_gate, v_up, v_down):
    n = lax.axis_size("dp")
    layers, d, ff = w_gate.shape
    rows, half = gate_up0.shape[1:]
    own_rows, moment_rows = ff // n, d // n
    steps = half // PART
    width = 2 * half + d
    cut = -(-width // 256) * 128
    count = 3 * layers * d * ff
    parts = (slice(0, cut), slice(cut, width))
    plan = []

    def body(gu0, gu1, d0, d1, wg, wu, wd, mg, mu, md, vg, vu, vd, ag, wd1, nmg, nmu, nmd, nvg, nvu, nvd,
             w_gu, w_d, mom, mom_d, packs, spare, tile, tiles, load, swap_s, swap_r, norm_s, norm_r, sent, arrived):
        me = lax.axis_index("dp")
        core = lax.rem(me, 2)
        other = me + 1 - 2 * core
        chip = lax.div(me, 2)
        x, y = lax.div(chip, SIDE), lax.rem(chip, SIDE)
        here = (x, y)
        mine, theirs = (pl.ds(pl.multiple_of(c * half, 128), half) for c in (core, 1 - core))

        moments = (mg, mu, vg, vu)
        new_moments = (nmg, nmu, nvg, nvu)
        loads = [
            *[(t.at[:, l, mine], mom.at[k, core, l]) for k, t in enumerate(moments) for l in range(layers)],
            (md, mom_d.at[0]),
            (vd, mom_d.at[1]),
            (wg.at[:, pl.ds(pl.multiple_of(chip * rows, 8), rows), mine], w_gu.at[0]),
            (wu.at[:, pl.ds(pl.multiple_of(chip * rows, 8), rows), mine], w_gu.at[1]),
            (wd.at[:, pl.ds(pl.multiple_of(me * own_rows, 16), own_rows), :], w_d),
        ]
        loads = [pltpu.make_async_copy(a, b, load.at[k]) for k, (a, b) in enumerate(loads)]
        for copy in loads:
            copy.start()

        barrier = pltpu.get_barrier_semaphore()

        def greet(i, _):
            pl.semaphore_signal(barrier, inc=1, device_id={"dp": lax.rem(me + i, n)}, device_id_type=pl.DeviceIdType.MESH)
            return 0

        lax.fori_loop(1, n, greet, 0)

        def square(t):
            t = t.astype(F32)
            t = t * t
            return sum(t[k * 8 : (k + 1) * 8] for k in range(t.shape[0] // 8))

        def squares(k, total):
            at = pl.ds(pl.multiple_of(k * PART, PART), PART)
            both = pl.ds(pl.multiple_of(k * 2 * PART, PART), 2 * PART)
            two = square(gu1[:, both])
            return total + square(gu0[0, :, at]) + square(gu0[1, :, at]) + two[:, :PART] + two[:, PART:]

        total = lax.fori_loop(0, steps, squares, jnp.zeros((8, PART), F32))
        downs = square(d0[...]) + square(d1[...])
        total = total[:, :128] + total[:, 128:] + sum(downs[:, k * 128 : (k + 1) * 128] for k in range(d // 128))
        tile[...] = total
        tiles[0] = total

        pl.semaphore_wait(barrier, n - 1)

        def swap(src, dst, k):
            return pltpu.make_async_remote_copy(
                src_ref=src, dst_ref=dst, send_sem=swap_s.at[k], recv_sem=swap_r.at[k], device_id={"dp": other}, device_id_type=pl.DeviceIdType.MESH
            )

        def size(i):
            return pltpu.make_async_remote_copy(
                src_ref=tile,
                dst_ref=tiles.at[i],
                send_sem=norm_s.at[i],
                recv_sem=norm_r.at[i],
                device_id={"dp": lax.rem(me + i, n)},
                device_id_type=pl.DeviceIdType.MESH,
            )

        lax.fori_loop(1, n, lambda i, _: (size(i).start(), 0)[1], 0)
        swaps = [swap(t.at[:, l, theirs], mom.at[k, core, l], k * layers + l) for k, t in enumerate(moments) for l in range(layers)]
        for copy in swaps:
            copy.start()
        for copy in loads:
            copy.wait()
        for copy in swaps:
            copy.wait()
        lax.fori_loop(1, n, lambda i, _: (size(i).wait(), 0)[1], 0)
        total = lax.fori_loop(0, n, lambda i, total: total + tiles[lax.rem(me - i + n, n)], jnp.zeros((8, 128), F32))
        total = jnp.sum(jnp.sum(total, 0, keepdims=True), 1, keepdims=True)
        factor = jnp.minimum(1.0, 0.5 * lax.rsqrt(total / count + 1e-30))

        def adamw(w, m, v, g):
            g = g * factor
            m = 0.9 * m + 0.1 * g
            v = 0.95 * v + 0.05 * g * g
            return w - 0.02 * (m * lax.rsqrt(v + 1e-8) + 0.1 * w), m, v

        def step_gate_up(layer):
            for gu in range(2):

                def columns(k, _, gu=gu):
                    at = pl.ds(pl.multiple_of(k * PART, PART), PART)
                    if layer == 0:
                        g = gu0[gu, :, at]
                    else:
                        g = gu1[:, pl.ds(pl.multiple_of((2 * k + gu) * PART, PART), PART)]
                    g = g.astype(F32)
                    w = w_gu[gu, layer, :, at].astype(F32)
                    new = []
                    for r in range(2):
                        p = slice(r * moment_rows, (r + 1) * moment_rows)
                        one, m, v = adamw(w[p], mom[gu, r, layer, :, at], mom[2 + gu, r, layer, :, at], g[p])
                        mom[gu, r, layer, :, at] = m
                        mom[2 + gu, r, layer, :, at] = v
                        new.append(one)
                    packs[layer, :, pl.ds(pl.multiple_of(gu * half + k * PART, PART), PART)] = jnp.concatenate(new, 0).astype(BF16)
                    return 0

                lax.fori_loop(0, steps, columns, 0)

        def step_down(layer, p, g):
            new, m, v = adamw(w_d[layer, p, :].astype(F32), mom_d[0, layer, p, :], mom_d[1, layer, p, :], g[p, :].astype(F32))
            mom_d[0, layer, p, :] = m
            mom_d[1, layer, p, :] = v
            return new.astype(BF16)

        def place(color, i, k, whose, part):
            i, k = (lax.rem(t + SIDE, SIDE) for t in (i, k))
            a, b = (i, k) if color == 0 else (k, i)
            return ag.at[a, b, whose, color, :, parts[part]]

        def beside(axis, way):
            to = lax.rem(here[axis] + (1 if way == 0 else SIDE - 1), SIDE)
            a, b = (to, y) if axis == 0 else (x, to)
            return {"dp": (a * SIDE + b) * 2 + core}

        started = {}

        def send(name, color, o, q, part, to):
            index = len(plan) if name not in plan else plan.index(name)
            if name not in plan:
                plan.append(name)
            dst = place(color, here[color] + o, here[1 - color] + q, core, part)
            src = packs.at[color, :, parts[part]] if (o, q) == (0, 0) else dst
            copy = pltpu.make_async_remote_copy(
                src_ref=src, dst_ref=dst, send_sem=sent.at[index], recv_sem=arrived.at[index], device_id=to, device_id_type=pl.DeviceIdType.MESH
            )
            copy.start()
            started[name] = copy

        def along_first(color, way, part):
            send(("a", color, way, part), color, 0, 0, part, beside(color, way))

        def on_first(color, way):
            send(("b", color, way), color, -1 if way == 0 else 1, 0, way, beside(color, way))

        def along_second(color, o, part):
            for way in range(2):
                send(("c", color, way, o, part), color, o, 0, part, beside(1 - color, way))

        def on_second(color, way, o):
            send(("d", color, way, o), color, o, -1 if way == 0 else 1, way, beside(1 - color, way))

        def share(color, o, q, part):
            send(("e", color, o, q, part), color, o, q, part, {"dp": other})

        def own(color):
            for part in range(2):
                for way in range(2):
                    along_first(color, way, part)
            for part in range(2):
                along_second(color, 0, part)
                share(color, 0, 0, part)
            copy = pltpu.make_async_copy(packs.at[color], ag.at[x, y, core, color], load.at[color])
            copy.start()
            return copy

        step_gate_up(0)
        packs[0, :, 2 * half :] = step_down(0, slice(0, rows), d0)
        kept = [own(0)]
        step_gate_up(1)
        packs[1, :, 2 * half :] = step_down(0, slice(rows, 2 * rows), d0)
        kept.append(own(1))
        spare[...] = step_down(1, slice(0, own_rows), d1)

        stores = [
            *[(mom.at[k, core, l], t.at[:, l, mine]) for k, t in enumerate(new_moments) for l in range(layers)],
            (mom_d.at[0], nmd),
            (mom_d.at[1], nvd),
            (spare, wd1),
        ]
        stores = [pltpu.make_async_copy(a, b, load.at[2 + k]) for k, (a, b) in enumerate(stores)]
        backs = [swap(mom.at[k, 1 - core, l], t.at[:, l, mine], 8 + k * layers + l) for k, t in enumerate(new_moments) for l in range(layers)]
        for copy in (*stores, *backs):
            copy.start()

        both = [(color, way) for color in range(2) for way in range(2)]
        for part in range(2):
            for color, way in both:
                started["a", color, way, part].wait_recv()
                if way == part:
                    on_first(color, way)
                o = -1 if way == 0 else 1
                along_second(color, o, part)
                share(color, o, 0, part)

        def arrivals(o):
            for part in range(2):
                for color, way in both:
                    started["c", color, way, o, part].wait_recv()
                    if way == part:
                        on_second(color, way, o)
                    share(color, o, -1 if way == 0 else 1, part)

        arrivals(0)
        for color, way in both:
            started["b", color, way].wait_recv()
            along_second(color, 2, way)
            share(color, 2, 0, way)
        for o in (-1, 1, 2):
            arrivals(o)
        for o in (0, -1, 1, 2):
            for color, way in both:
                started["d", color, way, o].wait_recv()
                share(color, o, 2, way)
        for name, copy in started.items():
            copy.wait_send()
            if name[0] == "e":
                copy.wait_recv()
        for copy in (*kept, *stores, *backs):
            copy.wait()

    m_gate, m_up, v_gate, v_up = (t.transpose(1, 0, 2) for t in (m_gate, m_up, v_gate, v_up))
    anywhere = pl.BlockSpec(memory_space=pl.ANY)
    vmem = pl.BlockSpec(memory_space=pltpu.VMEM)
    packs, last, *moments = call(
        body,
        1e9,
        1e8,
        pair_params(number),
        name="updated_and_gathered",
        in_specs=[vmem] * 4 + [anywhere] * 9,
        out_specs=[anywhere] * 8,
        out_shape=[
            jax.ShapeDtypeStruct((SIDE, SIDE, 2, 2, rows, width), BF16),
            jax.ShapeDtypeStruct((own_rows, d), BF16),
            *[jax.ShapeDtypeStruct(t.shape, F32) for t in (m_gate, m_up, m_down, v_gate, v_up, v_down)],
        ],
        scratch_shapes=[
            pltpu.VMEM((2, layers, rows, half), BF16),
            pltpu.VMEM((layers, own_rows, d), BF16),
            pltpu.VMEM((4, 2, layers, moment_rows, half), F32),
            pltpu.VMEM((2, layers, own_rows, d), F32),
            pltpu.VMEM((2, rows, width), BF16),
            pltpu.VMEM((own_rows, d), BF16),
            pltpu.VMEM((8, 128), F32),
            pltpu.VMEM((n, 8, 128), F32),
            pltpu.SemaphoreType.DMA((13,)),
            pltpu.SemaphoreType.DMA((16,)),
            pltpu.SemaphoreType.DMA((16,)),
            pltpu.SemaphoreType.DMA((n,)),
            pltpu.SemaphoreType.DMA((n,)),
            pltpu.SemaphoreType.DMA((124,)),
            pltpu.SemaphoreType.DMA((124,)),
        ],
    )(gate_up0, gate_up1, down0, down1, w_gate, w_up, w_down, m_gate, m_up, m_down, v_gate, v_up, v_down)
    return packs, last, *moments


def placed(packs, layers, d, ff):
    rows, width = packs.shape[-2:]
    half = ff // 2
    per = 2

    def body(t, gate, up, down):
        for b in range(per):
            for core in range(2):
                for color in range(2):
                    r = slice(b * rows, (b + 1) * rows)
                    c = slice(core * half, (core + 1) * half)
                    gate[color, r, c] = t[b, core, color, :, :half]
                    up[color, r, c] = t[b, core, color, :, half : 2 * half]
                    at = ((b * 2 + core) * 2 + color) * rows
                    down[at : at + rows, :] = t[b, core, color, :, 2 * half :]

    n = SIDE // per
    out = pl.BlockSpec((layers, per * rows, ff), lambda i, j: (0, i * n + j, 0))
    return call(
        body,
        1,
        4 * packs.size,
        name="placed",
        grid=(SIDE, n),
        in_specs=[pl.BlockSpec((None, per, 2, 2, rows, width), lambda i, j: (i, j, 0, 0, 0, 0))],
        out_specs=[out, out, pl.BlockSpec((None, per * 4 * rows, d), lambda i, j: (0, i * n + j, 0))],
        out_shape=[jax.ShapeDtypeStruct((layers, d, ff), BF16)] * 2 + [jax.ShapeDtypeStruct((layers, ff, d), BF16)],
    )(packs)


def copied(*arrays):
    steps = 4

    def body(*refs):
        for a, b in zip(refs[: len(arrays)], refs[len(arrays) :], strict=True):
            b[...] = a[...]

    specs = [pl.BlockSpec((t.shape[0] // steps, *t.shape[1:]), lambda i: (i, 0, 0)) for t in arrays]
    return call(
        body,
        1,
        sum(8 * t.size for t in arrays),
        name="copied",
        grid=(steps,),
        in_specs=specs,
        out_specs=specs,
        out_shape=[jax.ShapeDtypeStruct(t.shape, t.dtype) for t in arrays],
    )(*arrays)


def placed_last(down, gathered):
    layers, ff, d = down.shape
    bm = 1152

    def body(down, t, out):
        out[...] = t[...]

    return call(
        body,
        1,
        4 * gathered.size,
        name="placed_last",
        grid=(ff // bm,),
        in_specs=[pl.BlockSpec(memory_space=pl.ANY), pl.BlockSpec((bm, d), lambda i: (i, 0))],
        out_specs=pl.BlockSpec((None, bm, d), lambda i: (layers - 1, i, 0)),
        out_shape=jax.ShapeDtypeStruct(down.shape, BF16),
        input_output_aliases={0: 0},
    )(down, gathered)


def solution(mesh):
    chips = mesh.shape["dp"] // 2
    same_core = [[2 * chip + core for chip in range(chips)] for core in range(2)]

    def summed(part):
        return lax.psum_scatter(part, "dp", scatter_dimension=0, axis_index_groups=same_core, tiled=True)

    def step(x, dy, w_gate, w_up, w_down, *moments):
        x, dy = x[0], dy[0]
        layers, d, ff = w_gate.shape

        gate, up, hid0, a0_t = hidden_forward(0, x, w_gate, w_up)
        h1, a1, a1_t = down_forward(0, x, hid0, w_down)
        hid1, dg1, du1 = last_layer(1, a1, dy, w_gate, w_up, w_down)
        gate_up1 = gate_up_gradient(1, 0, ff // (2 * PART), a1_t, dg1, du1)
        hid1, gate_up1 = lax.optimization_barrier((hid1, gate_up1))
        gate_up1 = summed(gate_up1)
        down1 = down_gradient(2, hid1, dy)
        dg1, du1, down1 = lax.optimization_barrier((dg1, du1, down1))
        down1 = summed(down1)
        dh = states_cotangent(1, h1, dy, dg1, du1, w_gate, w_up)
        down0 = down_gradient(3, hid0, dh)
        dh, down0 = lax.optimization_barrier((dh, down0))
        down0 = summed(down0)
        gate_up0 = first_layer_gradient(4, 0, a0_t, dh, gate, up, w_down)
        gate_up0, gate_up1 = lax.optimization_barrier((gate_up0, gate_up1))
        gate_up1, down1 = lax.optimization_barrier((gate_up1, down1))
        down1, down0 = lax.optimization_barrier((down1, down0))
        packs, last, *moments = updated_and_gathered(5, gate_up0, gate_up1, down0, down1, w_gate, w_up, w_down, *moments)
        last = lax.all_gather(last, "dp", tiled=True)
        new_gate, new_up, new_down = placed(packs, layers, d, ff)
        down_moments = [t.reshape(-1, t.shape[1] // 2, d) for t in moments[2::3]]
        moments = copied(*(t for k, t in enumerate(moments) if k % 3 < 2), *down_moments)
        down_moments = [t.reshape(layers, -1, d) for t in moments[4:]]
        moments = [t.transpose(1, 0, 2) for t in moments[:4]]
        moments = [*moments[:2], down_moments[0], *moments[2:], down_moments[1]]
        new_down = placed_last(new_down, last)
        return new_gate, new_up, new_down, *moments

    sequences = P(("rep", "dp"))
    return jax.shard_map(
        step,
        mesh=mesh,
        in_specs=(sequences, sequences, P(), P(), P(), *[P(None, "dp")] * 6),
        out_specs=(P("rep"), P("rep"), P("rep"), *[P("rep", "dp")] * 6),
        check_vma=False,
    )
```

```python
import functools
import math

import jax
import jax.numpy as jnp
from jax import lax
from jax.experimental import pallas as pl
from jax.experimental.pallas import tpu as pltpu
from jax.sharding import PartitionSpec as P

F32, BF16 = jnp.float32, jnp.bfloat16
VMEM_LIMIT = 67_043_328
NN = (((1,), (0,)), ((), ()))
NT = (((1,), (1,)), ((), ()))
TN = (((0,), (0,)), ((), ()))


def dot(a, b, dims=NN):
    return lax.dot_general(a, b, dims, preferred_element_type=F32)


def sigmoid(x):
    return 1.0 / (1.0 + jnp.exp(-x))


def whole(shape):
    return pl.BlockSpec(shape, lambda *_: (0,) * len(shape), pipeline_mode=pl.Buffered(1))


def call(body, flops, moved, params=None, **kw):
    return pl.pallas_call(
        body,
        cost_estimate=pl.CostEstimate(flops=int(flops), bytes_accessed=int(moved), transcendentals=0),
        compiler_params=pltpu.CompilerParams(**{"vmem_limit_bytes": VMEM_LIMIT, **(params or {})}),
        **kw,
    )


def row_scale(wide):
    return lax.rsqrt(jnp.mean(wide * wide, -1, keepdims=True) + 1e-6)


def hidden_forward(layer, x, w_gate, w_up):
    tokens, d = x.shape
    ff = w_gate.shape[-1]
    bf, bm = 256, 512
    n = tokens // bm

    def body(x, wg, wu, gate, up, hid, a_t, x_in, a, came):
        j = pl.program_id(0)

        def rows(i):
            return pl.ds(pl.multiple_of(i * bm, bm), bm)

        def come(i):
            return pltpu.make_async_copy(x.at[rows(i)], x_in.at[rows(i)], came.at[i])

        def chunk(r):
            g, u = dot(a[r, :], wg[...]), dot(a[r, :], wu[...])
            gate[r, :] = g
            up[r, :] = u
            hid[r, :] = (g * sigmoid(g) * u).astype(BF16)

        @pl.when(j == 0)
        def _():
            for i in range(n):
                come(i).start()

            def first(i, _):
                come(i).wait()
                wide = x_in[rows(i), :].astype(F32)
                unit = wide * row_scale(wide)
                a[rows(i), :] = unit.astype(BF16)
                a_t[:, rows(i)] = unit.T.astype(BF16)
                chunk(rows(i))
                return 0

            lax.fori_loop(0, n, first, 0)

        @pl.when(j > 0)
        def _():
            for i in range(n):
                chunk(slice(i * bm, (i + 1) * bm))

    w_spec = pl.BlockSpec((None, d, bf), lambda j: (layer, 0, j))
    o_spec = pl.BlockSpec((tokens, bf), lambda j: (0, j))
    wide = jax.ShapeDtypeStruct((tokens, ff), F32)
    return call(
        body,
        4 * tokens * d * ff,
        10 * tokens * ff + 4 * d * ff,
        name="hidden_forward",
        grid=(ff // bf,),
        in_specs=[pl.BlockSpec(memory_space=pl.ANY), w_spec, w_spec],
        out_specs=[*[o_spec] * 3, whole((d, tokens))],
        out_shape=(wide, wide, jax.ShapeDtypeStruct((tokens, ff), BF16), jax.ShapeDtypeStruct((d, tokens), BF16)),
        scratch_shapes=[pltpu.VMEM((tokens, d), BF16), pltpu.VMEM((tokens, d), BF16), pltpu.SemaphoreType.DMA((n,))],
    )(x, w_gate, w_up)


def down_forward(layer, x, hid, w_down):
    tokens, ff = hid.shape
    d = x.shape[-1]
    bm = 256

    def body(x, hid, wd, h1, a1, a1_t):
        h = (x[...].astype(F32) + dot(hid[...], wd[...]).astype(BF16).astype(F32)).astype(BF16)
        h1[...] = h
        wide = h.astype(F32)
        unit = wide * row_scale(wide)
        a1[...] = unit.astype(BF16)
        a1_t[...] = unit.T.astype(BF16)

    rows = pl.BlockSpec((bm, d), lambda i: (i, 0))
    out = jax.ShapeDtypeStruct((tokens, d), BF16)
    return call(
        body,
        2 * tokens * d * ff,
        2 * tokens * ff + 2 * d * ff,
        name="down_forward",
        grid=(tokens // bm,),
        in_specs=[
            rows,
            pl.BlockSpec((bm, ff), lambda i: (i, 0)),
            pl.BlockSpec((None, ff, d), lambda i: (layer, 0, 0), pipeline_mode=pl.Buffered(1)),
        ],
        out_specs=[rows, rows, pl.BlockSpec((d, bm), lambda i: (0, i))],
        out_shape=(out, out, jax.ShapeDtypeStruct((d, tokens), BF16)),
    )(x, hid, w_down)


def gate_up_cotangents(g, u, dh):
    dh = dh.astype(BF16).astype(F32)
    s = sigmoid(g)
    silu = g * s
    return (dh * u * (s + silu * (1.0 - s))).astype(BF16), (dh * silu).astype(BF16), (silu * u).astype(BF16)


def last_layer(layer, a, dy, w_gate, w_up, w_down):
    tokens, d = a.shape
    ff = w_gate.shape[-1]
    bf, bm = 256, 512

    def body(a, dy, wg, wu, wd, hid, dg, du):
        for i in range(tokens // bm):
            r = slice(i * bm, (i + 1) * bm)
            g, u = dot(a[r, :], wg[...]), dot(a[r, :], wu[...])
            dg[r, :], du[r, :], hid[r, :] = gate_up_cotangents(g, u, dot(dy[r, :], wd[...], NT))

    w_spec = pl.BlockSpec((None, d, bf), lambda j: (layer, 0, j))
    o_spec = pl.BlockSpec((tokens, bf), lambda j: (0, j))
    out = jax.ShapeDtypeStruct((tokens, ff), BF16)
    return call(
        body,
        6 * tokens * d * ff,
        6 * tokens * ff + 6 * d * ff,
        name="last_layer",
        grid=(ff // bf,),
        in_specs=[whole((tokens, d)), whole((tokens, d)), w_spec, w_spec, pl.BlockSpec((None, bf, d), lambda j: (layer, j, 0))],
        out_specs=[o_spec] * 3,
        out_shape=(out, out, out),
    )(a, dy, w_gate, w_up, w_down)


def states_cotangent(layer, h, dy, dg, du, w_gate, w_up):
    tokens, ff = dg.shape
    d = h.shape[-1]
    bm, bk = 256, 512
    n = ff // bk

    def body(h, dy, dg, du, wg, wu, out, w, total, came):
        def k(c):
            return pl.ds(pl.multiple_of(c * bk, bk), bk)

        def come(c):
            return [pltpu.make_async_copy(t.at[layer, :, k(c)], w.at[i, :, k(c)], came.at[i, c]) for i, t in enumerate((wg, wu))]

        def rest(da):
            wide = h[...].astype(F32)
            da = da.astype(BF16).astype(F32)
            s = row_scale(wide)
            back = da * s - wide * (s * s * s * jnp.mean(da * wide, -1, keepdims=True))
            out[...] = (dy[...].astype(F32) + back).astype(BF16)

        @pl.when(pl.program_id(0) == 0)
        def _():
            for c in range(n):
                for copy in come(c):
                    copy.start()
            total[...] = jnp.zeros_like(total)

            def add(c, _):
                for copy in come(c):
                    copy.wait()
                total[...] += dot(dg[:, k(c)], w[0, :, k(c)], NT) + dot(du[:, k(c)], w[1, :, k(c)], NT)
                return 0

            lax.fori_loop(0, n, add, 0)
            rest(total[...])

        @pl.when(pl.program_id(0) > 0)
        def _():
            rest(dot(dg[...], w[0], NT) + dot(du[...], w[1], NT))

    rows = pl.BlockSpec((bm, d), lambda i: (i, 0))
    wide_rows = pl.BlockSpec((bm, ff), lambda i: (i, 0))
    anywhere = pl.BlockSpec(memory_space=pl.ANY)
    return call(
        body,
        4 * tokens * d * ff,
        4 * tokens * ff + 4 * d * ff,
        name="states_cotangent",
        grid=(tokens // bm,),
        in_specs=[rows, rows, wide_rows, wide_rows, anywhere, anywhere],
        out_specs=rows,
        out_shape=jax.ShapeDtypeStruct((tokens, d), BF16),
        scratch_shapes=[pltpu.VMEM((2, d, ff), BF16), pltpu.VMEM((bm, d), F32), pltpu.SemaphoreType.DMA((2, n))],
    )(h, dy, dg, du, w_gate, w_up)


SLOTS, ARRIVALS = 3, 4


def pair_scratch(rows, columns):
    return [
        pltpu.VMEM((SLOTS, 2, rows, columns), BF16),
        pltpu.VMEM((ARRIVALS, rows, columns), BF16),
        pltpu.SemaphoreType.DMA((SLOTS,)),
        pltpu.SemaphoreType.DMA((ARRIVALS,)),
    ]


def pair_step(n, make, put, made, came, sent, arrived):
    j = pl.program_id(0)
    me = lax.axis_index("dp")
    core = lax.rem(me, 2)
    other = me + 1 - 2 * core

    def transfer(step):
        slot, place = lax.rem(step, SLOTS), lax.rem(step, ARRIVALS)
        return pltpu.make_async_remote_copy(
            src_ref=made.at[slot, 1 - core],
            dst_ref=came.at[place],
            send_sem=sent.at[slot],
            recv_sem=arrived.at[place],
            device_id={"dp": other},
            device_id_type=pl.DeviceIdType.MESH,
        )

    @pl.when(j == 0)
    def _():
        barrier = pltpu.get_barrier_semaphore()
        pl.semaphore_signal(barrier, inc=1, device_id={"dp": other}, device_id_type=pl.DeviceIdType.MESH)
        pl.semaphore_wait(barrier, 1)

    @pl.when(j >= 2)
    def _():
        transfer(j - 2).wait()
        own = made[lax.rem(j - 2, SLOTS), core]
        put(own.astype(F32) + came[lax.rem(j - 2, ARRIVALS)].astype(F32))

    @pl.when(j < n)
    def _():
        make(made.at[lax.rem(j, SLOTS)])
        transfer(j).start()


def pair_params(number):
    return {"collective_id": number, "has_side_effects": True}


def down_gradient(number, hid, dy, joint=None):
    tokens, ff = hid.shape
    d = dy.shape[-1]
    chips = lax.axis_size("dp") // 2
    own = ff // (2 * chips)
    bf = 1152
    n, per = ff // bf, bf // (2 * own)

    def body(hid, dy, *rest):
        out, *scratch = rest[0 if joint is None else 1 :]

        def make(slot):
            block = dot(hid[...], dy[...], TN)
            for i in range(per):
                for half in range(2):
                    at = (2 * i + half) * own
                    slot[half, i * own : (i + 1) * own, :] = block[at : at + own].astype(BF16)

        def put(total):
            if joint is None:
                out[...] = total.astype(BF16)
            else:
                for i in range(per):
                    for half in range(2):
                        at = i * own + half * (own // 2)
                        out[i, :, half * d : (half + 1) * d] = total[at : at + own // 2].astype(BF16)

        pair_step(n, make, put, *scratch)

    if joint is None:
        more, out_shape = [], jax.ShapeDtypeStruct((ff // 2, d), BF16)
        out_spec = pl.BlockSpec((bf // 2, d), lambda j: (jnp.maximum(j - 2, 0), 0))
    else:
        more, out_shape = [joint], jax.ShapeDtypeStruct(joint.shape, BF16)
        out_spec = pl.BlockSpec((per, None, own // 2, 2 * d), lambda j: (jnp.maximum(j - 2, 0), 2, 0, 0))
    return call(
        body,
        2 * tokens * d * ff,
        2 * tokens * ff + d * ff,
        pair_params(number),
        name=f"down_gradient_{number}",
        grid=(n + 2,),
        in_specs=[
            pl.BlockSpec((tokens, bf), lambda j: (0, jnp.minimum(j, n - 1))),
            whole((tokens, d)),
            *[pl.BlockSpec(memory_space=pl.ANY) for _ in more],
        ],
        out_specs=out_spec,
        out_shape=out_shape,
        scratch_shapes=pair_scratch(bf // 2, d),
        input_output_aliases={2: 0} if more else {},
    )(hid, dy, *more)


PART = 256


def halves_specs(shape, first, n, half, layer=None, transposed=False):
    def spec(h):
        def at(j):
            k = h * half + first + jnp.minimum(j, n - 1)
            index = (k, 0) if transposed else (0, k)
            return index if layer is None else (layer, *index)

        return pl.BlockSpec(shape, at)

    return [spec(0), spec(1)]


def gate_up_gradient(number, a_t, dg, du):
    d, tokens = a_t.shape
    half = dg.shape[-1] // (2 * PART)
    n = half
    chips = lax.axis_size("dp") // 2
    rows = d // chips

    def body(a_t, dg0, dg1, du0, du1, out, *scratch):
        def make(slot):
            for h, (dg, du) in enumerate(((dg0, du0), (dg1, du1))):
                slot[h, :, :PART] = dot(a_t[...], dg[...]).astype(BF16)
                slot[h, :, PART:] = dot(a_t[...], du[...]).astype(BF16)

        def put(total):
            for k in range(chips):
                for i in range(2):
                    out[k, i] = total[k * rows : (k + 1) * rows, i * PART : (i + 1) * PART].astype(BF16)

        pair_step(n, make, put, *scratch)

    t_specs = halves_specs((tokens, PART), 0, n, half)
    return call(
        body,
        8 * tokens * d * PART * n,
        8 * tokens * PART * n,
        pair_params(number),
        name=f"gate_up_gradient_{number}",
        grid=(n + 2,),
        in_specs=[whole((d, tokens)), *t_specs, *t_specs],
        out_specs=pl.BlockSpec((chips, 2, rows, PART), lambda j: (0, 0, 0, jnp.maximum(j - 2, 0))),
        out_shape=jax.ShapeDtypeStruct((chips, 3, rows, PART * n), BF16),
        scratch_shapes=pair_scratch(d, 2 * PART),
    )(a_t, dg, dg, du, du)


SIDE = 4
PLACES = 4


def first_layer_gradient(number, layer, a_t, dy, gate, up, w_down):
    d, tokens = a_t.shape
    half = gate.shape[-1] // (2 * PART)
    n = half
    bm = 512
    rows = d // SIDE**2
    mid = PART // 2

    def body(a_t, dy, g0, g1, u0, u1, w0, w1, out, dg, du, made, came, sums, across1, pass1, got1, total1, across2, pass2, got2, ps, pr, sent, arrived):
        j = pl.program_id(0)
        me = lax.axis_index("dp")
        core = lax.rem(me, 2)
        other = me + 1 - 2 * core
        x, y = lax.div(me, 2 * SIDE), lax.rem(lax.div(me, 2), SIDE)

        def at(x, y):
            return {"dp": (x * SIDE + y) * 2 + core}

        def beside(axis, way):
            to = lax.rem((x if axis == 0 else y) + (1 if way == 0 else SIDE - 1), SIDE)
            return at(to, y) if axis == 0 else at(x, to)

        here = (x, y)

        def transfer(stage, color, way, block):
            place = lax.rem(block, PLACES)
            first, second = color, 1 - color
            columns = slice(color * PART, (color + 1) * PART)
            if stage == 1:
                far = lax.rem(here[first] + 2, SIDE)
                part = slice(2 * way, 2 * way + 2)
                src = sums.at[place, far, part, :, columns] if color == 0 else sums.at[place, part, far, :, columns]
                dst = across1.at[color, place, way]
            elif stage == 2:
                src, dst = pass1.at[color, lax.rem(block, 2), way], got1.at[color, place, way]
            elif stage == 3:
                far = lax.rem(here[second] + 2, SIDE)
                src = total1.at[color, place, far, :, slice(way * mid, (way + 1) * mid)]
                dst = across2.at[color, place, way]
            else:
                src, dst = pass2.at[color, place, way], got2.at[color, place, way]
            index = ((stage - 1) * 2 + color) * 2 + way
            return pltpu.make_async_remote_copy(
                src_ref=src,
                dst_ref=dst,
                send_sem=sent.at[index, place],
                recv_sem=arrived.at[index, place],
                device_id=beside(first if stage <= 2 else second, way),
                device_id_type=pl.DeviceIdType.MESH,
            )

        def swap(block):
            slot, place = lax.rem(block, SLOTS), lax.rem(block, PLACES)
            return pltpu.make_async_remote_copy(
                src_ref=made.at[slot, 1 - core],
                dst_ref=came.at[place],
                send_sem=ps.at[slot],
                recv_sem=pr.at[place],
                device_id={"dp": other},
                device_id_type=pl.DeviceIdType.MESH,
            )

        def of(color, place, i):
            columns = slice(color * PART, (color + 1) * PART)
            t = sums[place, i, :, :, columns] if color == 0 else sums[place, :, i, :, columns]
            return t.astype(F32)

        def stage(lag, act):
            @pl.when((j >= lag) & (j < n + lag))
            def _():
                act(j - lag)

        @pl.when(j == 0)
        def _():
            barrier = pltpu.get_barrier_semaphore()
            for peer in ({"dp": other}, beside(0, 0), beside(0, 1), beside(1, 0), beside(1, 1)):
                pl.semaphore_signal(barrier, inc=1, device_id=peer, device_id_type=pl.DeviceIdType.MESH)
            pl.semaphore_wait(barrier, 5)

        def last(block):
            place = lax.rem(block, PLACES)
            for color in range(2):
                for way in range(2):
                    transfer(4, color, way, block).wait()
                b = here[1 - color]
                t = total1[color, place, b].astype(F32) + got2[color, place, 0].astype(F32) + got2[color, place, 1].astype(F32)
                out[color] = t.astype(BF16)

        def fourth(block):
            place = lax.rem(block, PLACES)
            for color in range(2):
                for way in range(2):
                    transfer(3, color, way, block).wait()
                for way in range(2):
                    b = lax.rem(here[1 - color] + (1 if way == 0 else SIDE - 1), SIDE)
                    pass2[color, place, way] = total1[color, place, b]
                    c = slice(way * mid, (way + 1) * mid)
                    more = total1[color, place, b, :, c].astype(F32) + across2[color, place, way].astype(F32)
                    pass2[color, place, way, :, c] = more.astype(BF16)
                    transfer(4, color, way, block).start()

        def third(block):
            place = lax.rem(block, PLACES)
            for color in range(2):
                for way in range(2):
                    transfer(2, color, way, block).wait()
                t = of(color, place, here[color]) + got1[color, place, 0].astype(F32) + got1[color, place, 1].astype(F32)
                total1[color, place] = t.astype(BF16)
                for way in range(2):
                    transfer(3, color, way, block).start()

        def second(block):
            place = lax.rem(block, PLACES)
            for color in range(2):
                for way in range(2):
                    transfer(1, color, way, block).wait()
                for way in range(2):
                    t = of(color, place, lax.rem(here[color] + (1 if way == 0 else SIDE - 1), SIDE))
                    p = slice(2 * way, 2 * way + 2)
                    q = slice(2 - 2 * way, 4 - 2 * way)
                    pass1[color, lax.rem(block, 2), way, p] = (t[p] + across1[color, place, way].astype(F32)).astype(BF16)
                    pass1[color, lax.rem(block, 2), way, q] = t[q].astype(BF16)
                    transfer(2, color, way, block).start()

        def first(block):
            place, slot = lax.rem(block, PLACES), lax.rem(block, SLOTS)
            swap(block).wait()
            for k in range(SIDE**2):
                r = slice(k * rows, (k + 1) * rows)
                t = made[slot, core, r, :].astype(F32) + came[place, r, :].astype(F32)
                sums[place, k // SIDE, k % SIDE] = t.astype(BF16)
            for color in range(2):
                for way in range(2):
                    transfer(1, color, way, block).start()

        def make(block):
            slot = lax.rem(block, SLOTS)
            for h, (g, u, w) in enumerate(((g0, u0, w0), (g1, u1, w1))):
                for i in range(tokens // bm):
                    r = slice(i * bm, (i + 1) * bm)
                    dg[h, r, :], du[h, r, :], _ = gate_up_cotangents(g[r, :], u[r, :], dot(dy[r, :], w[...], NT))
                made[slot, h, :, :PART] = dot(a_t[...], dg[h]).astype(BF16)
                made[slot, h, :, PART:] = dot(a_t[...], du[h]).astype(BF16)
            swap(block).start()

        stage(8, last)
        stage(7, fourth)
        stage(6, third)
        stage(4, second)
        stage(2, first)
        stage(0, make)

    t_specs = halves_specs((tokens, PART), 0, n, half)
    block = (SIDE, rows, PART)
    return call(
        body,
        12 * tokens * d * PART * n,
        16 * tokens * PART * n,
        pair_params(number),
        name="first_layer_gradient",
        grid=(n + 8,),
        in_specs=[whole((d, tokens)), whole((tokens, d)), *t_specs, *t_specs, *halves_specs((None, PART, d), 0, n, half, layer, True)],
        out_specs=pl.BlockSpec((2, rows, PART), lambda j: (0, 0, jnp.maximum(j - 8, 0))),
        out_shape=jax.ShapeDtypeStruct((2, rows, PART * n), BF16),
        scratch_shapes=[
            pltpu.VMEM((2, tokens, PART), BF16),
            pltpu.VMEM((2, tokens, PART), BF16),
            pltpu.VMEM((SLOTS, 2, d, 2 * PART), BF16),
            pltpu.VMEM((PLACES, d, 2 * PART), BF16),
            pltpu.VMEM((PLACES, SIDE, SIDE, rows, 2 * PART), BF16),
            pltpu.VMEM((2, PLACES, 2, SIDE // 2, rows, PART), BF16),
            pltpu.VMEM((2, 2, 2, *block), BF16),
            pltpu.VMEM((2, PLACES, 2, *block), BF16),
            pltpu.VMEM((2, PLACES, *block), BF16),
            pltpu.VMEM((2, PLACES, 2, rows, mid), BF16),
            pltpu.VMEM((2, PLACES, 2, rows, PART), BF16),
            pltpu.VMEM((2, PLACES, 2, rows, PART), BF16),
            pltpu.SemaphoreType.DMA((SLOTS,)),
            pltpu.SemaphoreType.DMA((PLACES,)),
            pltpu.SemaphoreType.DMA((16, PLACES)),
            pltpu.SemaphoreType.DMA((16, PLACES)),
        ],
    )(a_t, dy, gate, gate, up, up, w_down, w_down)


def updated_and_gathered(number, gate_up0, down0, last_layer, w_gate, w_up, w_down, m_gate, m_up, m_down, v_gate, v_up, v_down):
    n = lax.axis_size("dp")
    layers, d, ff = w_gate.shape
    rows, half = gate_up0.shape[1:]
    own_rows, moment_rows = ff // n, d // n
    steps = half // PART
    width = 2 * half + d
    cut = -(-width // 256) * 128
    count = 3 * layers * d * ff
    parts = (slice(0, cut), slice(cut, width))
    plan = []

    def body(gu0, d0, gu1, wg, wu, wd, mg, mu, md, vg, vu, vd, ag, wd1, nmg, nmu, nmd, nvg, nvu, nvd,
             w_gu, w_d, mom, mom_d, packs, spare, tile, tiles, load, swap_s, swap_r, norm_s, norm_r, sent, arrived):
        me = lax.axis_index("dp")
        core = lax.rem(me, 2)
        other = me + 1 - 2 * core
        chip = lax.div(me, 2)
        x, y = lax.div(chip, SIDE), lax.rem(chip, SIDE)
        here = (x, y)
        mine, theirs = (pl.ds(pl.multiple_of(c * half, 128), half) for c in (core, 1 - core))

        moments = (mg, mu, vg, vu)
        new_moments = (nmg, nmu, nvg, nvu)
        loads = [
            *[(t.at[:, l, mine], mom.at[k, core, l]) for k, t in enumerate(moments) for l in range(layers)],
            (md, mom_d.at[0]),
            (vd, mom_d.at[1]),
            (wg.at[:, pl.ds(pl.multiple_of(chip * rows, 8), rows), mine], w_gu.at[0]),
            (wu.at[:, pl.ds(pl.multiple_of(chip * rows, 8), rows), mine], w_gu.at[1]),
            (wd.at[:, pl.ds(pl.multiple_of(me * own_rows, 16), own_rows), :], w_d),
        ]
        loads = [pltpu.make_async_copy(a, b, load.at[k]) for k, (a, b) in enumerate(loads)]
        for copy in loads:
            copy.start()

        barrier = pltpu.get_barrier_semaphore()

        def greet(i, _):
            pl.semaphore_signal(barrier, inc=1, device_id={"dp": lax.rem(me + i, n)}, device_id_type=pl.DeviceIdType.MESH)
            return 0

        lax.fori_loop(1, n, greet, 0)

        def square(t):
            t = t.astype(F32)
            t = t * t
            return sum(t[k * 8 : (k + 1) * 8] for k in range(t.shape[0] // 8))

        def squares(k, total):
            at = pl.ds(pl.multiple_of(k * PART, PART), PART)
            return total + sum(square(gu0[i, :, at]) for i in range(2)) + sum(square(gu1[i, :, at]) for i in range(3))

        total = lax.fori_loop(0, steps, squares, jnp.zeros((8, PART), F32))
        downs = square(d0[...])
        total = total[:, :128] + total[:, 128:] + sum(downs[:, k * 128 : (k + 1) * 128] for k in range(d // 128))
        tile[...] = total
        tiles[0] = total

        pl.semaphore_wait(barrier, n - 1)

        def swap(src, dst, k):
            return pltpu.make_async_remote_copy(
                src_ref=src, dst_ref=dst, send_sem=swap_s.at[k], recv_sem=swap_r.at[k], device_id={"dp": other}, device_id_type=pl.DeviceIdType.MESH
            )

        def size(i):
            return pltpu.make_async_remote_copy(
                src_ref=tile,
                dst_ref=tiles.at[i],
                send_sem=norm_s.at[i],
                recv_sem=norm_r.at[i],
                device_id={"dp": lax.rem(me + i, n)},
                device_id_type=pl.DeviceIdType.MESH,
            )

        lax.fori_loop(1, n, lambda i, _: (size(i).start(), 0)[1], 0)
        swaps = [swap(t.at[:, l, theirs], mom.at[k, core, l], k * layers + l) for k, t in enumerate(moments) for l in range(layers)]
        for copy in swaps:
            copy.start()
        for copy in loads:
            copy.wait()
        for copy in swaps:
            copy.wait()
        lax.fori_loop(1, n, lambda i, _: (size(i).wait(), 0)[1], 0)
        total = lax.fori_loop(0, n, lambda i, total: total + tiles[lax.rem(me - i + n, n)], jnp.zeros((8, 128), F32))
        total = jnp.sum(jnp.sum(total, 0, keepdims=True), 1, keepdims=True)
        factor = jnp.minimum(1.0, 0.5 * lax.rsqrt(total / count + 1e-30))

        def adamw(w, m, v, g):
            g = g * factor
            m = 0.9 * m + 0.1 * g
            v = 0.95 * v + 0.05 * g * g
            return w - 0.02 * (m * lax.rsqrt(v + 1e-8) + 0.1 * w), m, v

        def step_gate_up(layer):
            for gu in range(2):

                def columns(k, _, gu=gu):
                    at = pl.ds(pl.multiple_of(k * PART, PART), PART)
                    g = (gu0, gu1)[layer][gu, :, at].astype(F32)
                    w = w_gu[gu, layer, :, at].astype(F32)
                    new = []
                    for r in range(2):
                        p = slice(r * moment_rows, (r + 1) * moment_rows)
                        one, m, v = adamw(w[p], mom[gu, r, layer, :, at], mom[2 + gu, r, layer, :, at], g[p])
                        mom[gu, r, layer, :, at] = m
                        mom[2 + gu, r, layer, :, at] = v
                        new.append(one)
                    packs[layer, :, pl.ds(pl.multiple_of(gu * half + k * PART, PART), PART)] = jnp.concatenate(new, 0).astype(BF16)
                    return 0

                lax.fori_loop(0, steps, columns, 0)

        def step_down(layer, p, g):
            new, m, v = adamw(w_d[layer, p, :].astype(F32), mom_d[0, layer, p, :], mom_d[1, layer, p, :], g.astype(F32))
            mom_d[0, layer, p, :] = m
            mom_d[1, layer, p, :] = v
            return new.astype(BF16)

        def place(color, i, k, whose, part):
            i, k = (lax.rem(t + SIDE, SIDE) for t in (i, k))
            a, b = (i, k) if color == 0 else (k, i)
            return ag.at[a, b, whose, color, :, parts[part]]

        def beside(axis, way):
            to = lax.rem(here[axis] + (1 if way == 0 else SIDE - 1), SIDE)
            a, b = (to, y) if axis == 0 else (x, to)
            return {"dp": (a * SIDE + b) * 2 + core}

        started = {}

        def send(name, color, o, q, part, to):
            index = len(plan) if name not in plan else plan.index(name)
            if name not in plan:
                plan.append(name)
            dst = place(color, here[color] + o, here[1 - color] + q, core, part)
            src = packs.at[color, :, parts[part]] if (o, q) == (0, 0) else dst
            copy = pltpu.make_async_remote_copy(
                src_ref=src, dst_ref=dst, send_sem=sent.at[index], recv_sem=arrived.at[index], device_id=to, device_id_type=pl.DeviceIdType.MESH
            )
            copy.start()
            started[name] = copy

        def along_first(color, way, part):
            send(("a", color, way, part), color, 0, 0, part, beside(color, way))

        def on_first(color, way):
            send(("b", color, way), color, -1 if way == 0 else 1, 0, way, beside(color, way))

        def along_second(color, o, part):
            for way in range(2):
                send(("c", color, way, o, part), color, o, 0, part, beside(1 - color, way))

        def on_second(color, way, o):
            send(("d", color, way, o), color, o, -1 if way == 0 else 1, way, beside(1 - color, way))

        def share(color, o, q, part):
            send(("e", color, o, q, part), color, o, q, part, {"dp": other})

        def own(color):
            for part in range(2):
                for way in range(2):
                    along_first(color, way, part)
            for part in range(2):
                along_second(color, 0, part)
                share(color, 0, 0, part)
            copy = pltpu.make_async_copy(packs.at[color], ag.at[x, y, core, color], load.at[color])
            copy.start()
            return copy

        step_gate_up(0)
        packs[0, :, 2 * half :] = step_down(0, slice(0, rows), d0[:rows])
        kept = [own(0)]
        step_gate_up(1)
        packs[1, :, 2 * half :] = step_down(0, slice(rows, 2 * rows), d0[rows:])
        kept.append(own(1))
        for i in range(2):
            p = slice(i * rows, (i + 1) * rows)
            spare[p] = step_down(1, p, gu1[2, :, i * d : (i + 1) * d])

        stores = [
            *[(mom.at[k, core, l], t.at[:, l, mine]) for k, t in enumerate(new_moments) for l in range(layers)],
            (mom_d.at[0], nmd),
            (mom_d.at[1], nvd),
            (spare, wd1),
        ]
        stores = [pltpu.make_async_copy(a, b, load.at[2 + k]) for k, (a, b) in enumerate(stores)]
        backs = [swap(mom.at[k, 1 - core, l], t.at[:, l, mine], 8 + k * layers + l) for k, t in enumerate(new_moments) for l in range(layers)]
        for copy in (*stores, *backs):
            copy.start()

        both = [(color, way) for color in range(2) for way in range(2)]
        for part in range(2):
            for color, way in both:
                started["a", color, way, part].wait_recv()
                if way == part:
                    on_first(color, way)
                o = -1 if way == 0 else 1
                along_second(color, o, part)
                share(color, o, 0, part)

        def arrivals(o):
            for part in range(2):
                for color, way in both:
                    started["c", color, way, o, part].wait_recv()
                    if way == part:
                        on_second(color, way, o)
                    share(color, o, -1 if way == 0 else 1, part)

        arrivals(0)
        for color, way in both:
            started["b", color, way].wait_recv()
            along_second(color, 2, way)
            share(color, 2, 0, way)
        for o in (-1, 1, 2):
            arrivals(o)
        for o in (0, -1, 1, 2):
            for color, way in both:
                started["d", color, way, o].wait_recv()
                share(color, o, 2, way)
        for name, copy in started.items():
            copy.wait_send()
            if name[0] == "e":
                copy.wait_recv()
        for copy in (*kept, *stores, *backs):
            copy.wait()

    m_gate, m_up, v_gate, v_up = (t.transpose(1, 0, 2) for t in (m_gate, m_up, v_gate, v_up))
    anywhere = pl.BlockSpec(memory_space=pl.ANY)
    vmem = pl.BlockSpec(memory_space=pltpu.VMEM)
    packs, last, *moments = call(
        body,
        1e9,
        1e8,
        pair_params(number),
        name="updated_and_gathered",
        in_specs=[vmem] * 3 + [anywhere] * 9,
        out_specs=[anywhere] * 8,
        out_shape=[
            jax.ShapeDtypeStruct((SIDE, SIDE, 2, 2, rows, width), BF16),
            jax.ShapeDtypeStruct((own_rows, d), BF16),
            *[jax.ShapeDtypeStruct(t.shape, F32) for t in (m_gate, m_up, m_down, v_gate, v_up, v_down)],
        ],
        scratch_shapes=[
            pltpu.VMEM((2, layers, rows, half), BF16),
            pltpu.VMEM((layers, own_rows, d), BF16),
            pltpu.VMEM((4, 2, layers, moment_rows, half), F32),
            pltpu.VMEM((2, layers, own_rows, d), F32),
            pltpu.VMEM((2, rows, width), BF16),
            pltpu.VMEM((own_rows, d), BF16),
            pltpu.VMEM((8, 128), F32),
            pltpu.VMEM((n, 8, 128), F32),
            pltpu.SemaphoreType.DMA((13,)),
            pltpu.SemaphoreType.DMA((16,)),
            pltpu.SemaphoreType.DMA((16,)),
            pltpu.SemaphoreType.DMA((n,)),
            pltpu.SemaphoreType.DMA((n,)),
            pltpu.SemaphoreType.DMA((124,)),
            pltpu.SemaphoreType.DMA((124,)),
        ],
    )(gate_up0, down0, last_layer, w_gate, w_up, w_down, m_gate, m_up, m_down, v_gate, v_up, v_down)
    return packs, last, *moments


def placed(packs, layers, d, ff):
    rows, width = packs.shape[-2:]
    half = ff // 2
    per = 2

    def body(t, gate, up, down):
        for b in range(per):
            for core in range(2):
                for color in range(2):
                    r = slice(b * rows, (b + 1) * rows)
                    c = slice(core * half, (core + 1) * half)
                    gate[color, r, c] = t[b, core, color, :, :half]
                    up[color, r, c] = t[b, core, color, :, half : 2 * half]
                    at = ((b * 2 + core) * 2 + color) * rows
                    down[at : at + rows, :] = t[b, core, color, :, 2 * half :]

    n = SIDE // per
    out = pl.BlockSpec((layers, per * rows, ff), lambda i, j: (0, i * n + j, 0))
    return call(
        body,
        1,
        4 * packs.size,
        name="placed",
        grid=(SIDE, n),
        in_specs=[pl.BlockSpec((None, per, 2, 2, rows, width), lambda i, j: (i, j, 0, 0, 0, 0))],
        out_specs=[out, out, pl.BlockSpec((None, per * 4 * rows, d), lambda i, j: (0, i * n + j, 0))],
        out_shape=[jax.ShapeDtypeStruct((layers, d, ff), BF16)] * 2 + [jax.ShapeDtypeStruct((layers, ff, d), BF16)],
    )(packs)


def copied(*arrays):
    steps = 4

    def body(*refs):
        for a, b in zip(refs[: len(arrays)], refs[len(arrays) :], strict=True):
            b[...] = a[...]

    specs = [pl.BlockSpec((t.shape[0] // steps, *t.shape[1:]), lambda i: (i, 0, 0)) for t in arrays]
    return call(
        body,
        1,
        sum(8 * t.size for t in arrays),
        name="copied",
        grid=(steps,),
        in_specs=specs,
        out_specs=specs,
        out_shape=[jax.ShapeDtypeStruct(t.shape, t.dtype) for t in arrays],
    )(*arrays)


def placed_last(down, gathered):
    layers, ff, d = down.shape
    bm = 1152

    def body(down, t, out):
        out[...] = t[...]

    return call(
        body,
        1,
        4 * gathered.size,
        name="placed_last",
        grid=(ff // bm,),
        in_specs=[pl.BlockSpec(memory_space=pl.ANY), pl.BlockSpec((bm, d), lambda i: (i, 0))],
        out_specs=pl.BlockSpec((None, bm, d), lambda i: (layers - 1, i, 0)),
        out_shape=jax.ShapeDtypeStruct(down.shape, BF16),
        input_output_aliases={0: 0},
    )(down, gathered)


def solution(mesh):
    chips = mesh.shape["dp"] // 2
    same_core = [[2 * chip + core for chip in range(chips)] for core in range(2)]

    def summed(part):
        return lax.psum_scatter(part, "dp", scatter_dimension=0, axis_index_groups=same_core, tiled=True)

    def step(x, dy, w_gate, w_up, w_down, *moments):
        x, dy = x[0], dy[0]
        layers, d, ff = w_gate.shape

        gate, up, hid0, a0_t = hidden_forward(0, x, w_gate, w_up)
        h1, a1, a1_t = down_forward(0, x, hid0, w_down)
        hid1, dg1, du1 = last_layer(1, a1, dy, w_gate, w_up, w_down)
        joint = gate_up_gradient(1, a1_t, dg1, du1)
        joint = down_gradient(2, hid1, dy, joint)
        dg1, du1, joint = lax.optimization_barrier((dg1, du1, joint))
        of_last = summed(joint.reshape(-1, joint.shape[-1])).reshape(joint.shape[1:])
        dh = states_cotangent(1, h1, dy, dg1, du1, w_gate, w_up)
        down0 = down_gradient(3, hid0, dh)
        dh, down0 = lax.optimization_barrier((dh, down0))
        down0 = summed(down0)
        gate_up0 = first_layer_gradient(4, 0, a0_t, dh, gate, up, w_down)
        gate_up0, of_last = lax.optimization_barrier((gate_up0, of_last))
        of_last, down0 = lax.optimization_barrier((of_last, down0))
        packs, last, *moments = updated_and_gathered(5, gate_up0, down0, of_last, w_gate, w_up, w_down, *moments)
        last = lax.all_gather(last, "dp", tiled=True)
        new_gate, new_up, new_down = placed(packs, layers, d, ff)
        down_moments = [t.reshape(-1, t.shape[1] // 2, d) for t in moments[2::3]]
        moments = copied(*(t for k, t in enumerate(moments) if k % 3 < 2), *down_moments)
        down_moments = [t.reshape(layers, -1, d) for t in moments[4:]]
        moments = [t.transpose(1, 0, 2) for t in moments[:4]]
        moments = [*moments[:2], down_moments[0], *moments[2:], down_moments[1]]
        new_down = placed_last(new_down, last)
        return new_gate, new_up, new_down, *moments

    sequences = P(("rep", "dp"))
    return jax.shard_map(
        step,
        mesh=mesh,
        in_specs=(sequences, sequences, P(), P(), P(), *[P(None, "dp")] * 6),
        out_specs=(P("rep"), P("rep"), P("rep"), *[P("rep", "dp")] * 6),
        check_vma=False,
    )
```

```python
import functools
import math

import jax
import jax.numpy as jnp
from jax import lax
from jax.experimental import pallas as pl
from jax.experimental.pallas import tpu as pltpu
from jax.sharding import PartitionSpec as P

F32, BF16 = jnp.float32, jnp.bfloat16
VMEM_LIMIT = 67_043_328
NN = (((1,), (0,)), ((), ()))
NT = (((1,), (1,)), ((), ()))
TN = (((0,), (0,)), ((), ()))


def dot(a, b, dims=NN):
    return lax.dot_general(a, b, dims, preferred_element_type=F32)


def sigmoid(x):
    return 1.0 / (1.0 + jnp.exp(-x))


def whole(shape):
    return pl.BlockSpec(shape, lambda *_: (0,) * len(shape), pipeline_mode=pl.Buffered(1))


def call(body, flops, moved, params=None, **kw):
    return pl.pallas_call(
        body,
        cost_estimate=pl.CostEstimate(flops=int(flops), bytes_accessed=int(moved), transcendentals=0),
        compiler_params=pltpu.CompilerParams(**{"vmem_limit_bytes": VMEM_LIMIT, **(params or {})}),
        **kw,
    )


def row_scale(wide):
    return lax.rsqrt(jnp.mean(wide * wide, -1, keepdims=True) + 1e-6)


def hidden_forward(layer, x, w_gate, w_up):
    tokens, d = x.shape
    ff = w_gate.shape[-1]
    bf, bm = 256, 512
    n = tokens // bm

    def body(x, wg, wu, gate, up, hid, a_t, x_in, a, came):
        j = pl.program_id(0)

        def rows(i):
            return pl.ds(pl.multiple_of(i * bm, bm), bm)

        def come(i):
            return pltpu.make_async_copy(x.at[rows(i)], x_in.at[rows(i)], came.at[i])

        def chunk(r):
            g, u = dot(a[r, :], wg[...]), dot(a[r, :], wu[...])
            gate[r, :] = g
            up[r, :] = u
            hid[r, :] = (g * sigmoid(g) * u).astype(BF16)

        @pl.when(j == 0)
        def _():
            for i in range(n):
                come(i).start()

            def first(i, _):
                come(i).wait()
                wide = x_in[rows(i), :].astype(F32)
                unit = wide * row_scale(wide)
                a[rows(i), :] = unit.astype(BF16)
                a_t[:, rows(i)] = unit.T.astype(BF16)
                chunk(rows(i))
                return 0

            lax.fori_loop(0, n, first, 0)

        @pl.when(j > 0)
        def _():
            for i in range(n):
                chunk(slice(i * bm, (i + 1) * bm))

    w_spec = pl.BlockSpec((None, d, bf), lambda j: (layer, 0, j))
    o_spec = pl.BlockSpec((tokens, bf), lambda j: (0, j))
    wide = jax.ShapeDtypeStruct((tokens, ff), F32)
    return call(
        body,
        4 * tokens * d * ff,
        10 * tokens * ff + 4 * d * ff,
        name="hidden_forward",
        grid=(ff // bf,),
        in_specs=[pl.BlockSpec(memory_space=pl.ANY), w_spec, w_spec],
        out_specs=[*[o_spec] * 3, whole((d, tokens))],
        out_shape=(wide, wide, jax.ShapeDtypeStruct((tokens, ff), BF16), jax.ShapeDtypeStruct((d, tokens), BF16)),
        scratch_shapes=[pltpu.VMEM((tokens, d), BF16), pltpu.VMEM((tokens, d), BF16), pltpu.SemaphoreType.DMA((n,))],
    )(x, w_gate, w_up)


def down_forward(layer, x, hid, w_down):
    tokens, ff = hid.shape
    d = x.shape[-1]
    bm = 256

    def body(x, hid, wd, h1, a1, a1_t):
        h = (x[...].astype(F32) + dot(hid[...], wd[...]).astype(BF16).astype(F32)).astype(BF16)
        h1[...] = h
        wide = h.astype(F32)
        unit = wide * row_scale(wide)
        a1[...] = unit.astype(BF16)
        a1_t[...] = unit.T.astype(BF16)

    rows = pl.BlockSpec((bm, d), lambda i: (i, 0))
    out = jax.ShapeDtypeStruct((tokens, d), BF16)
    return call(
        body,
        2 * tokens * d * ff,
        2 * tokens * ff + 2 * d * ff,
        name="down_forward",
        grid=(tokens // bm,),
        in_specs=[
            rows,
            pl.BlockSpec((bm, ff), lambda i: (i, 0)),
            pl.BlockSpec((None, ff, d), lambda i: (layer, 0, 0), pipeline_mode=pl.Buffered(1)),
        ],
        out_specs=[rows, rows, pl.BlockSpec((d, bm), lambda i: (0, i))],
        out_shape=(out, out, jax.ShapeDtypeStruct((d, tokens), BF16)),
    )(x, hid, w_down)


def gate_up_cotangents(g, u, dh):
    dh = dh.astype(BF16).astype(F32)
    s = sigmoid(g)
    silu = g * s
    return (dh * u * (s + silu * (1.0 - s))).astype(BF16), (dh * silu).astype(BF16), (silu * u).astype(BF16)


def last_layer(layer, a, dy, w_gate, w_up, w_down):
    tokens, d = a.shape
    ff = w_gate.shape[-1]
    bf, bm = 256, 512

    def body(a, dy, wg, wu, wd, hid, dg, du):
        for i in range(tokens // bm):
            r = slice(i * bm, (i + 1) * bm)
            g, u = dot(a[r, :], wg[...]), dot(a[r, :], wu[...])
            dg[r, :], du[r, :], hid[r, :] = gate_up_cotangents(g, u, dot(dy[r, :], wd[...], NT))

    w_spec = pl.BlockSpec((None, d, bf), lambda j: (layer, 0, j))
    o_spec = pl.BlockSpec((tokens, bf), lambda j: (0, j))
    out = jax.ShapeDtypeStruct((tokens, ff), BF16)
    return call(
        body,
        6 * tokens * d * ff,
        6 * tokens * ff + 6 * d * ff,
        name="last_layer",
        grid=(ff // bf,),
        in_specs=[whole((tokens, d)), whole((tokens, d)), w_spec, w_spec, pl.BlockSpec((None, bf, d), lambda j: (layer, j, 0))],
        out_specs=[o_spec] * 3,
        out_shape=(out, out, out),
    )(a, dy, w_gate, w_up, w_down)


def states_cotangent(layer, h, dy, dg, du, w_gate, w_up):
    tokens, ff = dg.shape
    d = h.shape[-1]
    bm, bk = 256, 512
    n = ff // bk

    def body(h, dy, dg, du, wg, wu, out, w, total, came):
        def k(c):
            return pl.ds(pl.multiple_of(c * bk, bk), bk)

        def come(c):
            return [pltpu.make_async_copy(t.at[layer, :, k(c)], w.at[i, :, k(c)], came.at[i, c]) for i, t in enumerate((wg, wu))]

        def rest(da):
            wide = h[...].astype(F32)
            da = da.astype(BF16).astype(F32)
            s = row_scale(wide)
            back = da * s - wide * (s * s * s * jnp.mean(da * wide, -1, keepdims=True))
            out[...] = (dy[...].astype(F32) + back).astype(BF16)

        @pl.when(pl.program_id(0) == 0)
        def _():
            for c in range(n):
                for copy in come(c):
                    copy.start()
            total[...] = jnp.zeros_like(total)

            def add(c, _):
                for copy in come(c):
                    copy.wait()
                total[...] += dot(dg[:, k(c)], w[0, :, k(c)], NT) + dot(du[:, k(c)], w[1, :, k(c)], NT)
                return 0

            lax.fori_loop(0, n, add, 0)
            rest(total[...])

        @pl.when(pl.program_id(0) > 0)
        def _():
            rest(dot(dg[...], w[0], NT) + dot(du[...], w[1], NT))

    rows = pl.BlockSpec((bm, d), lambda i: (i, 0))
    wide_rows = pl.BlockSpec((bm, ff), lambda i: (i, 0))
    anywhere = pl.BlockSpec(memory_space=pl.ANY)
    return call(
        body,
        4 * tokens * d * ff,
        4 * tokens * ff + 4 * d * ff,
        name="states_cotangent",
        grid=(tokens // bm,),
        in_specs=[rows, rows, wide_rows, wide_rows, anywhere, anywhere],
        out_specs=rows,
        out_shape=jax.ShapeDtypeStruct((tokens, d), BF16),
        scratch_shapes=[pltpu.VMEM((2, d, ff), BF16), pltpu.VMEM((bm, d), F32), pltpu.SemaphoreType.DMA((2, n))],
    )(h, dy, dg, du, w_gate, w_up)


SLOTS, ARRIVALS = 3, 4


def pair_scratch(rows, columns):
    return [
        pltpu.VMEM((SLOTS, 2, rows, columns), BF16),
        pltpu.VMEM((ARRIVALS, rows, columns), BF16),
        pltpu.SemaphoreType.DMA((SLOTS,)),
        pltpu.SemaphoreType.DMA((ARRIVALS,)),
    ]


def pair_step(n, make, put, made, came, sent, arrived):
    j = pl.program_id(0)
    me = lax.axis_index("dp")
    core = lax.rem(me, 2)
    other = me + 1 - 2 * core

    def transfer(step):
        slot, place = lax.rem(step, SLOTS), lax.rem(step, ARRIVALS)
        return pltpu.make_async_remote_copy(
            src_ref=made.at[slot, 1 - core],
            dst_ref=came.at[place],
            send_sem=sent.at[slot],
            recv_sem=arrived.at[place],
            device_id={"dp": other},
            device_id_type=pl.DeviceIdType.MESH,
        )

    @pl.when(j == 0)
    def _():
        barrier = pltpu.get_barrier_semaphore()
        pl.semaphore_signal(barrier, inc=1, device_id={"dp": other}, device_id_type=pl.DeviceIdType.MESH)
        pl.semaphore_wait(barrier, 1)

    @pl.when(j >= 2)
    def _():
        transfer(j - 2).wait()
        own = made[lax.rem(j - 2, SLOTS), core]
        put(own.astype(F32) + came[lax.rem(j - 2, ARRIVALS)].astype(F32))

    @pl.when(j < n)
    def _():
        make(made.at[lax.rem(j, SLOTS)])
        transfer(j).start()


def pair_params(number):
    return {"collective_id": number, "has_side_effects": True}


def down_gradient(number, hid, dy, joint=None):
    tokens, ff = hid.shape
    d = dy.shape[-1]
    chips = lax.axis_size("dp") // 2
    own = ff // (2 * chips)
    bf = 1152
    n, per = ff // bf, bf // (2 * own)

    def body(hid, dy, *rest):
        out, *scratch = rest[0 if joint is None else 1 :]

        def make(slot):
            block = dot(hid[...], dy[...], TN)
            for i in range(per):
                for half in range(2):
                    at = (2 * i + half) * own
                    slot[half, i * own : (i + 1) * own, :] = block[at : at + own].astype(BF16)

        def put(total):
            if joint is None:
                out[...] = total.astype(BF16)
            else:
                for i in range(per):
                    for half in range(2):
                        at = i * own + half * (own // 2)
                        out[i, :, half * d : (half + 1) * d] = total[at : at + own // 2].astype(BF16)

        pair_step(n, make, put, *scratch)

    if joint is None:
        more, out_shape = [], jax.ShapeDtypeStruct((ff // 2, d), BF16)
        out_spec = pl.BlockSpec((bf // 2, d), lambda j: (jnp.maximum(j - 2, 0), 0))
    else:
        more, out_shape = [joint], jax.ShapeDtypeStruct(joint.shape, BF16)
        out_spec = pl.BlockSpec((per, None, own // 2, 2 * d), lambda j: (jnp.maximum(j - 2, 0), 2, 0, 0))
    return call(
        body,
        2 * tokens * d * ff,
        2 * tokens * ff + d * ff,
        pair_params(number),
        name=f"down_gradient_{number}",
        grid=(n + 2,),
        in_specs=[
            pl.BlockSpec((tokens, bf), lambda j: (0, jnp.minimum(j, n - 1))),
            whole((tokens, d)),
            *[pl.BlockSpec(memory_space=pl.ANY) for _ in more],
        ],
        out_specs=out_spec,
        out_shape=out_shape,
        scratch_shapes=pair_scratch(bf // 2, d),
        input_output_aliases={2: 0} if more else {},
    )(hid, dy, *more)


PART = 256


def halves_specs(shape, first, n, half, layer=None, transposed=False):
    def spec(h):
        def at(j):
            k = h * half + first + jnp.minimum(j, n - 1)
            index = (k, 0) if transposed else (0, k)
            return index if layer is None else (layer, *index)

        return pl.BlockSpec(shape, at)

    return [spec(0), spec(1)]


def gate_up_gradient(number, a_t, dg, du):
    d, tokens = a_t.shape
    half = dg.shape[-1] // (2 * PART)
    n = half
    chips = lax.axis_size("dp") // 2
    rows = d // chips

    def body(a_t, dg0, dg1, du0, du1, out, *scratch):
        def make(slot):
            for h, (dg, du) in enumerate(((dg0, du0), (dg1, du1))):
                slot[h, :, :PART] = dot(a_t[...], dg[...]).astype(BF16)
                slot[h, :, PART:] = dot(a_t[...], du[...]).astype(BF16)

        def put(total):
            for k in range(chips):
                for i in range(2):
                    out[k, i] = total[k * rows : (k + 1) * rows, i * PART : (i + 1) * PART].astype(BF16)

        pair_step(n, make, put, *scratch)

    t_specs = halves_specs((tokens, PART), 0, n, half)
    return call(
        body,
        8 * tokens * d * PART * n,
        8 * tokens * PART * n,
        pair_params(number),
        name=f"gate_up_gradient_{number}",
        grid=(n + 2,),
        in_specs=[whole((d, tokens)), *t_specs, *t_specs],
        out_specs=pl.BlockSpec((chips, 2, rows, PART), lambda j: (0, 0, 0, jnp.maximum(j - 2, 0))),
        out_shape=jax.ShapeDtypeStruct((chips, 3, rows, PART * n), BF16),
        scratch_shapes=pair_scratch(d, 2 * PART),
    )(a_t, dg, dg, du, du)


SIDE = 4
PLACES = 4


def first_layer_gradient(number, layer, a_t, dy, gate, up, w_down):
    d, tokens = a_t.shape
    half = gate.shape[-1] // (2 * PART)
    n = half
    bm = 512
    rows = d // SIDE**2
    mid = PART // 2

    def body(a_t, dy, g0, g1, u0, u1, w0, w1, out, dg, du, made, came, sums, across1, pass1, got1, total1, across2, pass2, got2, ps, pr, sent, arrived):
        j = pl.program_id(0)
        me = lax.axis_index("dp")
        core = lax.rem(me, 2)
        other = me + 1 - 2 * core
        x, y = lax.div(me, 2 * SIDE), lax.rem(lax.div(me, 2), SIDE)

        def at(x, y):
            return {"dp": (x * SIDE + y) * 2 + core}

        def beside(axis, way):
            to = lax.rem((x if axis == 0 else y) + (1 if way == 0 else SIDE - 1), SIDE)
            return at(to, y) if axis == 0 else at(x, to)

        here = (x, y)

        def transfer(stage, color, way, block):
            place = lax.rem(block, PLACES)
            first, second = color, 1 - color
            columns = slice(color * PART, (color + 1) * PART)
            if stage == 1:
                far = lax.rem(here[first] + 2, SIDE)
                part = slice(2 * way, 2 * way + 2)
                src = sums.at[place, far, part, :, columns] if color == 0 else sums.at[place, part, far, :, columns]
                dst = across1.at[color, place, way]
            elif stage == 2:
                src, dst = pass1.at[color, lax.rem(block, 2), way], got1.at[color, place, way]
            elif stage == 3:
                far = lax.rem(here[second] + 2, SIDE)
                src = total1.at[color, place, far, :, slice(way * mid, (way + 1) * mid)]
                dst = across2.at[color, place, way]
            else:
                src, dst = pass2.at[color, place, way], got2.at[color, place, way]
            index = ((stage - 1) * 2 + color) * 2 + way
            return pltpu.make_async_remote_copy(
                src_ref=src,
                dst_ref=dst,
                send_sem=sent.at[index, place],
                recv_sem=arrived.at[index, place],
                device_id=beside(first if stage <= 2 else second, way),
                device_id_type=pl.DeviceIdType.MESH,
            )

        def swap(block):
            slot, place = lax.rem(block, SLOTS), lax.rem(block, PLACES)
            return pltpu.make_async_remote_copy(
                src_ref=made.at[slot, 1 - core],
                dst_ref=came.at[place],
                send_sem=ps.at[slot],
                recv_sem=pr.at[place],
                device_id={"dp": other},
                device_id_type=pl.DeviceIdType.MESH,
            )

        def of(color, place, i):
            columns = slice(color * PART, (color + 1) * PART)
            t = sums[place, i, :, :, columns] if color == 0 else sums[place, :, i, :, columns]
            return t.astype(F32)

        def stage(lag, act):
            @pl.when((j >= lag) & (j < n + lag))
            def _():
                act(j - lag)

        @pl.when(j == 0)
        def _():
            barrier = pltpu.get_barrier_semaphore()
            for peer in ({"dp": other}, beside(0, 0), beside(0, 1), beside(1, 0), beside(1, 1)):
                pl.semaphore_signal(barrier, inc=1, device_id=peer, device_id_type=pl.DeviceIdType.MESH)
            pl.semaphore_wait(barrier, 5)

        def last(block):
            place = lax.rem(block, PLACES)
            for color in range(2):
                for way in range(2):
                    transfer(4, color, way, block).wait()
                b = here[1 - color]
                t = total1[color, place, b].astype(F32) + got2[color, place, 0].astype(F32) + got2[color, place, 1].astype(F32)
                out[color] = t.astype(BF16)

        def fourth(block):
            place = lax.rem(block, PLACES)
            for color in range(2):
                for way in range(2):
                    transfer(3, color, way, block).wait()
                for way in range(2):
                    b = lax.rem(here[1 - color] + (1 if way == 0 else SIDE - 1), SIDE)
                    pass2[color, place, way] = total1[color, place, b]
                    c = slice(way * mid, (way + 1) * mid)
                    more = total1[color, place, b, :, c].astype(F32) + across2[color, place, way].astype(F32)
                    pass2[color, place, way, :, c] = more.astype(BF16)
                    transfer(4, color, way, block).start()

        def third(block):
            place = lax.rem(block, PLACES)
            for color in range(2):
                for way in range(2):
                    transfer(2, color, way, block).wait()
                t = of(color, place, here[color]) + got1[color, place, 0].astype(F32) + got1[color, place, 1].astype(F32)
                total1[color, place] = t.astype(BF16)
                for way in range(2):
                    transfer(3, color, way, block).start()

        def second(block):
            place = lax.rem(block, PLACES)
            for color in range(2):
                for way in range(2):
                    transfer(1, color, way, block).wait()
                for way in range(2):
                    t = of(color, place, lax.rem(here[color] + (1 if way == 0 else SIDE - 1), SIDE))
                    p = slice(2 * way, 2 * way + 2)
                    q = slice(2 - 2 * way, 4 - 2 * way)
                    pass1[color, lax.rem(block, 2), way, p] = (t[p] + across1[color, place, way].astype(F32)).astype(BF16)
                    pass1[color, lax.rem(block, 2), way, q] = t[q].astype(BF16)
                    transfer(2, color, way, block).start()

        def first(block):
            place, slot = lax.rem(block, PLACES), lax.rem(block, SLOTS)
            swap(block).wait()
            for k in range(SIDE**2):
                r = slice(k * rows, (k + 1) * rows)
                t = made[slot, core, r, :].astype(F32) + came[place, r, :].astype(F32)
                sums[place, k // SIDE, k % SIDE] = t.astype(BF16)
            for color in range(2):
                for way in range(2):
                    transfer(1, color, way, block).start()

        def make(block):
            slot = lax.rem(block, SLOTS)
            for h, (g, u, w) in enumerate(((g0, u0, w0), (g1, u1, w1))):
                for i in range(tokens // bm):
                    r = slice(i * bm, (i + 1) * bm)
                    dg[h, r, :], du[h, r, :], _ = gate_up_cotangents(g[r, :], u[r, :], dot(dy[r, :], w[...], NT))
                made[slot, h, :, :PART] = dot(a_t[...], dg[h]).astype(BF16)
                made[slot, h, :, PART:] = dot(a_t[...], du[h]).astype(BF16)
            swap(block).start()

        stage(7, last)
        stage(6, fourth)
        stage(5, third)
        stage(3, second)
        stage(2, first)
        stage(0, make)

    t_specs = halves_specs((tokens, PART), 0, n, half)
    block = (SIDE, rows, PART)
    return call(
        body,
        12 * tokens * d * PART * n,
        16 * tokens * PART * n,
        pair_params(number),
        name="first_layer_gradient",
        grid=(n + 7,),
        in_specs=[whole((d, tokens)), whole((tokens, d)), *t_specs, *t_specs, *halves_specs((None, PART, d), 0, n, half, layer, True)],
        out_specs=pl.BlockSpec((2, rows, PART), lambda j: (0, 0, jnp.maximum(j - 7, 0))),
        out_shape=jax.ShapeDtypeStruct((2, rows, PART * n), BF16),
        scratch_shapes=[
            pltpu.VMEM((2, tokens, PART), BF16),
            pltpu.VMEM((2, tokens, PART), BF16),
            pltpu.VMEM((SLOTS, 2, d, 2 * PART), BF16),
            pltpu.VMEM((PLACES, d, 2 * PART), BF16),
            pltpu.VMEM((PLACES, SIDE, SIDE, rows, 2 * PART), BF16),
            pltpu.VMEM((2, PLACES, 2, SIDE // 2, rows, PART), BF16),
            pltpu.VMEM((2, 2, 2, *block), BF16),
            pltpu.VMEM((2, PLACES, 2, *block), BF16),
            pltpu.VMEM((2, PLACES, *block), BF16),
            pltpu.VMEM((2, PLACES, 2, rows, mid), BF16),
            pltpu.VMEM((2, PLACES, 2, rows, PART), BF16),
            pltpu.VMEM((2, PLACES, 2, rows, PART), BF16),
            pltpu.SemaphoreType.DMA((SLOTS,)),
            pltpu.SemaphoreType.DMA((PLACES,)),
            pltpu.SemaphoreType.DMA((16, PLACES)),
            pltpu.SemaphoreType.DMA((16, PLACES)),
        ],
    )(a_t, dy, gate, gate, up, up, w_down, w_down)


def updated_and_gathered(number, gate_up0, down0, last_layer, w_gate, w_up, w_down, m_gate, m_up, m_down, v_gate, v_up, v_down):
    n = lax.axis_size("dp")
    layers, d, ff = w_gate.shape
    rows, half = gate_up0.shape[1:]
    own_rows, moment_rows = ff // n, d // n
    steps = half // PART
    width = 2 * half + d
    cut = -(-width // 256) * 128
    count = 3 * layers * d * ff
    parts = (slice(0, cut), slice(cut, width))
    plan = []

    def body(gu0, d0, gu1, wg, wu, wd, mg, mu, md, vg, vu, vd, ag, wd1, nmg, nmu, nmd, nvg, nvu, nvd,
             w_gu, w_d, mom, mom_d, packs, spare, tile, tiles, load, swap_s, swap_r, norm_s, norm_r, sent, arrived):
        me = lax.axis_index("dp")
        core = lax.rem(me, 2)
        other = me + 1 - 2 * core
        chip = lax.div(me, 2)
        x, y = lax.div(chip, SIDE), lax.rem(chip, SIDE)
        here = (x, y)
        mine, theirs = (pl.ds(pl.multiple_of(c * half, 128), half) for c in (core, 1 - core))

        moments = (mg, mu, vg, vu)
        new_moments = (nmg, nmu, nvg, nvu)
        loads = [
            *[(t.at[:, l, mine], mom.at[k, core, l]) for k, t in enumerate(moments) for l in range(layers)],
            (md, mom_d.at[0]),
            (vd, mom_d.at[1]),
            (wg.at[:, pl.ds(pl.multiple_of(chip * rows, 8), rows), mine], w_gu.at[0]),
            (wu.at[:, pl.ds(pl.multiple_of(chip * rows, 8), rows), mine], w_gu.at[1]),
            (wd.at[:, pl.ds(pl.multiple_of(me * own_rows, 16), own_rows), :], w_d),
        ]
        loads = [pltpu.make_async_copy(a, b, load.at[k]) for k, (a, b) in enumerate(loads)]
        for copy in loads:
            copy.start()

        barrier = pltpu.get_barrier_semaphore()

        def greet(i, _):
            pl.semaphore_signal(barrier, inc=1, device_id={"dp": lax.rem(me + i, n)}, device_id_type=pl.DeviceIdType.MESH)
            return 0

        lax.fori_loop(1, n, greet, 0)

        def square(t):
            t = t.astype(F32)
            t = t * t
            return sum(t[k * 8 : (k + 1) * 8] for k in range(t.shape[0] // 8))

        def squares(k, total):
            at = pl.ds(pl.multiple_of(k * PART, PART), PART)
            return total + sum(square(gu0[i, :, at]) for i in range(2)) + sum(square(gu1[i, :, at]) for i in range(3))

        total = lax.fori_loop(0, steps, squares, jnp.zeros((8, PART), F32))
        downs = square(d0[...])
        total = total[:, :128] + total[:, 128:] + sum(downs[:, k * 128 : (k + 1) * 128] for k in range(d // 128))
        tile[...] = total
        tiles[0] = total

        pl.semaphore_wait(barrier, n - 1)

        def swap(src, dst, k):
            return pltpu.make_async_remote_copy(
                src_ref=src, dst_ref=dst, send_sem=swap_s.at[k], recv_sem=swap_r.at[k], device_id={"dp": other}, device_id_type=pl.DeviceIdType.MESH
            )

        def size(i):
            return pltpu.make_async_remote_copy(
                src_ref=tile,
                dst_ref=tiles.at[i],
                send_sem=norm_s.at[i],
                recv_sem=norm_r.at[i],
                device_id={"dp": lax.rem(me + i, n)},
                device_id_type=pl.DeviceIdType.MESH,
            )

        lax.fori_loop(1, n, lambda i, _: (size(i).start(), 0)[1], 0)
        swaps = [swap(t.at[:, l, theirs], mom.at[k, core, l], k * layers + l) for k, t in enumerate(moments) for l in range(layers)]
        for copy in swaps:
            copy.start()
        for copy in loads:
            copy.wait()
        for copy in swaps:
            copy.wait()
        lax.fori_loop(1, n, lambda i, _: (size(i).wait(), 0)[1], 0)
        total = lax.fori_loop(0, n, lambda i, total: total + tiles[lax.rem(me - i + n, n)], jnp.zeros((8, 128), F32))
        total = jnp.sum(jnp.sum(total, 0, keepdims=True), 1, keepdims=True)
        factor = jnp.minimum(1.0, 0.5 * lax.rsqrt(total / count + 1e-30))

        def adamw(w, m, v, g):
            g = g * factor
            m = 0.9 * m + 0.1 * g
            v = 0.95 * v + 0.05 * g * g
            return w - 0.02 * (m * lax.rsqrt(v + 1e-8) + 0.1 * w), m, v

        def step_gate_up(layer):
            for gu in range(2):

                def columns(k, _, gu=gu):
                    at = pl.ds(pl.multiple_of(k * PART, PART), PART)
                    g = (gu0, gu1)[layer][gu, :, at].astype(F32)
                    w = w_gu[gu, layer, :, at].astype(F32)
                    new = []
                    for r in range(2):
                        p = slice(r * moment_rows, (r + 1) * moment_rows)
                        one, m, v = adamw(w[p], mom[gu, r, layer, :, at], mom[2 + gu, r, layer, :, at], g[p])
                        mom[gu, r, layer, :, at] = m
                        mom[2 + gu, r, layer, :, at] = v
                        new.append(one)
                    packs[layer, :, pl.ds(pl.multiple_of(gu * half + k * PART, PART), PART)] = jnp.concatenate(new, 0).astype(BF16)
                    return 0

                lax.fori_loop(0, steps, columns, 0)

        def step_down(layer, p, g):
            new, m, v = adamw(w_d[layer, p, :].astype(F32), mom_d[0, layer, p, :], mom_d[1, layer, p, :], g.astype(F32))
            mom_d[0, layer, p, :] = m
            mom_d[1, layer, p, :] = v
            return new.astype(BF16)

        def place(color, i, k, whose, part):
            i, k = (lax.rem(t + SIDE, SIDE) for t in (i, k))
            a, b = (i, k) if color == 0 else (k, i)
            return ag.at[a, b, whose, color, :, parts[part]]

        def beside(axis, way):
            to = lax.rem(here[axis] + (1 if way == 0 else SIDE - 1), SIDE)
            a, b = (to, y) if axis == 0 else (x, to)
            return {"dp": (a * SIDE + b) * 2 + core}

        started = {}

        def send(name, color, o, q, part, to):
            index = len(plan) if name not in plan else plan.index(name)
            if name not in plan:
                plan.append(name)
            dst = place(color, here[color] + o, here[1 - color] + q, core, part)
            src = packs.at[color, :, parts[part]] if (o, q) == (0, 0) else dst
            copy = pltpu.make_async_remote_copy(
                src_ref=src, dst_ref=dst, send_sem=sent.at[index], recv_sem=arrived.at[index], device_id=to, device_id_type=pl.DeviceIdType.MESH
            )
            copy.start()
            started[name] = copy

        def along_first(color, way, part):
            send(("a", color, way, part), color, 0, 0, part, beside(color, way))

        def on_first(color, way):
            send(("b", color, way), color, -1 if way == 0 else 1, 0, way, beside(color, way))

        def along_second(color, o, part):
            for way in range(2):
                send(("c", color, way, o, part), color, o, 0, part, beside(1 - color, way))

        def on_second(color, way, o):
            send(("d", color, way, o), color, o, -1 if way == 0 else 1, way, beside(1 - color, way))

        def share(color, o, q, part):
            send(("e", color, o, q, part), color, o, q, part, {"dp": other})

        def own(color):
            for part in range(2):
                for way in range(2):
                    along_first(color, way, part)
            for part in range(2):
                along_second(color, 0, part)
                share(color, 0, 0, part)
            copy = pltpu.make_async_copy(packs.at[color], ag.at[x, y, core, color], load.at[color])
            copy.start()
            return copy

        step_gate_up(0)
        packs[0, :, 2 * half :] = step_down(0, slice(0, rows), d0[:rows])
        kept = [own(0)]
        step_gate_up(1)
        packs[1, :, 2 * half :] = step_down(0, slice(rows, 2 * rows), d0[rows:])
        kept.append(own(1))
        for i in range(2):
            p = slice(i * rows, (i + 1) * rows)
            spare[p] = step_down(1, p, gu1[2, :, i * d : (i + 1) * d])

        stores = [
            *[(mom.at[k, core, l], t.at[:, l, mine]) for k, t in enumerate(new_moments) for l in range(layers)],
            (mom_d.at[0], nmd),
            (mom_d.at[1], nvd),
            (spare, wd1),
        ]
        stores = [pltpu.make_async_copy(a, b, load.at[2 + k]) for k, (a, b) in enumerate(stores)]
        backs = [swap(mom.at[k, 1 - core, l], t.at[:, l, mine], 8 + k * layers + l) for k, t in enumerate(new_moments) for l in range(layers)]
        for copy in (*stores, *backs):
            copy.start()

        both = [(color, way) for color in range(2) for way in range(2)]
        for part in range(2):
            for color, way in both:
                started["a", color, way, part].wait_recv()
                if way == part:
                    on_first(color, way)
                o = -1 if way == 0 else 1
                along_second(color, o, part)
                share(color, o, 0, part)

        def arrivals(o):
            for part in range(2):
                for color, way in both:
                    started["c", color, way, o, part].wait_recv()
                    if way == part:
                        on_second(color, way, o)
                    share(color, o, -1 if way == 0 else 1, part)

        arrivals(0)
        for color, way in both:
            started["b", color, way].wait_recv()
            along_second(color, 2, way)
            share(color, 2, 0, way)
        for o in (-1, 1, 2):
            arrivals(o)
        for o in (0, -1, 1, 2):
            for color, way in both:
                started["d", color, way, o].wait_recv()
                share(color, o, 2, way)
        for name, copy in started.items():
            copy.wait_send()
            if name[0] == "e":
                copy.wait_recv()
        for copy in (*kept, *stores, *backs):
            copy.wait()

    m_gate, m_up, v_gate, v_up = (t.transpose(1, 0, 2) for t in (m_gate, m_up, v_gate, v_up))
    anywhere = pl.BlockSpec(memory_space=pl.ANY)
    vmem = pl.BlockSpec(memory_space=pltpu.VMEM)
    packs, last, *moments = call(
        body,
        1e9,
        1e8,
        pair_params(number),
        name="updated_and_gathered",
        in_specs=[vmem] * 3 + [anywhere] * 9,
        out_specs=[anywhere] * 8,
        out_shape=[
            jax.ShapeDtypeStruct((SIDE, SIDE, 2, 2, rows, width), BF16),
            jax.ShapeDtypeStruct((own_rows, d), BF16),
            *[jax.ShapeDtypeStruct(t.shape, F32) for t in (m_gate, m_up, m_down, v_gate, v_up, v_down)],
        ],
        scratch_shapes=[
            pltpu.VMEM((2, layers, rows, half), BF16),
            pltpu.VMEM((layers, own_rows, d), BF16),
            pltpu.VMEM((4, 2, layers, moment_rows, half), F32),
            pltpu.VMEM((2, layers, own_rows, d), F32),
            pltpu.VMEM((2, rows, width), BF16),
            pltpu.VMEM((own_rows, d), BF16),
            pltpu.VMEM((8, 128), F32),
            pltpu.VMEM((n, 8, 128), F32),
            pltpu.SemaphoreType.DMA((13,)),
            pltpu.SemaphoreType.DMA((16,)),
            pltpu.SemaphoreType.DMA((16,)),
            pltpu.SemaphoreType.DMA((n,)),
            pltpu.SemaphoreType.DMA((n,)),
            pltpu.SemaphoreType.DMA((124,)),
            pltpu.SemaphoreType.DMA((124,)),
        ],
    )(gate_up0, down0, last_layer, w_gate, w_up, w_down, m_gate, m_up, m_down, v_gate, v_up, v_down)
    return packs, last, *moments


def placed(packs, layers, d, ff):
    rows, width = packs.shape[-2:]
    half = ff // 2
    per = 2

    def body(t, gate, up, down):
        for b in range(per):
            for core in range(2):
                for color in range(2):
                    r = slice(b * rows, (b + 1) * rows)
                    c = slice(core * half, (core + 1) * half)
                    gate[color, r, c] = t[b, core, color, :, :half]
                    up[color, r, c] = t[b, core, color, :, half : 2 * half]
                    at = ((b * 2 + core) * 2 + color) * rows
                    down[at : at + rows, :] = t[b, core, color, :, 2 * half :]

    n = SIDE // per
    out = pl.BlockSpec((layers, per * rows, ff), lambda i, j: (0, i * n + j, 0))
    return call(
        body,
        1,
        4 * packs.size,
        name="placed",
        grid=(SIDE, n),
        in_specs=[pl.BlockSpec((None, per, 2, 2, rows, width), lambda i, j: (i, j, 0, 0, 0, 0))],
        out_specs=[out, out, pl.BlockSpec((None, per * 4 * rows, d), lambda i, j: (0, i * n + j, 0))],
        out_shape=[jax.ShapeDtypeStruct((layers, d, ff), BF16)] * 2 + [jax.ShapeDtypeStruct((layers, ff, d), BF16)],
    )(packs)


def copied(*arrays):
    steps = 4

    def body(*refs):
        for a, b in zip(refs[: len(arrays)], refs[len(arrays) :], strict=True):
            b[...] = a[...]

    specs = [pl.BlockSpec((t.shape[0] // steps, *t.shape[1:]), lambda i: (i, 0, 0)) for t in arrays]
    return call(
        body,
        1,
        sum(8 * t.size for t in arrays),
        name="copied",
        grid=(steps,),
        in_specs=specs,
        out_specs=specs,
        out_shape=[jax.ShapeDtypeStruct(t.shape, t.dtype) for t in arrays],
    )(*arrays)


def placed_last(down, gathered):
    layers, ff, d = down.shape
    bm = 1152

    def body(down, t, out):
        out[...] = t[...]

    return call(
        body,
        1,
        4 * gathered.size,
        name="placed_last",
        grid=(ff // bm,),
        in_specs=[pl.BlockSpec(memory_space=pl.ANY), pl.BlockSpec((bm, d), lambda i: (i, 0))],
        out_specs=pl.BlockSpec((None, bm, d), lambda i: (layers - 1, i, 0)),
        out_shape=jax.ShapeDtypeStruct(down.shape, BF16),
        input_output_aliases={0: 0},
    )(down, gathered)


def solution(mesh):
    chips = mesh.shape["dp"] // 2
    same_core = [[2 * chip + core for chip in range(chips)] for core in range(2)]

    def summed(part):
        return lax.psum_scatter(part, "dp", scatter_dimension=0, axis_index_groups=same_core, tiled=True)

    def step(x, dy, w_gate, w_up, w_down, *moments):
        x, dy = x[0], dy[0]
        layers, d, ff = w_gate.shape

        gate, up, hid0, a0_t = hidden_forward(0, x, w_gate, w_up)
        h1, a1, a1_t = down_forward(0, x, hid0, w_down)
        hid1, dg1, du1 = last_layer(1, a1, dy, w_gate, w_up, w_down)
        joint = gate_up_gradient(1, a1_t, dg1, du1)
        joint = down_gradient(2, hid1, dy, joint)
        dg1, du1, joint = lax.optimization_barrier((dg1, du1, joint))
        of_last = summed(joint.reshape(-1, joint.shape[-1])).reshape(joint.shape[1:])
        dh = states_cotangent(1, h1, dy, dg1, du1, w_gate, w_up)
        down0 = down_gradient(3, hid0, dh)
        dh, down0 = lax.optimization_barrier((dh, down0))
        down0 = summed(down0)
        gate_up0 = first_layer_gradient(4, 0, a0_t, dh, gate, up, w_down)
        gate_up0, of_last = lax.optimization_barrier((gate_up0, of_last))
        of_last, down0 = lax.optimization_barrier((of_last, down0))
        packs, last, *moments = updated_and_gathered(5, gate_up0, down0, of_last, w_gate, w_up, w_down, *moments)
        last = lax.all_gather(last, "dp", tiled=True)
        new_gate, new_up, new_down = placed(packs, layers, d, ff)
        down_moments = [t.reshape(-1, t.shape[1] // 2, d) for t in moments[2::3]]
        moments = copied(*(t for k, t in enumerate(moments) if k % 3 < 2), *down_moments)
        down_moments = [t.reshape(layers, -1, d) for t in moments[4:]]
        moments = [t.transpose(1, 0, 2) for t in moments[:4]]
        moments = [*moments[:2], down_moments[0], *moments[2:], down_moments[1]]
        new_down = placed_last(new_down, last)
        return new_gate, new_up, new_down, *moments

    sequences = P(("rep", "dp"))
    return jax.shard_map(
        step,
        mesh=mesh,
        in_specs=(sequences, sequences, P(), P(), P(), *[P(None, "dp")] * 6),
        out_specs=(P("rep"), P("rep"), P("rep"), *[P("rep", "dp")] * 6),
        check_vma=False,
    )
```
